32 devices in a mesh: dp: 4 (over x, y), sp: 8 (over z, core).
Axes of the slice: x: 2, y: 2, z: 4, core: 2. Of those that a mesh axis runs over, the one named last changes fastest.
Arguments:
- x: bfloat16 [16384, 2304], P(('dp', 'sp')), parts along dimension 0
- gain: bfloat16 [2304], replicated
- wq: bfloat16 [2304, 2048], replicated
- wk: bfloat16 [2304, 1024], replicated
- wv: bfloat16 [2304, 1024], replicated
- wo: bfloat16 [2048, 2304], replicated
Outputs:
- output: bfloat16 [16384, 2304], P(('dp', 'sp')), parts along dimension 0
There are 4 independent parts. The reference program is written for one: setup_inputs(seed, part) draws one part's arguments, and reference() takes and returns one part's arrays. A program takes and returns all parts, laid end to end along the dimension named above; an argument that names none is the same for every part.
All inputs are finite; a program needn't handle non-finite values.
Results may differ from the reference program's by a relative error of at most 0.012.
Values are sent between devices in bfloat16 or wider.
A program may use at most 2 GiB of HBM per device.

```python
import jax
import jax.numpy as jnp
from jax import lax

ROWS = 4096
D = 2304
HEADS = 8
KV_HEADS = 4
HEAD = 256
THETA = 10000


def setup_inputs(seed: int = 0, part: int = 0) -> dict:
    kx, kn, kq, kk, kv, ko = jax.random.split(jax.random.key(seed), 6)

    def weights(key, rows, columns):
        return jax.random.normal(key, (rows, columns), jnp.float32) * rows**-0.5

    drawn = {
        "x": jax.random.normal(jax.random.fold_in(kx, part), (ROWS, D), jnp.float32),
        "gain": 1 + 0.1 * jax.random.normal(kn, (D,), jnp.float32),
        "wq": 2 * weights(kq, D, HEADS * HEAD),
        "wk": 2 * weights(kk, D, KV_HEADS * HEAD),
        "wv": 4 * weights(kv, D, KV_HEADS * HEAD),
        "wo": weights(ko, HEADS * HEAD, D),
    }
    return {k: v.astype(jnp.bfloat16) for k, v in drawn.items()}


def normed(x, gain):
    wide = x.astype(jnp.float32)
    scale = lax.rsqrt(jnp.mean(wide * wide, -1, keepdims=True) + 1e-6)
    return (wide * scale * gain.astype(jnp.float32)).astype(jnp.bfloat16)


def turned(t, place, theta):
    half = t.shape[-1] // 2
    angle = place.astype(jnp.float32)[:, None] * theta ** (-jnp.arange(half, dtype=jnp.float32) / half)
    cos, sin = jnp.cos(angle)[:, None], jnp.sin(angle)[:, None]
    a, b = t[..., :half].astype(jnp.float32), t[..., half:].astype(jnp.float32)
    return jnp.concatenate([a * cos - b * sin, b * cos + a * sin], -1).astype(jnp.bfloat16)


def matmul(a, w):
    return jnp.dot(a, w, preferred_element_type=jnp.float32).astype(jnp.bfloat16)


def einsum(form, a, b):
    return jnp.einsum(form, a.astype(jnp.float32), b.astype(jnp.float32))


def attention(q, k, v):
    scores = einsum("tgsd,ugd->gstu", q, k) * q.shape[-1] ** -0.5
    token = jnp.arange(q.shape[0])
    scores = jnp.where(token[:, None] >= token, scores, -jnp.inf)
    weights = jax.nn.softmax(scores, -1).astype(jnp.bfloat16)
    return einsum("gstu,ugd->tgsd", weights, v).astype(jnp.bfloat16)


def reference(x, gain, wq, wk, wv, wo):
    a, place = normed(x, gain), jnp.arange(ROWS)
    q = turned(matmul(a, wq).reshape(ROWS, HEADS, HEAD), place, THETA).reshape(ROWS, KV_HEADS, -1, HEAD)
    k = turned(matmul(a, wk).reshape(ROWS, KV_HEADS, HEAD), place, THETA)
    v = matmul(a, wv).reshape(ROWS, KV_HEADS, HEAD)
    seen = attention(q, k, v).reshape(ROWS, HEADS * HEAD)
    return (x.astype(jnp.float32) + jnp.dot(seen, wo, preferred_element_type=jnp.float32)).astype(jnp.bfloat16)
```

```python
import functools

import jax
import jax.numpy as jnp
import numpy as np
from jax import lax
from jax.experimental import pallas as pl
from jax.experimental.pallas import tpu as pltpu
from jax.sharding import PartitionSpec as P

HEAD = 256
THETA = 10000
NEG = -1e30
LOG2E = 1.4426950408889634
FINE = 32
MESH = pl.DeviceIdType.MESH
BF, F32 = jnp.bfloat16, jnp.float32

TASKS = [
    [(1, 0), (1, 1), (0, 0), (0, 1)],
    [(1, 4), (1, 5), (1, 2), (1, 3), (1, 6), (1, 7), (0, 2), (0, 3)],
    [(1, 4), (1, 5), (0, 6), (0, 7), (0, 4), (0, 5)],
    [(0, 6), (0, 7), (1, 6), (1, 7)],
]
FIRST = [[0, 0], [0, 0], [0, 4], [6, 4]]
WAITS = [[0] * 4, [1, 0, 0, 0, 0, 0, 1, 0], [0, 0, 3, 0, 0, 0], [0, 0, 4, 0]]


def _dot(a, b, ca, cb):
    return lax.dot_general(a, b, (((ca,), (cb,)), ((), ())), preferred_element_type=F32)


def _pick(z, i, table):
    out = jnp.int32(0)
    for zz, row in enumerate(table):
        got = jnp.int32(0)
        for ii, value in enumerate(row):
            got = jnp.where(i == ii, jnp.int32(value), got)
        out = jnp.where(z == zz, got, out)
    return out


def kernel(x_hbm, gain_ref, coarse_ref, fine_ref, wq_hbm, wk_hbm, wv_hbm, wo_hbm, y_hbm,
           xb, ab, wqb, wkb, wvb, wob, kb, vb, qb, ob, ls, top_s, mix_s, of, yacc, cs,
           wsem, asend, arecv, ksend, vsend, krecv, vrecv, qsend, qrecv, osend, lsend, orecv, lrecv):
    dp, sp = lax.axis_index("dp"), lax.axis_index("sp")
    z, c = sp // 2, sp % 2
    n, wide = xb.shape
    rows = n // 4
    scale = HEAD**-0.5
    e = scale * LOG2E

    def device(s):
        return (dp, s)

    barrier = pltpu.get_barrier_semaphore()
    for step in range(1, 8):
        pl.semaphore_signal(barrier, 1, device_id=device((sp + step) % 8), device_id_type=MESH)

    def x_copy(i):
        at = pl.ds(i * rows, rows)
        return pltpu.make_async_copy(x_hbm.at[at], xb.at[at], wsem.at[i])

    def w_copy(hbm, buf, g, width, sem):
        at = pl.ds(pl.multiple_of((c * 2 + g) * width, width), width)
        return pltpu.make_async_copy(hbm.at[:, at], buf.at[g], sem)

    wk_copy = lambda g: w_copy(wk_hbm, wkb, g, HEAD, wsem.at[4 + g])
    wv_copy = lambda g: w_copy(wv_hbm, wvb, g, HEAD, wsem.at[6 + g])
    wq_copy = lambda g: w_copy(wq_hbm, wqb, g, 2 * HEAD, wsem.at[8 + g])
    wo_copy = pltpu.make_async_copy(wo_hbm, wob, wsem.at[10])
    g_first = jnp.where(z == 0, 1, 0)

    for i in range(4):
        x_copy(i).start()
    wk_copy(g_first).start()
    wv_copy(g_first).start()

    for l in range(2):
        for g in range(2):
            @pl.when((z < 2) | ((z == 2) & (g == 0)))
            def _():
                ob[12 + l * 2 + g] = jnp.zeros(ob.shape[1:], BF)
                ls[12 + l * 2 + g] = jnp.full(ls.shape[1:], NEG, F32)

    count = 2 * n // FINE
    fc, fs = fine_ref[0], fine_ref[1]

    def turn_table(i, _):
        cc = coarse_ref[0, pl.ds(z * count + i, 1), :]
        ss = coarse_ref[1, pl.ds(z * count + i, 1), :]
        at = pl.ds(pl.multiple_of(i * FINE, FINE), FINE)
        cs[0, at, :] = cc * fc - ss * fs
        cs[1, at, :] = ss * fc + cc * fs

    lax.fori_loop(0, count, turn_table, None)

    def a_copy(i):
        at = pl.ds(i * rows, rows)
        return pltpu.make_async_remote_copy(ab.at[c, at], ab.at[c, at], asend.at[i], arecv.at[i], device_id=device(z * 2 + 1 - c), device_id_type=MESH)

    gain = gain_ref[...].astype(F32)
    for i in range(4):
        x_copy(i).wait()
        at = pl.ds(i * rows, rows)
        w = xb[at, :].astype(F32)
        yacc[at, :] = w
        ab[c, at, :] = (w * lax.rsqrt(jnp.mean(w * w, -1, keepdims=True) + 1e-6) * gain).astype(BF)
        if i == 0:
            pl.semaphore_wait(barrier, 7)
        a_copy(i).start()
    wk_copy(1 - g_first).start()
    wv_copy(1 - g_first).start()
    wq_copy(1).start()
    wq_copy(0).start()

    def kv_copies(g, h, to, way):
        j = 2 * z + h
        return [pltpu.make_async_remote_copy(buf.at[g, j], buf.at[g, j], send.at[g, h, way], recv.at[g, j], device_id=device(2 * to + c), device_id_type=MESH)
                for buf, send, recv in ((kb, ksend, krecv), (vb, vsend, vrecv))]

    def q_copy(g, h, to):
        j = 2 * z + h
        return pltpu.make_async_remote_copy(qb.at[g, j], qb.at[g, j], qsend.at[g, h], qrecv.at[g, j], device_id=device(2 * to + c), device_id_type=MESH)

    def start(copies):
        for copy in copies:
            copy.start()

    def turned(t, h):
        at = pl.ds(pl.multiple_of(h * n, n), n)
        cos, sin = cs[0, at, :], cs[1, at, :]
        t = t.astype(BF).astype(F32)
        a, b = t[:, : HEAD // 2], t[:, HEAD // 2 :]
        return jnp.concatenate([a * cos - b * sin, b * cos + a * sin], -1).astype(BF)

    def project(hh, _):
        h = jnp.where(hh == 0, c, 1 - c)

        @pl.when(hh == 1)
        def _():
            for i in range(4):
                a_other = pltpu.make_async_remote_copy(ab.at[1 - c, pl.ds(i * rows, rows)], ab.at[1 - c, pl.ds(i * rows, rows)], asend.at[i], arecv.at[i],
                                                       device_id=device(z * 2 + 1 - c), device_id_type=MESH)
                a_other.wait_recv()

        def keys(gi, _):
            g = jnp.where(gi == 0, g_first, 1 - g_first)

            @pl.when(hh == 0)
            def _():
                wk_copy(g).wait()
                wv_copy(g).wait()

            kb[g, 2 * z + h] = turned(_dot(ab[h], wkb[g], 1, 0), h)
            vb[g, 2 * z + h] = _dot(ab[h], wvb[g], 1, 0).astype(BF).T

            @pl.when((z == 1) & (g == 0))
            def _():
                start(kv_copies(0, h, 2, 0))

            @pl.when((z == 2) & (g == 1))
            def _():
                start(kv_copies(1, h, 3, 0))

            @pl.when((z == 0) & (gi == 0))
            def _():
                start(kv_copies(1, h, 1, 0))

            @pl.when((z == 0) & (hh == 1))
            def _():
                @pl.when(gi == 0)
                def _():
                    start(kv_copies(0, c, 2, 1))

                @pl.when(gi == 1)
                def _():
                    start(kv_copies(0, 1 - c, 2, 1))
                    start(kv_copies(0, c, 1, 0))
                    start(kv_copies(0, 1 - c, 1, 0))

        lax.fori_loop(0, 2, keys, None)

        def queries(gi, _):
            g = 1 - gi

            @pl.when(hh == 0)
            def _():
                wq_copy(g).wait()

            q = _dot(ab[h], wqb[g], 1, 0)
            for s in range(2):
                qb[g, 2 * z + h, s] = turned(q[:, s * HEAD : (s + 1) * HEAD], h)

            @pl.when((z >= 2) & (g == 1))
            def _():
                q_copy(1, h, 1).start()

            @pl.when((z == 3) & (g == 0))
            def _():
                q_copy(0, h, 2).start()

        lax.fori_loop(0, 2, queries, None)

    lax.fori_loop(0, 2, project, None)
    wo_copy.start()

    ones = jnp.ones((8, n), BF)

    def task(t, _):
        code = _pick(z, t, [[g * 8 + q for g, q in row] for row in TASKS])
        g, q = code // 8, code % 8
        local = q // 2 == z
        first = _pick(z, g, FIRST)
        waits = _pick(z, t, WAITS)
        for o in range(3):
            @pl.when((waits // 2**o) % 2 == 1)
            def _():
                for h in range(2):
                    j = 2 * o + h
                    for buf, send, recv in ((kb, ksend, krecv), (vb, vsend, vrecv)):
                        pltpu.make_async_remote_copy(buf.at[g, j], buf.at[g, j], send.at[0, 0, 0], recv.at[g, j], device_id=device(sp), device_id_type=MESH).wait_recv()

        @pl.when(jnp.logical_not(local))
        def _():
            pltpu.make_async_remote_copy(qb.at[g, q], qb.at[g, q], qsend.at[0, 0], qrecv.at[g, q], device_id=device(sp), device_id_type=MESH).wait_recv()

        top_s[...] = jnp.full(top_s.shape, NEG, F32)
        mix_s[...] = jnp.zeros(mix_s.shape, F32)

        def block(j, masked):
            scores = [_dot(kb[g, j], qb[g, q, s], 1, 1) for s in range(2)]
            weights, keeps = [], []
            for s in range(2):
                score = scores[s]
                if masked:
                    ok = lax.broadcasted_iota(jnp.int32, (n, n), 0) <= lax.broadcasted_iota(jnp.int32, (n, n), 1)
                    score = jnp.where(ok, score, 2 * NEG)
                old = top_s[s : s + 1, :]
                top = jnp.maximum(old, score.max(axis=0, keepdims=True))
                top_s[s : s + 1, :] = top
                weights.append(jnp.exp2((score - top) * e).astype(BF))
                keeps.append(jnp.exp2((old - top) * e))
            values = jnp.concatenate([vb[g, j], ones], axis=0)
            for s in range(2):
                mix_s[s] = mix_s[s] * keeps[s] + _dot(values, weights[s], 1, 0)

        lax.fori_loop(first, jnp.minimum(q, 2 * z + 2), lambda j, _: block(j, False), None)

        @pl.when(local)
        def _():
            block(q, True)

        slot = 8 + jnp.where(local, 0, 4) + c * 2 + g
        here = jnp.where(q == sp, slot, t)
        for s in range(2):
            total = mix_s[s, HEAD : HEAD + 1, :]
            ob[here, s] = (mix_s[s, :HEAD, :] * (1 / total)).astype(BF)
            lse = top_s[s : s + 1, :] * e + jnp.log2(total)
            per = n // 128
            for i in range(per):
                ls[here, s * per + i : s * per + i + 1, :] = lse[:, i * 128 : (i + 1) * 128]

        @pl.when(q != sp)
        def _():
            start(o_copies(t, slot, q))

    def o_copies(t, slot, owner):
        return [pltpu.make_async_remote_copy(buf.at[t], buf.at[slot], send.at[t], recv.at[slot - 8], device_id=device(owner), device_id_type=MESH)
                for buf, send, recv in ((ob, osend, orecv), (ls, lsend, lrecv))]

    tasks = jnp.where(z == 1, 8, jnp.where(z == 2, 6, 4))
    lax.fori_loop(0, tasks, task, None)

    wo_copy.wait()

    def finish(i, _):
        g = i // 2
        l = (c + i) % 2
        base = l * 2 + g

        @pl.when(l != c)
        def _():
            for copy in o_copies(0, 8 + base, sp):
                copy.wait_recv()

        @pl.when((z == 3) | ((z == 2) & (g == 1)))
        def _():
            for copy in o_copies(0, 12 + base, sp):
                copy.wait_recv()

        per = n // 128
        for s in range(2):
            la, lb = (jnp.concatenate([ls[at + base, s * per + k : s * per + k + 1, :] for k in range(per)], axis=1) for at in (8, 12))
            m = jnp.maximum(la, lb)
            wa, wb = jnp.exp2(la - m), jnp.exp2(lb - m)
            r = 1 / (wa + wb)
            o = ob[8 + base, s].astype(F32) * (wa * r) + ob[12 + base, s].astype(F32) * (wb * r)
            of[:, s * HEAD : (s + 1) * HEAD] = o.T.astype(BF)
        at = pl.ds(pl.multiple_of((l * 4 + g * 2) * HEAD, HEAD), 2 * HEAD)

        def columns(k, _):
            cols = pl.ds(pl.multiple_of(k * HEAD, HEAD), HEAD)
            yacc[:, cols] += _dot(of[...], wob[at, cols], 1, 0)

        lax.fori_loop(0, wide // HEAD, columns, None)

    lax.fori_loop(0, 4, finish, None)
    xb[...] = yacc[...].astype(BF)
    out = pltpu.make_async_copy(xb, y_hbm, wsem.at[11])
    out.start()

    for i in range(4):
        a_copy(i).wait_send()

    def sent(copies):
        for copy in copies:
            copy.wait_send()

    for h in range(2):
        @pl.when(z == 0)
        def _():
            sent(kv_copies(1, h, 1, 0))
            sent(kv_copies(0, h, 2, 1))
            sent(kv_copies(0, h, 1, 0))

        @pl.when(z == 1)
        def _():
            sent(kv_copies(0, h, 2, 0))

        @pl.when(z == 2)
        def _():
            sent(kv_copies(1, h, 3, 0))

        @pl.when(z >= 2)
        def _():
            q_copy(1, h, 1).wait_send()

        @pl.when(z == 3)
        def _():
            q_copy(0, h, 2).wait_send()

    def drain(t, _):
        q = _pick(z, t, [[q for _, q in row] for row in TASKS])

        @pl.when(q != sp)
        def _():
            sent(o_copies(t, 8, q))

    lax.fori_loop(0, tasks, drain, None)
    out.wait()


def solution(mesh):
    def step(x, gain, wq, wk, wv, wo):
        n, wide = x.shape
        half = HEAD // 2
        rate = np.float64(THETA) ** (-np.arange(half) / half)
        table = lambda places: jnp.asarray(np.stack([f(places[:, None] * rate) for f in (np.cos, np.sin)]).astype(np.float32))
        coarse, fine = table(np.arange(8 * n // FINE) * FINE), table(np.arange(FINE))
        hbm, vmem = pl.BlockSpec(memory_space=pl.ANY), pl.BlockSpec(memory_space=pltpu.VMEM)
        dma = pltpu.SemaphoreType.DMA
        return pl.pallas_call(
            kernel,
            out_shape=jax.ShapeDtypeStruct((n, wide), BF),
            in_specs=[hbm, vmem, vmem, vmem, hbm, hbm, hbm, hbm],
            out_specs=hbm,
            scratch_shapes=[
                pltpu.VMEM((n, wide), BF),
                pltpu.VMEM((2, n, wide), BF),
                pltpu.VMEM((2, wide, 2 * HEAD), BF),
                pltpu.VMEM((2, wide, HEAD), BF),
                pltpu.VMEM((2, wide, HEAD), BF),
                pltpu.VMEM((8 * HEAD, wide), BF),
                pltpu.VMEM((2, 8, n, HEAD), BF),
                pltpu.VMEM((2, 8, HEAD, n), BF),
                pltpu.VMEM((2, 8, 2, n, HEAD), BF),
                pltpu.VMEM((16, 2, HEAD, n), BF),
                pltpu.VMEM((16, 8, 128), F32),
                pltpu.VMEM((8, n), F32),
                pltpu.VMEM((2, HEAD + 8, n), F32),
                pltpu.VMEM((n, 2 * HEAD), BF),
                pltpu.VMEM((n, wide), F32),
                pltpu.VMEM((2, 2 * n, half), F32),
                dma((12,)), dma((4,)), dma((4,)),
                dma((2, 2, 2)), dma((2, 2, 2)), dma((2, 8)), dma((2, 8)),
                dma((2, 2)), dma((2, 8)),
                dma((8,)), dma((8,)), dma((8,)), dma((8,)),
            ],
            compiler_params=pltpu.CompilerParams(collective_id=0, has_side_effects=True, vmem_limit_bytes=67043328),
        )(x, gain.reshape(1, wide), coarse, fine, wq, wk, wv, wo)

    tokens, whole = P(("dp", "sp"), None), P(None, None)
    return jax.shard_map(
        step,
        mesh=mesh,
        in_specs=(tokens, P(None), whole, whole, whole, whole),
        out_specs=tokens,
        check_vma=False,
    )
```

```python
import functools

import jax
import jax.numpy as jnp
import numpy as np
from jax import lax
from jax.experimental import pallas as pl
from jax.experimental.pallas import tpu as pltpu
from jax.sharding import PartitionSpec as P

HEAD = 256
THETA = 10000
NEG = -1e30
LOG2E = 1.4426950408889634
FINE = 32
MESH = pl.DeviceIdType.MESH
BF, F32 = jnp.bfloat16, jnp.float32

TASKS = [
    [(1, 0), (1, 1), (0, 0), (0, 1)],
    [(1, 6), (1, 7), (1, 2), (1, 3), (1, 4), (1, 5), (0, 2), (0, 3)],
    [(1, 4), (1, 5), (0, 6), (0, 7), (0, 4), (0, 5)],
    [(0, 6), (0, 7), (1, 6), (1, 7)],
]
FIRST = [[0, 0], [0, 0], [0, 4], [6, 4]]
WAITS = [[0] * 4, [1, 0, 0, 0, 0, 0, 1, 0], [0, 0, 3, 0, 0, 0], [0, 0, 4, 0]]


def _dot(a, b, ca, cb):
    return lax.dot_general(a, b, (((ca,), (cb,)), ((), ())), preferred_element_type=F32)


def _pick(z, i, table):
    out = jnp.int32(0)
    for zz, row in enumerate(table):
        got = jnp.int32(0)
        for ii, value in enumerate(row):
            got = jnp.where(i == ii, jnp.int32(value), got)
        out = jnp.where(z == zz, got, out)
    return out


def kernel(x_hbm, gain_ref, coarse_ref, fine_ref, wq_hbm, wk_hbm, wv_hbm, wo_hbm, y_ref,
           xb, ab, wqb, wkb, wvb, wob, kb, vb, qb, ob, ls, top_s, mix_s, of, yacc, cs,
           wsem, asend, arecv, ksend, vsend, krecv, vrecv, qsend, qrecv, osend, lsend, orecv, lrecv, go):
    dp, sp = lax.axis_index("dp"), lax.axis_index("sp")
    z, c = sp // 2, sp % 2
    n, wide = xb.shape
    rows = n // 4
    scale = HEAD**-0.5
    e = scale * LOG2E

    def device(s):
        return (dp, s)

    barrier = pltpu.get_barrier_semaphore()
    for step in range(1, 8):
        pl.semaphore_signal(barrier, 1, device_id=device((sp + step) % 8), device_id_type=MESH)

    def x_copy(i):
        at = pl.ds(i * rows, rows)
        return pltpu.make_async_copy(x_hbm.at[at], xb.at[at], wsem.at[i])

    def w_copy(hbm, buf, g, width, sem):
        at = pl.ds(pl.multiple_of((c * 2 + g) * width, width), width)
        return pltpu.make_async_copy(hbm.at[:, at], buf.at[g], sem)

    wk_copy = lambda g: w_copy(wk_hbm, wkb, g, HEAD, wsem.at[4 + g])
    wv_copy = lambda g: w_copy(wv_hbm, wvb, g, HEAD, wsem.at[6 + g])
    wq_copy = lambda g: w_copy(wq_hbm, wqb, g, 2 * HEAD, wsem.at[8 + g])
    wo_copy = pltpu.make_async_copy(wo_hbm, wob, wsem.at[10])
    g_first = jnp.where(z == 0, 1, 0)

    for i in range(4):
        x_copy(i).start()
    wk_copy(g_first).start()
    wv_copy(g_first).start()

    for l in range(2):
        for g in range(2):
            @pl.when((z < 2) | ((z == 2) & (g == 0)))
            def _():
                ob[12 + l * 2 + g] = jnp.zeros(ob.shape[1:], BF)
                ls[12 + l * 2 + g] = jnp.full(ls.shape[1:], NEG, F32)

    count = 2 * n // FINE
    fc, fs = fine_ref[0], fine_ref[1]

    def turn_table(i, _):
        cc = coarse_ref[0, pl.ds(z * count + i, 1), :]
        ss = coarse_ref[1, pl.ds(z * count + i, 1), :]
        at = pl.ds(pl.multiple_of(i * FINE, FINE), FINE)
        cs[0, at, :] = cc * fc - ss * fs
        cs[1, at, :] = ss * fc + cc * fs

    lax.fori_loop(0, count, turn_table, None)

    def a_copy(i):
        at = pl.ds(i * rows, rows)
        return pltpu.make_async_remote_copy(ab.at[c, at], ab.at[c, at], asend.at[i], arecv.at[i], device_id=device(z * 2 + 1 - c), device_id_type=MESH)

    gain = gain_ref[...].astype(F32)[None, :]
    for i in range(4):
        x_copy(i).wait()
        at = pl.ds(i * rows, rows)
        w = xb[at, :].astype(F32)
        yacc[at, :] = w
        ab[c, at, :] = (w * lax.rsqrt(jnp.mean(w * w, -1, keepdims=True) + 1e-6) * gain).astype(BF)
        if i == 0:
            pl.semaphore_wait(barrier, 7)
        a_copy(i).start()
    wk_copy(1 - g_first).start()
    wv_copy(1 - g_first).start()
    wq_copy(1).start()
    wq_copy(0).start()

    def kv_copies(g, h, to, way):
        j = 2 * z + h
        return [pltpu.make_async_remote_copy(buf.at[g, j], buf.at[g, j], send.at[g, h, way], recv.at[g, j], device_id=device(2 * to + c), device_id_type=MESH)
                for buf, send, recv in ((kb, ksend, krecv), (vb, vsend, vrecv))]

    def q_copy(g, h, to):
        j = 2 * z + h
        return pltpu.make_async_remote_copy(qb.at[g, j], qb.at[g, j], qsend.at[g, h], qrecv.at[g, j], device_id=device(2 * to + c), device_id_type=MESH)

    def start(copies):
        for copy in copies:
            copy.start()

    def turned(t, h):
        at = pl.ds(pl.multiple_of(h * n, n), n)
        cos, sin = cs[0, at, :], cs[1, at, :]
        t = t.astype(BF).astype(F32)
        a, b = t[:, : HEAD // 2], t[:, HEAD // 2 :]
        return jnp.concatenate([a * cos - b * sin, b * cos + a * sin], -1).astype(BF)

    def project(hh, _):
        h = jnp.where(hh == 0, c, 1 - c)

        @pl.when(hh == 1)
        def _():
            for i in range(4):
                a_other = pltpu.make_async_remote_copy(ab.at[1 - c, pl.ds(i * rows, rows)], ab.at[1 - c, pl.ds(i * rows, rows)], asend.at[i], arecv.at[i],
                                                       device_id=device(z * 2 + 1 - c), device_id_type=MESH)
                a_other.wait_recv()

        def keys(gi, _):
            g = jnp.where(gi == 0, g_first, 1 - g_first)

            @pl.when(hh == 0)
            def _():
                wk_copy(g).wait()
                wv_copy(g).wait()

            kb[g, 2 * z + h] = turned(_dot(ab[h], wkb[g], 1, 0), h)
            vb[g, 2 * z + h] = _dot(ab[h], wvb[g], 1, 0).astype(BF).T

            @pl.when((z == 1) & (g == 0))
            def _():
                start(kv_copies(0, h, 2, 0))

            @pl.when((z == 2) & (g == 1))
            def _():
                start(kv_copies(1, h, 3, 0))

            @pl.when((z == 0) & (gi == 0))
            def _():
                start(kv_copies(1, h, 1, 0))

            @pl.when((z == 0) & (hh == 1))
            def _():
                @pl.when(gi == 0)
                def _():
                    start(kv_copies(0, c, 2, 1))

                @pl.when(gi == 1)
                def _():
                    start(kv_copies(0, 1 - c, 2, 1))
                    start(kv_copies(0, c, 1, 0))
                    start(kv_copies(0, 1 - c, 1, 0))

        lax.fori_loop(0, 2, keys, None)

        def queries(gi, _):
            g = 1 - gi

            @pl.when(hh == 0)
            def _():
                wq_copy(g).wait()

            q = _dot(ab[h], wqb[g], 1, 0)
            for s in range(2):
                qb[g, 2 * z + h, s] = turned(q[:, s * HEAD : (s + 1) * HEAD], h)

            @pl.when((z == 3) & (g == 1))
            def _():
                q_copy(1, h, 1).start()

            @pl.when((z == 3) & (hh == 1) & (g == 0))
            def _():
                q_copy(0, c, 2).start()
                q_copy(0, 1 - c, 2).start()

        lax.fori_loop(0, 2, queries, None)

    lax.fori_loop(0, 2, project, None)
    wo_copy.start()

    ones = jnp.ones((8, n), BF)

    def task(t, _):
        code = _pick(z, t, [[g * 8 + q for g, q in row] for row in TASKS])
        g, q = code // 8, code % 8
        local = q // 2 == z
        first = _pick(z, g, FIRST)
        waits = _pick(z, t, WAITS)
        def q_wait(qq):
            pltpu.make_async_remote_copy(qb.at[g, qq], qb.at[g, qq], qsend.at[0, 0], qrecv.at[g, qq], device_id=device(sp), device_id_type=MESH).wait_recv()

        @pl.when((z == 1) & (t == 0))
        def _():
            q_wait(6)
            q_wait(7)
            pl.semaphore_signal(go, 1, device_id=device(sp + 2), device_id_type=MESH)

        @pl.when(jnp.logical_not(local) & ((z == 2) | (q < 6)))
        def _():
            q_wait(q)

        @pl.when((z == 2) & (t == 2))
        def _():
            pl.semaphore_wait(go, 1)
            q_copy(1, c, 1).start()
            q_copy(1, 1 - c, 1).start()

        for o in range(3):
            @pl.when((waits // 2**o) % 2 == 1)
            def _():
                for h in range(2):
                    j = 2 * o + h
                    for buf, send, recv in ((kb, ksend, krecv), (vb, vsend, vrecv)):
                        pltpu.make_async_remote_copy(buf.at[g, j], buf.at[g, j], send.at[0, 0, 0], recv.at[g, j], device_id=device(sp), device_id_type=MESH).wait_recv()

        top_s[...] = jnp.full(top_s.shape, NEG, F32)
        mix_s[...] = jnp.zeros(mix_s.shape, F32)

        def block(j, masked):
            scores = [_dot(kb[g, j], qb[g, q, s], 1, 1) for s in range(2)]
            weights, keeps = [], []
            for s in range(2):
                score = scores[s]
                if masked:
                    ok = lax.broadcasted_iota(jnp.int32, (n, n), 0) <= lax.broadcasted_iota(jnp.int32, (n, n), 1)
                    score = jnp.where(ok, score, 2 * NEG)
                old = top_s[s : s + 1, :]
                top = jnp.maximum(old, score.max(axis=0, keepdims=True))
                top_s[s : s + 1, :] = top
                weights.append(jnp.exp2((score - top) * e).astype(BF))
                keeps.append(jnp.exp2((old - top) * e))
            values = jnp.concatenate([vb[g, j], ones], axis=0)
            for s in range(2):
                mix_s[s] = mix_s[s] * keeps[s] + _dot(values, weights[s], 1, 0)

        lax.fori_loop(first, jnp.minimum(q, 2 * z + 2), lambda j, _: block(j, False), None)

        @pl.when(local)
        def _():
            block(q, True)

        slot = 8 + jnp.where(local, 0, 4) + c * 2 + g
        here = jnp.where(q == sp, slot, t)
        for s in range(2):
            total = mix_s[s, HEAD : HEAD + 1, :]
            ob[here, s] = (mix_s[s, :HEAD, :] * (1 / total)).astype(BF)
            lse = top_s[s : s + 1, :] * e + jnp.log2(total)
            per = n // 128
            for i in range(per):
                ls[here, s * per + i : s * per + i + 1, :] = lse[:, i * 128 : (i + 1) * 128]

        @pl.when(q != sp)
        def _():
            start(o_copies(t, slot, q))

    def o_copies(t, slot, owner):
        return [pltpu.make_async_remote_copy(buf.at[t], buf.at[slot], send.at[t], recv.at[slot - 8], device_id=device(owner), device_id_type=MESH)
                for buf, send, recv in ((ob, osend, orecv), (ls, lsend, lrecv))]

    tasks = jnp.where(z == 1, 8, jnp.where(z == 2, 6, 4))
    lax.fori_loop(0, tasks, task, None)

    wo_copy.wait()

    def finish(i, _):
        g = jnp.where(z % 2 == 1, 1 - i // 2, i // 2)
        l = (c + i) % 2
        base = l * 2 + g

        @pl.when(l != c)
        def _():
            for copy in o_copies(0, 8 + base, sp):
                copy.wait_recv()

        @pl.when((z == 3) | ((z == 2) & (g == 1)))
        def _():
            for copy in o_copies(0, 12 + base, sp):
                copy.wait_recv()

        per = n // 128
        for s in range(2):
            la, lb = (jnp.concatenate([ls[at + base, s * per + k : s * per + k + 1, :] for k in range(per)], axis=1) for at in (8, 12))
            m = jnp.maximum(la, lb)
            wa, wb = jnp.exp2(la - m), jnp.exp2(lb - m)
            r = 1 / (wa + wb)
            o = ob[8 + base, s].astype(F32) * (wa * r) + ob[12 + base, s].astype(F32) * (wb * r)
            of[:, s * HEAD : (s + 1) * HEAD] = o.T.astype(BF)
        at = pl.ds(pl.multiple_of((l * 4 + g * 2) * HEAD, HEAD), 2 * HEAD)

        last = i == 3

        def columns(k, _):
            cols = pl.ds(pl.multiple_of(k * (wide // 3), 128), wide // 3)
            y = yacc[:, cols] + _dot(of[...], wob[at, cols], 1, 0)

            @pl.when(jnp.logical_not(last))
            def _():
                yacc[:, cols] = y

            @pl.when(last)
            def _():
                y_ref[:, cols] = y.astype(BF)

        lax.fori_loop(0, 3, columns, None)

    lax.fori_loop(0, 4, finish, None)

    for i in range(4):
        a_copy(i).wait_send()

    def sent(copies):
        for copy in copies:
            copy.wait_send()

    for h in range(2):
        @pl.when(z == 0)
        def _():
            sent(kv_copies(1, h, 1, 0))
            sent(kv_copies(0, h, 2, 1))
            sent(kv_copies(0, h, 1, 0))

        @pl.when(z == 1)
        def _():
            sent(kv_copies(0, h, 2, 0))

        @pl.when(z == 2)
        def _():
            sent(kv_copies(1, h, 3, 0))

        @pl.when(z >= 2)
        def _():
            q_copy(1, h, 1).wait_send()

        @pl.when(z == 3)
        def _():
            q_copy(0, h, 2).wait_send()

    def drain(t, _):
        q = _pick(z, t, [[q for _, q in row] for row in TASKS])

        @pl.when(q != sp)
        def _():
            sent(o_copies(t, 8, q))

    lax.fori_loop(0, tasks, drain, None)


def solution(mesh):
    def step(x, gain, wq, wk, wv, wo):
        n, wide = x.shape
        half = HEAD // 2
        rate = np.float64(THETA) ** (-np.arange(half) / half)
        table = lambda places: jnp.asarray(np.stack([f(places[:, None] * rate) for f in (np.cos, np.sin)]).astype(np.float32))
        coarse, fine = table(np.arange(8 * n // FINE) * FINE), table(np.arange(FINE))
        hbm, vmem = pl.BlockSpec(memory_space=pl.ANY), pl.BlockSpec(memory_space=pltpu.VMEM)
        dma = pltpu.SemaphoreType.DMA
        return pl.pallas_call(
            kernel,
            out_shape=jax.ShapeDtypeStruct((n, wide), BF),
            in_specs=[hbm, vmem, vmem, vmem, hbm, hbm, hbm, hbm],
            out_specs=vmem,
            scratch_shapes=[
                pltpu.VMEM((n, wide), BF),
                pltpu.VMEM((2, n, wide), BF),
                pltpu.VMEM((2, wide, 2 * HEAD), BF),
                pltpu.VMEM((2, wide, HEAD), BF),
                pltpu.VMEM((2, wide, HEAD), BF),
                pltpu.VMEM((8 * HEAD, wide), BF),
                pltpu.VMEM((2, 8, n, HEAD), BF),
                pltpu.VMEM((2, 8, HEAD, n), BF),
                pltpu.VMEM((2, 8, 2, n, HEAD), BF),
                pltpu.VMEM((16, 2, HEAD, n), BF),
                pltpu.VMEM((16, 8, 128), F32),
                pltpu.VMEM((8, n), F32),
                pltpu.VMEM((2, HEAD + 8, n), F32),
                pltpu.VMEM((n, 2 * HEAD), BF),
                pltpu.VMEM((n, wide), F32),
                pltpu.VMEM((2, 2 * n, half), F32),
                dma((11,)), dma((4,)), dma((4,)),
                dma((2, 2, 2)), dma((2, 2, 2)), dma((2, 8)), dma((2, 8)),
                dma((2, 2)), dma((2, 8)),
                dma((8,)), dma((8,)), dma((8,)), dma((8,)),
                pltpu.SemaphoreType.REGULAR,
            ],
            compiler_params=pltpu.CompilerParams(collective_id=0, has_side_effects=True, vmem_limit_bytes=67043328),
        )(x, gain, coarse, fine, wq, wk, wv, wo)

    tokens, whole = P(("dp", "sp"), None), P(None, None)
    return jax.shard_map(
        step,
        mesh=mesh,
        in_specs=(tokens, P(None), whole, whole, whole, whole),
        out_specs=tokens,
        check_vma=False,
    )
```

```python
import functools

import jax
import jax.numpy as jnp
import numpy as np
from jax import lax
from jax.experimental import pallas as pl
from jax.experimental.pallas import tpu as pltpu
from jax.sharding import PartitionSpec as P

HEAD = 256
THETA = 10000
NEG = -1e30
LOG2E = 1.4426950408889634
FINE = 32
MESH = pl.DeviceIdType.MESH
BF, F32 = jnp.bfloat16, jnp.float32

FIRST = [[0, 0], [0, 0], [0, 4], [6, 4]]
STAGED = [2, 6, 4, 2]


def plan(z, c):
    steps, staged = [], 0

    def attention(g, a, b, waits=0):
        nonlocal staged
        for q in (a, b) if c == 0 else (b, a):
            steps.append(2 * g + 4 * q + 32 * staged + 256 * waits)
            waits = 0
            staged += q != 2 * z + c

    def output(g):
        steps.extend(1 + 2 * g + 4 * (2 * l + s) for l in range(2) for s in range(2))

    if z == 0:
        attention(1, 0, 1), attention(0, 0, 1), output(1), output(0)
    elif z == 1:
        attention(1, 6, 7, 1), attention(1, 2, 3), attention(1, 4, 5), output(1), attention(0, 2, 3, 1), output(0)
    elif z == 2:
        attention(1, 4, 5), attention(0, 6, 7, 3), attention(0, 4, 5), output(0), output(1)
    else:
        attention(0, 6, 7), attention(1, 6, 7, 4), output(1), output(0)
    return steps


PLAN = [plan(z, c) for z in range(4) for c in range(2)]


def _dot(a, b, ca, cb):
    return lax.dot_general(a, b, (((ca,), (cb,)), ((), ())), preferred_element_type=F32)


def _pick(z, i, table):
    out = jnp.int32(0)
    for zz, row in enumerate(table):
        got = jnp.int32(0)
        for ii, value in enumerate(row):
            got = jnp.where(i == ii, jnp.int32(value), got)
        out = jnp.where(z == zz, got, out)
    return out


def kernel(x_hbm, gain_hbm, coarse_hbm, fine_hbm, wq_hbm, wk_hbm, wv_hbm, wo_hbm, y_ref,
           xb, gainb, coarse_ref, fine_ref, ab, wqb, wkb, wvb, wob, kb, vb, qb, ob, ls, top_s, mix_s, of, yacc, cs,
           wsem, asend, arecv, ksend, vsend, krecv, vrecv, qsend, qrecv, osend, lsend, orecv, lrecv, go):
    dp, sp = lax.axis_index("dp"), lax.axis_index("sp")
    z, c = sp // 2, sp % 2
    n, wide = xb.shape
    rows = n // 4
    scale = HEAD**-0.5
    e = scale * LOG2E

    def device(s):
        return (dp, s)

    def x_copy(i):
        at = pl.ds(i * rows, rows)
        return pltpu.make_async_copy(x_hbm.at[at], xb.at[at], wsem.at[i])

    def w_copy(hbm, buf, g, width, sem):
        at = pl.ds(pl.multiple_of((c * 2 + g) * width, width), width)
        return pltpu.make_async_copy(hbm.at[:, at], buf.at[g], sem)

    wk_copy = lambda g: w_copy(wk_hbm, wkb, g, HEAD, wsem.at[4 + g])
    wv_copy = lambda g: w_copy(wv_hbm, wvb, g, HEAD, wsem.at[6 + g])
    wq_copy = lambda g: w_copy(wq_hbm, wqb, g, 2 * HEAD, wsem.at[8 + g])
    wo_copy = pltpu.make_async_copy(wo_hbm, wob, wsem.at[10])
    g_first = jnp.where(z == 0, 1, 0)

    count = 2 * n // FINE
    tables = [pltpu.make_async_copy(gain_hbm, gainb, wsem.at[11]), pltpu.make_async_copy(fine_hbm, fine_ref, wsem.at[12]),
              pltpu.make_async_copy(coarse_hbm.at[:, pl.ds(pl.multiple_of(z * count, 8), count)], coarse_ref, wsem.at[13])]

    for copy in tables[1:]:
        copy.start()
    for i in range(4):
        x_copy(i).start()
    tables[0].start()
    wk_copy(g_first).start()
    wv_copy(g_first).start()

    barrier = pltpu.get_barrier_semaphore()
    for step in range(1, 8):
        pl.semaphore_signal(barrier, 1, device_id=device((sp + step) % 8), device_id_type=MESH)

    for copy in tables[1:]:
        copy.wait()
    fc, fs = fine_ref[0], fine_ref[1]

    def turn_table(i, _):
        cc = coarse_ref[0, pl.ds(i, 1), :]
        ss = coarse_ref[1, pl.ds(i, 1), :]
        at = pl.ds(pl.multiple_of(i * FINE, FINE), FINE)
        cs[0, at, :] = cc * fc - ss * fs
        cs[1, at, :] = ss * fc + cc * fs

    lax.fori_loop(0, count, turn_table, None)

    def a_copy(cc):
        return pltpu.make_async_remote_copy(ab.at[cc], ab.at[cc], asend.at[0], arecv.at[0], device_id=device(z * 2 + 1 - c), device_id_type=MESH)

    tables[0].wait()
    gain = gainb[...].astype(F32)[None, :]
    for i in range(4):
        x_copy(i).wait()
        at = pl.ds(i * rows, rows)
        w = xb[at, :].astype(F32)
        yacc[at, :] = w
        ab[c, at, :] = (w * lax.rsqrt(jnp.mean(w * w, -1, keepdims=True) + 1e-6) * gain).astype(BF)
    pl.semaphore_wait(barrier, 7)
    a_copy(c).start()
    wk_copy(1 - g_first).start()
    wv_copy(1 - g_first).start()
    wq_copy(1).start()
    wq_copy(0).start()

    def kv_copies(g, h, to, way, which=(0, 1)):
        j = 2 * z + h
        pairs = ((kb, ksend, krecv), (vb, vsend, vrecv))
        return [pltpu.make_async_remote_copy(buf.at[g, j], buf.at[g, j], send.at[g, h, way], recv.at[g, j], device_id=device(2 * to + c), device_id_type=MESH)
                for buf, send, recv in (pairs[i] for i in which)]

    def q_copy(g, h, to):
        j = 2 * z + h
        return pltpu.make_async_remote_copy(qb.at[g, j], qb.at[g, j], qsend.at[g, h], qrecv.at[g, j], device_id=device(2 * to + c), device_id_type=MESH)

    def start(copies):
        for copy in copies:
            copy.start()

    def turned(t, h):
        at = pl.ds(pl.multiple_of(h * n, n), n)
        cos, sin = cs[0, at, :], cs[1, at, :]
        t = t.astype(BF).astype(F32)
        a, b = t[:, : HEAD // 2], t[:, HEAD // 2 :]
        return jnp.concatenate([a * cos - b * sin, b * cos + a * sin], -1).astype(BF)

    def project(hh, _):
        h = jnp.where(hh == 0, c, 1 - c)

        @pl.when(hh == 1)
        def _():
            a_copy(1 - c).wait_recv()
            wo_copy.start()

        def keys(gi, _):
            g = jnp.where(gi == 0, g_first, 1 - g_first)

            @pl.when(hh == 0)
            def _():
                wk_copy(g).wait()
                wv_copy(g).wait()

            def first_sends(which):
                @pl.when((z == 1) & (g == 0))
                def _():
                    start(kv_copies(0, h, 2, 0, which))

                @pl.when((z == 2) & (g == 1))
                def _():
                    start(kv_copies(1, h, 3, 0, which))

                @pl.when((z == 0) & (gi == 0))
                def _():
                    start(kv_copies(1, h, 1, 0, which))

            kb[g, 2 * z + h] = turned(_dot(ab[h], wkb[g], 1, 0), h)
            first_sends((0,))
            vb[g, 2 * z + h] = _dot(ab[h], wvb[g], 1, 0).astype(BF).T
            first_sends((1,))

            @pl.when((z == 0) & (hh == 1))
            def _():
                @pl.when(gi == 0)
                def _():
                    start(kv_copies(0, c, 2, 1))

                @pl.when(gi == 1)
                def _():
                    start(kv_copies(0, 1 - c, 2, 1))
                    start(kv_copies(0, c, 1, 0))
                    start(kv_copies(0, 1 - c, 1, 0))

        lax.fori_loop(0, 2, keys, None)

        def queries(gi, _):
            g = 1 - gi

            @pl.when(hh == 0)
            def _():
                wq_copy(g).wait()

            q = _dot(ab[h], wqb[g], 1, 0)
            for s in range(2):
                qb[g, 2 * z + h, s] = turned(q[:, s * HEAD : (s + 1) * HEAD], h)

            @pl.when((z == 3) & (g == 1))
            def _():
                q_copy(1, h, 1).start()

            @pl.when((z == 3) & (hh == 1) & (g == 0))
            def _():
                q_copy(0, c, 2).start()
                q_copy(0, 1 - c, 2).start()

        lax.fori_loop(0, 2, queries, None)

    lax.fori_loop(0, 2, project, None)

    for l in range(2):
        for g in range(2):
            @pl.when((z < 2) | ((z == 2) & (g == 0)))
            def _():
                ob[12 + l * 2 + g] = jnp.zeros(ob.shape[1:], BF)
                ls[12 + l * 2 + g] = jnp.full(ls.shape[1:], NEG, F32)

    ones = jnp.ones((8, n), BF)

    wo_copy.wait()

    def task(code):
        g, q, t, waits = (code // 2) % 2, (code // 4) % 8, (code // 32) % 8, code // 256
        local = q // 2 == z
        first = _pick(z, g, FIRST)
        def q_wait(qq):
            pltpu.make_async_remote_copy(qb.at[g, qq], qb.at[g, qq], qsend.at[0, 0], qrecv.at[g, qq], device_id=device(sp), device_id_type=MESH).wait_recv()

        @pl.when((z == 1) & (waits > 0) & (g == 1))
        def _():
            q_wait(6)
            q_wait(7)
            pl.semaphore_signal(go, 1, device_id=device(sp + 2), device_id_type=MESH)

        @pl.when((z == 2) & (waits > 0))
        def _():
            pl.semaphore_wait(go, 1)
            q_copy(1, c, 1).start()
            q_copy(1, 1 - c, 1).start()

        @pl.when(jnp.logical_not(local) & ((z == 2) | (q < 6)))
        def _():
            q_wait(q)

        for o in range(3):
            @pl.when((waits // 2**o) % 2 == 1)
            def _():
                for h in range(2):
                    j = 2 * o + h
                    for buf, send, recv in ((kb, ksend, krecv), (vb, vsend, vrecv)):
                        pltpu.make_async_remote_copy(buf.at[g, j], buf.at[g, j], send.at[0, 0, 0], recv.at[g, j], device_id=device(sp), device_id_type=MESH).wait_recv()

        top_s[...] = jnp.full(top_s.shape, NEG, F32)
        mix_s[...] = jnp.zeros(mix_s.shape, F32)

        def block(j, masked):
            scores = [_dot(kb[g, j], qb[g, q, s], 1, 1) for s in range(2)]
            weights, keeps = [], []
            for s in range(2):
                score = scores[s]
                if masked:
                    ok = lax.broadcasted_iota(jnp.int32, (n, n), 0) <= lax.broadcasted_iota(jnp.int32, (n, n), 1)
                    score = jnp.where(ok, score, 2 * NEG)
                old = top_s[s : s + 1, :]
                top = jnp.maximum(old, score.max(axis=0, keepdims=True))
                top_s[s : s + 1, :] = top
                weights.append(jnp.exp2((score - top) * e).astype(BF))
                keeps.append(jnp.exp2((old - top) * e))
            values = jnp.concatenate([vb[g, j], ones], axis=0)
            for s in range(2):
                mix_s[s] = mix_s[s] * keeps[s] + _dot(values, weights[s], 1, 0)

        lax.fori_loop(first, jnp.minimum(q, 2 * z + 2), lambda j, _: block(j, False), None)

        @pl.when(local)
        def _():
            block(q, True)

        slot = 8 + jnp.where(local, 0, 4) + c * 2 + g
        here = jnp.where(q == sp, slot, t)
        for s in range(2):
            total = mix_s[s, HEAD : HEAD + 1, :]
            ob[here, s] = (mix_s[s, :HEAD, :] * (1 / total)).astype(BF)
            lse = top_s[s : s + 1, :] * e + jnp.log2(total)
            per = n // 128
            for i in range(per):
                ls[here, s * per + i : s * per + i + 1, :] = lse[:, i * 128 : (i + 1) * 128]

        @pl.when(q != sp)
        def _():
            l_copy(t, slot, q).start()
            for s in range(2):
                o_copy(t, slot, s, q).start()

    def o_copy(t, slot, s, owner):
        return pltpu.make_async_remote_copy(ob.at[t, s], ob.at[slot, s], osend.at[t, s], orecv.at[slot - 8, s], device_id=device(owner), device_id_type=MESH)

    def l_copy(t, slot, owner):
        return pltpu.make_async_remote_copy(ls.at[t], ls.at[slot], lsend.at[t], lrecv.at[slot - 8], device_id=device(owner), device_id_type=MESH)

    def finish(code, last):
        g, s = (code // 2) % 2, (code // 4) % 2
        other = (code // 8) % 2
        l = (c + other) % 2
        base = l * 2 + g

        def arrived(slot):
            @pl.when(s == 0)
            def _():
                l_copy(0, slot, sp).wait_recv()

            o_copy(0, slot, s, sp).wait_recv()

        @pl.when(other == 1)
        def _():
            arrived(8 + base)

        @pl.when((z == 3) | ((z == 2) & (g == 1)))
        def _():
            arrived(12 + base)

        per = n // 128
        la, lb = (jnp.concatenate([ls[at + base, pl.ds(s * per + k, 1), :] for k in range(per)], axis=1) for at in (8, 12))
        m = jnp.maximum(la, lb)
        wa, wb = jnp.exp2(la - m), jnp.exp2(lb - m)
        r = 1 / (wa + wb)
        o = ob[8 + base, s].astype(F32) * (wa * r) + ob[12 + base, s].astype(F32) * (wb * r)
        of[...] = o.T.astype(BF)
        at = pl.ds(pl.multiple_of((l * 4 + g * 2 + s) * HEAD, HEAD), HEAD)

        def columns(k, _):
            cols = pl.ds(pl.multiple_of(k * (wide // 3), 128), wide // 3)
            y = yacc[:, cols] + _dot(of[...], wob[at, cols], 1, 0)

            @pl.when(jnp.logical_not(last))
            def _():
                yacc[:, cols] = y

            @pl.when(last)
            def _():
                y_ref[:, cols] = y.astype(BF)

        lax.fori_loop(0, 3, columns, None)

    steps = jnp.where(z == 1, 16, jnp.where(z == 2, 14, 12))

    def step(i, _):
        code = _pick(sp, i, PLAN)

        @pl.when(code % 2 == 0)
        def _():
            task(code)

        @pl.when(code % 2 == 1)
        def _():
            finish(code, i == steps - 1)

    lax.fori_loop(0, steps, step, None)

    a_copy(c).wait_send()

    def sent(copies):
        for copy in copies:
            copy.wait_send()

    for h in range(2):
        @pl.when(z == 0)
        def _():
            sent(kv_copies(1, h, 1, 0))
            sent(kv_copies(0, h, 2, 1))
            sent(kv_copies(0, h, 1, 0))

        @pl.when(z == 1)
        def _():
            sent(kv_copies(0, h, 2, 0))

        @pl.when(z == 2)
        def _():
            sent(kv_copies(1, h, 3, 0))

        @pl.when(z >= 2)
        def _():
            q_copy(1, h, 1).wait_send()

        @pl.when(z == 3)
        def _():
            q_copy(0, h, 2).wait_send()

    for t in range(6):
        @pl.when(t < _pick(0, z, [STAGED]))
        def _():
            l_copy(t, 8, sp).wait_send()
            for s in range(2):
                o_copy(t, 8, s, sp).wait_send()


def solution(mesh):
    def step(x, gain, wq, wk, wv, wo):
        n, wide = x.shape
        half = HEAD // 2
        rate = np.float64(THETA) ** (-np.arange(half) / half)
        table = lambda places: jnp.asarray(np.stack([f(places[:, None] * rate) for f in (np.cos, np.sin)]).astype(np.float32))
        coarse, fine = table(np.arange(8 * n // FINE) * FINE), table(np.arange(FINE))
        hbm, vmem = pl.BlockSpec(memory_space=pl.ANY), pl.BlockSpec(memory_space=pltpu.VMEM)
        dma = pltpu.SemaphoreType.DMA
        return pl.pallas_call(
            kernel,
            out_shape=pltpu.VMEM((n, wide), BF),
            in_specs=[hbm] * 8,
            out_specs=vmem,
            scratch_shapes=[
                pltpu.VMEM((n, wide), BF),
                pltpu.VMEM((wide,), BF),
                pltpu.VMEM((2, 2 * n // FINE, half), F32),
                pltpu.VMEM((2, FINE, half), F32),
                pltpu.VMEM((2, n, wide), BF),
                pltpu.VMEM((2, wide, 2 * HEAD), BF),
                pltpu.VMEM((2, wide, HEAD), BF),
                pltpu.VMEM((2, wide, HEAD), BF),
                pltpu.VMEM((8 * HEAD, wide), BF),
                pltpu.VMEM((2, 8, n, HEAD), BF),
                pltpu.VMEM((2, 8, HEAD, n), BF),
                pltpu.VMEM((2, 8, 2, n, HEAD), BF),
                pltpu.VMEM((16, 2, HEAD, n), BF),
                pltpu.VMEM((16, 8, 128), F32),
                pltpu.VMEM((8, n), F32),
                pltpu.VMEM((2, HEAD + 8, n), F32),
                pltpu.VMEM((n, HEAD), BF),
                pltpu.VMEM((n, wide), F32),
                pltpu.VMEM((2, 2 * n, half), F32),
                dma((14,)), dma((1,)), dma((1,)),
                dma((2, 2, 2)), dma((2, 2, 2)), dma((2, 8)), dma((2, 8)),
                dma((2, 2)), dma((2, 8)),
                dma((8, 2)), dma((8,)), dma((8, 2)), dma((8,)),
                pltpu.SemaphoreType.REGULAR,
            ],
            compiler_params=pltpu.CompilerParams(collective_id=0, has_side_effects=True, vmem_limit_bytes=61 << 20),
        )(x, gain, coarse, fine, wq, wk, wv, wo)

    tokens, whole = P(("dp", "sp"), None), P(None, None)
    return jax.shard_map(
        step,
        mesh=mesh,
        in_specs=(tokens, P(None), whole, whole, whole, whole),
        out_specs=tokens,
        check_vma=False,
    )
```

```python
import functools

import jax
import jax.numpy as jnp
import numpy as np
from jax import lax
from jax.experimental import pallas as pl
from jax.experimental.pallas import tpu as pltpu
from jax.sharding import PartitionSpec as P

HEAD = 256
THETA = 10000
NEG = -1e30
LOG2E = 1.4426950408889634
FINE = 32
MESH = pl.DeviceIdType.MESH
BF, F32 = jnp.bfloat16, jnp.float32
PAIR = (0, 1)
LOCAL, REMOTE = 8, 12

FIRST = [[0, 0], [0, 0], [0, 4], [6, 4]]
STAGED = [2, 6, 4, 2]
SENT = [6, 2, 4, 4]
SIZES = (4, 2, 8, 8)


def plan(z, c):
    steps, staged = [], 0

    def step(kind, g, what, slot=0, waits=0):
        code = waits
        for field, size in reversed(list(zip((kind, g, what, slot), SIZES))):
            code = code * size + field
        steps.append(code)

    def attention(g, a, b, waits=0):
        nonlocal staged
        for q in (a, b) if c == 0 else (b, a):
            step(0, g, q, staged, waits)
            waits = 0
            staged += q != 2 * z + c

    def output(g, last=False):
        step(2, g, 0)
        for piece in range(4, 8 if last else 5):
            step(1 if last else 2, g, piece)

    if z == 0:
        attention(1, 0, 1), attention(0, 0, 1), output(1), output(0, True)
    elif z == 1:
        attention(1, 6, 7, 1), attention(1, 2, 3), attention(1, 4, 5), output(1), attention(0, 2, 3, 1), output(0, True)
    elif z == 2:
        attention(1, 4, 5), attention(0, 6, 7, 3), attention(0, 4, 5), output(0), output(1, True)
    else:
        attention(0, 6, 7), attention(1, 6, 7, 4), output(1), output(0, True)
    return steps


PLAN = [plan(z, c) for z in range(4) for c in PAIR]


def fields(code):
    got = []
    for size in SIZES:
        got.append(code % size)
        code = code // size
    return *got, code


def _dot(a, b, ca, cb):
    return lax.dot_general(a, b, (((ca,), (cb,)), ((), ())), preferred_element_type=F32)


def _pick(z, i, table):
    out = jnp.int32(0)
    for zz, row in enumerate(table):
        got = jnp.int32(0)
        for ii, value in enumerate(row):
            got = jnp.where(i == ii, jnp.int32(value), got)
        out = jnp.where(z == zz, got, out)
    return out


def kernel(x_hbm, gain_hbm, coarse_hbm, fine_hbm, wq_hbm, wk_hbm, wv_hbm, wo_hbm, y_ref,
           xb, gainb, coarse_ref, fine_ref, ab, wqb, wkvb, wob, kb, vb, qb, ob, ls, top_s, mix_s, of, yacc, cs,
           wsem, sent, arecv, krecv, qrecv, local_o, local_l, remote_o, remote_l, go):
    dp, sp = lax.axis_index("dp"), lax.axis_index("sp")
    z, c = sp // 2, sp % 2
    n, wide = xb.shape
    rows = n // 4
    scale = HEAD**-0.5
    e = scale * LOG2E

    def push(src, dst, send, recv, to):
        pltpu.make_async_remote_copy(src, dst, sent.at[send], recv, device_id=(dp, to), device_id_type=MESH).start()

    def wait(ref, sem):
        pltpu.make_async_copy(ref, ref, sem).wait()

    def x_copy(i):
        at = pl.ds(i * rows, rows)
        return pltpu.make_async_copy(x_hbm.at[at], xb.at[at], wsem.at[i])

    def w_copy(hbm, dst, g, width, sem):
        at = pl.ds(pl.multiple_of((c * 2 + g) * width, width), width)
        return pltpu.make_async_copy(hbm.at[:, at], dst, sem)

    wk_copy = lambda g: w_copy(wk_hbm, wkvb.at[g, :, pl.ds(0, HEAD)], g, HEAD, wsem.at[4 + g])
    wv_copy = lambda g: w_copy(wv_hbm, wkvb.at[g, :, pl.ds(HEAD, HEAD)], g, HEAD, wsem.at[4 + g])
    wq_copy = lambda g: w_copy(wq_hbm, wqb.at[g], g, 2 * HEAD, wsem.at[6 + g])
    wo_copy = pltpu.make_async_copy(wo_hbm, wob, wsem.at[8])
    g_first = jnp.where(z == 0, 1, 0)

    count = 2 * n // FINE
    gain_copy = pltpu.make_async_copy(gain_hbm, gainb, wsem.at[9])
    tables = [pltpu.make_async_copy(fine_hbm, fine_ref, wsem.at[10]),
              pltpu.make_async_copy(coarse_hbm.at[:, pl.ds(pl.multiple_of(z * count, 8), count)], coarse_ref, wsem.at[11])]

    gain_copy.start()
    for i in range(4):
        x_copy(i).start()
    for copy in tables:
        copy.start()
    wk_copy(g_first).start()
    wv_copy(g_first).start()

    barrier = pltpu.get_barrier_semaphore()
    for step in range(1, 8):
        pl.semaphore_signal(barrier, 1, device_id=(dp, (sp + step) % 8), device_id_type=MESH)

    gain_copy.wait()
    gain = gainb[...].astype(F32)[None, :]
    for i in range(4):
        x_copy(i).wait()
        at = pl.ds(i * rows, rows)
        w = xb[at, :].astype(F32)
        yacc[at, :] = w
        ab[c, at, :] = (w * lax.rsqrt(jnp.mean(w * w, -1, keepdims=True) + 1e-6) * gain).astype(BF)
    for copy in tables:
        copy.wait()
    fc, fs = fine_ref[0], fine_ref[1]

    def turn_table(i, _):
        cc = coarse_ref[0, pl.ds(i, 1), :]
        ss = coarse_ref[1, pl.ds(i, 1), :]
        at = pl.ds(pl.multiple_of(i * FINE, FINE), FINE)
        cs[0, at, :] = cc * fc - ss * fs
        cs[1, at, :] = ss * fc + cc * fs

    lax.fori_loop(0, count, turn_table, None)

    pl.semaphore_wait(barrier, 7)
    push(ab.at[c], ab.at[c], 0, arecv, z * 2 + 1 - c)
    wk_copy(1 - g_first).start()
    wv_copy(1 - g_first).start()
    wq_copy(1).start()
    wq_copy(0).start()

    def send_keys(g, h, to, r):
        ref = kb.at[g, 2 * z + h, pl.ds(r * (n // 2), n // 2)]
        push(ref, ref, 1, krecv.at[g, z], 2 * to + c)

    def send_values(g, h, to):
        ref = vb.at[g, 2 * z + h]
        push(ref, ref, 1, krecv.at[g, z], 2 * to + c)

    def send_both(g, h, to):
        for r in PAIR:
            send_keys(g, h, to, r)
        send_values(g, h, to)

    def send_queries(g, h, to):
        ref = qb.at[g, 2 * z + h]
        push(ref, ref, 1, qrecv.at[2 * z + h - 4], 2 * to + c)

    def turned(t, first):
        at = pl.ds(pl.multiple_of(first, n // 2), t.shape[0])
        cos, sin = cs[0, at, :], cs[1, at, :]
        t = t.astype(BF).astype(F32)
        a, b = t[:, : HEAD // 2], t[:, HEAD // 2 :]
        return jnp.concatenate([a * cos - b * sin, b * cos + a * sin], -1).astype(BF)

    def project(hh, _):
        h = jnp.where(hh == 0, c, 1 - c)

        @pl.when(hh == 1)
        def _():
            wait(ab.at[1 - c], arecv)
            wo_copy.start()

        def keys(gi, _):
            g = jnp.where(gi == 0, g_first, 1 - g_first)

            @pl.when(hh == 0)
            def _():
                wait(wkvb.at[g], wsem.at[4 + g])

            def send(what, *more):
                for at, gg, to in ((z == 1) & (g == 0), 0, 2), ((z == 2) & (g == 1), 1, 3), ((z == 0) & (gi == 0), 1, 1):
                    pl.when(at)(functools.partial(what, gg, h, to, *more))

            for r in PAIR:
                at = slice(r * (n // 2), (r + 1) * (n // 2))
                kv = _dot(ab[h, at, :], wkvb[g], 1, 0)
                kb[g, 2 * z + h, at, :] = turned(kv[:, :HEAD], h * n + r * (n // 2))
                send(send_keys, r)
                vb[g, 2 * z + h, :, at] = kv[:, HEAD:].astype(BF).T
            send(send_values)

            @pl.when((z == 0) & (gi == 1))
            def _():
                send_both(0, h, 2)

                @pl.when(hh == 1)
                def _():
                    send_both(0, c, 1)
                    send_both(0, 1 - c, 1)

        lax.fori_loop(0, 2, keys, None)

        def queries(gi, _):
            g = 1 - gi

            @pl.when(hh == 0)
            def _():
                wq_copy(g).wait()

            q = _dot(ab[h], wqb[g], 1, 0)
            for s in PAIR:
                qb[g, 2 * z + h, s] = turned(q[:, s * HEAD : (s + 1) * HEAD], h * n)

            @pl.when((z == 3) & (g == 1))
            def _():
                send_queries(1, h, 1)

            @pl.when((z == 3) & (hh == 1) & (g == 0))
            def _():
                send_queries(0, c, 2)
                send_queries(0, 1 - c, 2)

        lax.fori_loop(0, 2, queries, None)

    lax.fori_loop(0, 2, project, None)

    for l in range(2):
        for g in PAIR:
            @pl.when((z < 2) | ((z == 2) & (g == 0)))
            def _():
                ob[REMOTE + l * 2 + g] = jnp.zeros(ob.shape[1:], BF)
                ls[REMOTE + l * 2 + g] = jnp.full(ls.shape[1:], NEG, F32)

    ones = jnp.ones((8, n), BF)

    wo_copy.wait()

    def task(code):
        _, g, q, t, waits = fields(code)
        local = q // 2 == z
        first = _pick(z, g, FIRST)
        def q_wait(qq):
            wait(qb.at[g, qq], qrecv.at[qq - 4])

        @pl.when((z == 1) & (waits > 0) & (g == 1))
        def _():
            q_wait(6)
            q_wait(7)
            pl.semaphore_signal(go, 1, device_id=(dp, sp + 2), device_id_type=MESH)

        @pl.when((z == 2) & (waits > 0))
        def _():
            pl.semaphore_wait(go, 1)
            send_queries(1, c, 1)
            send_queries(1, 1 - c, 1)

        @pl.when(jnp.logical_not(local) & ((z == 2) | (q < 6)))
        def _():
            q_wait(q)

        for o in range(3):
            @pl.when((waits // 2**o) % 2 == 1)
            def _():
                wait(kb.at[g, pl.ds(0, 4)], krecv.at[g, o])

        top_s[...] = jnp.full(top_s.shape, NEG, F32)
        mix_s[...] = jnp.zeros(mix_s.shape, F32)

        def block(j, masked):
            scores = [_dot(kb[g, j], qb[g, q, s], 1, 1) for s in range(2)]
            weights, keeps = [], []
            for s in PAIR:
                score = scores[s]
                if masked:
                    ok = lax.broadcasted_iota(jnp.int32, (n, n), 0) <= lax.broadcasted_iota(jnp.int32, (n, n), 1)
                    score = jnp.where(ok, score, 2 * NEG)
                old = top_s[s : s + 1, :]
                top = jnp.maximum(old, score.max(axis=0, keepdims=True))
                top_s[s : s + 1, :] = top
                weights.append(jnp.exp2((score - top) * e).astype(BF))
                keeps.append(jnp.exp2((old - top) * e))
            values = jnp.concatenate([vb[g, j], ones], axis=0)
            for s in PAIR:
                mix_s[s] = mix_s[s] * keeps[s] + _dot(values, weights[s], 1, 0)

        lax.fori_loop(first, jnp.minimum(q, 2 * z + 2), lambda j, _: block(j, False), None)

        @pl.when(local)
        def _():
            block(q, True)

        slot = jnp.where(local, LOCAL, REMOTE) + c * 2 + g
        here = jnp.where(q == sp, slot, t)
        for s in PAIR:
            total = mix_s[s, HEAD : HEAD + 1, :]
            o = (mix_s[s, :HEAD, :] * (1 / total)).astype(BF)
            for half in PAIR:
                ob[here, s, half] = o[:, half * n // 2 : (half + 1) * n // 2]
            lse = top_s[s : s + 1, :] * e + jnp.log2(total)
            per = n // 128
            for i in range(per):
                ls[here, s * per + i : s * per + i + 1, :] = lse[:, i * 128 : (i + 1) * 128]

        @pl.when(local & (q != sp))
        def _():
            push(ls.at[t], ls.at[slot], 3, local_l.at[g], q)
            push(ob.at[t], ob.at[slot], 2, local_o.at[g], q)

        @pl.when(jnp.logical_not(local))
        def _():
            own = q % 2 == c
            push(ls.at[t], ls.at[slot], 3, remote_l.at[g, jnp.where(own, 0, 1)], q)

            @pl.when(own)
            def _():
                push(ob.at[t], ob.at[slot], 2, remote_o.at[g, 0], q)

            @pl.when(jnp.logical_not(own))
            def _():
                for s in PAIR:
                    for half in PAIR:
                        push(ob.at[t, s, half], ob.at[slot, s, half], 2, remote_o.at[g, 1 + 2 * s + half], q)

    def merged(base, s, half):
        per = n // 256
        la, lb = (jnp.concatenate([ls[at + base, pl.ds((2 * s + half) * per + k, 1), :] for k in range(per)], axis=1) for at in (LOCAL, REMOTE))
        m = jnp.maximum(la, lb)
        wa, wb = jnp.exp2(la - m), jnp.exp2(lb - m)
        r = 1 / (wa + wb)
        o = ob[LOCAL + base, s, half].astype(F32) * (wa * r) + ob[REMOTE + base, s, half].astype(F32) * (wb * r)
        return o.T.astype(BF)

    def arrivals(g, other, first, pieces):
        piece = ob.at[0, 0, 0]

        @pl.when(first & (other == 1))
        def _():
            wait(ls.at[0], local_l.at[g])
            wait(ob.at[0], local_o.at[g])

        @pl.when((z == 3) | ((z == 2) & (g == 1)))
        def _():
            @pl.when(first)
            def _():
                wait(ls.at[0], remote_l.at[g, other])

            @pl.when(other == 0)
            def _():
                wait(ob.at[0], remote_o.at[g, 0])

            @pl.when(other == 1)
            def _():
                for i in pieces:
                    wait(piece, remote_o.at[g, 1 + i])

    third = wide // 3

    def finish_line(code):
        _, g, what, _, _ = fields(code)
        other = what // 4
        l = (c + other) % 2
        base = l * 2 + g
        arrivals(g, other, True, range(4))
        for s in PAIR:
            for half in PAIR:
                of[half * (n // 2) : (half + 1) * (n // 2), s * HEAD : (s + 1) * HEAD] = merged(base, s, half)
        at = pl.ds(pl.multiple_of((l * 4 + g * 2) * HEAD, 2 * HEAD), 2 * HEAD)

        def columns(k, _):
            cols = pl.ds(pl.multiple_of(k * third, 128), third)
            yacc[:, cols] += _dot(of[...], wob[at, cols], 1, 0)

        lax.fori_loop(0, 3, columns, None)

    def finish_piece(code, last):
        _, g, what, _, _ = fields(code)
        s, half = (what // 2) % 2, what % 2
        l = 1 - c
        base = l * 2 + g
        arrivals(g, 1, what == 4, [what - 4])
        of[0 : n // 2, 0:HEAD] = merged(base, s, half)
        at = pl.ds(pl.multiple_of((l * 4 + g * 2 + s) * HEAD, HEAD), HEAD)
        tokens = pl.ds(pl.multiple_of(half * (n // 2), n // 2), n // 2)

        @pl.when(jnp.logical_not(last))
        def _():
            for k in range(3):
                cols = slice(k * third, (k + 1) * third)
                yacc[tokens, cols] += _dot(of[0 : n // 2, 0:HEAD], wob[at, cols], 1, 0)

        @pl.when(last)
        def _():
            for k in range(3):
                cols = slice(k * third, (k + 1) * third)
                y_ref[tokens, cols] = (yacc[tokens, cols] + _dot(of[0 : n // 2, 0:HEAD], wob[at, cols], 1, 0)).astype(BF)

    steps = jnp.where(z == 1, 15, jnp.where(z == 2, 13, 11))

    def drain():
        wait(ab.at[c], sent.at[0])
        for zz in range(4):
            @pl.when(z == zz)
            def _():
                wait(qb.at[0, pl.ds(0, SENT[zz])], sent.at[1])
                wait(ob.at[pl.ds(0, STAGED[zz])], sent.at[2])
                wait(ls.at[pl.ds(0, STAGED[zz])], sent.at[3])

    def step(i, _):
        code = _pick(sp, i, PLAN)

        @pl.when(code % 4 == 0)
        def _():
            task(code)

        @pl.when(code % 4 == 2)
        def _():
            finish_line(code)

        @pl.when(code % 4 == 1)
        def _():
            @pl.when((z != 1) & (i == steps - 1))
            def _():
                drain()

            finish_piece(code, i >= steps - 2)

    lax.fori_loop(0, steps, step, None)

    @pl.when(z == 1)
    def _():
        drain()


def solution(mesh):
    def step(x, gain, wq, wk, wv, wo):
        n, wide = x.shape
        half = HEAD // 2
        rate = np.float64(THETA) ** (-np.arange(half) / half)
        table = lambda places: jnp.asarray(np.stack([f(places[:, None] * rate) for f in (np.cos, np.sin)]).astype(np.float32))
        coarse, fine = table(np.arange(8 * n // FINE) * FINE), table(np.arange(FINE))
        hbm, vmem = pl.BlockSpec(memory_space=pl.ANY), pl.BlockSpec(memory_space=pltpu.VMEM)
        dma = pltpu.SemaphoreType.DMA
        return pl.pallas_call(
            kernel,
            out_shape=pltpu.VMEM((n, wide), BF),
            in_specs=[hbm] * 8,
            out_specs=vmem,
            scratch_shapes=[
                pltpu.VMEM((n, wide), BF),
                pltpu.VMEM((wide,), BF),
                pltpu.VMEM((2, 2 * n // FINE, half), F32),
                pltpu.VMEM((2, FINE, half), F32),
                pltpu.VMEM((2, n, wide), BF),
                pltpu.VMEM((2, wide, 2 * HEAD), BF),
                pltpu.VMEM((2, wide, 2 * HEAD), BF),
                pltpu.VMEM((8 * HEAD, wide), BF),
                pltpu.VMEM((2, 8, n, HEAD), BF),
                pltpu.VMEM((2, 8, HEAD, n), BF),
                pltpu.VMEM((2, 8, 2, n, HEAD), BF),
                pltpu.VMEM((16, 2, 2, HEAD, n // 2), BF),
                pltpu.VMEM((16, 8, 128), F32),
                pltpu.VMEM((8, n), F32),
                pltpu.VMEM((2, HEAD + 8, n), F32),
                pltpu.VMEM((n, 2 * HEAD), BF),
                pltpu.VMEM((n, wide), F32),
                pltpu.VMEM((2, 2 * n, half), F32),
                dma((12,)), dma((4,)), dma,
                dma((2, 3)), dma((4,)),
                dma((2,)), dma((2,)), dma((2, 5)), dma((2, 2)),
                pltpu.SemaphoreType.REGULAR,
            ],
            compiler_params=pltpu.CompilerParams(collective_id=0, has_side_effects=True, vmem_limit_bytes=61 << 20),
        )(x, gain, coarse, fine, wq, wk, wv, wo)

    tokens, whole = P(("dp", "sp"), None), P(None, None)
    return jax.shard_map(
        step,
        mesh=mesh,
        in_specs=(tokens, P(None), whole, whole, whole, whole),
        out_specs=tokens,
        check_vma=False,
    )
```

```python
import functools

import jax
import jax.numpy as jnp
import numpy as np
from jax import lax
from jax.experimental import pallas as pl
from jax.experimental.pallas import tpu as pltpu
from jax.sharding import PartitionSpec as P

HEAD = 256
THETA = 10000
NEG = -1e30
LOG2E = 1.4426950408889634
FINE = 32
MESH = pl.DeviceIdType.MESH
BF, F32 = jnp.bfloat16, jnp.float32
PAIR = (0, 1)
LOCAL, REMOTE = 8, 12

FIRST = [[0, 0], [0, 0], [0, 4], [6, 4]]
STAGED = [2, 6, 4, 2]
SENT = [6, 2, 4, 4]
SIZES = (4, 2, 8, 8)


def plan(z, c):
    steps, staged = [], 0

    def step(kind, g, what, slot=0, waits=0):
        code = waits
        for field, size in reversed(list(zip((kind, g, what, slot), SIZES))):
            code = code * size + field
        steps.append(code)

    def attention(g, a, b, waits=0):
        nonlocal staged
        for q in (a, b) if c == 0 else (b, a):
            step(0, g, q, staged, waits)
            waits = 0
            staged += q != 2 * z + c

    def output(g, last=False):
        step(2, g, 0)
        for piece in range(4, 8 if last else 5):
            step(1 if last else 2, g, piece)

    if z == 0:
        attention(1, 0, 1), attention(0, 0, 1), output(1), output(0, True)
    elif z == 1:
        attention(1, 6, 7, 1), attention(1, 2, 3), attention(1, 4, 5), output(1), attention(0, 2, 3, 1), output(0, True)
    elif z == 2:
        attention(1, 4, 5), attention(0, 6, 7, 3), attention(0, 4, 5), output(0), output(1, True)
    else:
        attention(0, 6, 7), attention(1, 6, 7, 4), output(1), output(0, True)
    return steps


PLAN = [plan(z, c) for z in range(4) for c in PAIR]


def fields(code):
    got = []
    for size in SIZES:
        got.append(code % size)
        code = code // size
    return *got, code


def _dot(a, b, ca, cb):
    return lax.dot_general(a, b, (((ca,), (cb,)), ((), ())), preferred_element_type=F32)


def _pick(z, i, table):
    out = jnp.int32(0)
    for zz, row in enumerate(table):
        got = jnp.int32(0)
        for ii, value in enumerate(row):
            got = jnp.where(i == ii, jnp.int32(value), got)
        out = jnp.where(z == zz, got, out)
    return out


def kernel(x_hbm, gain_hbm, coarse_hbm, fine_hbm, wq_hbm, wk_hbm, wv_hbm, wo_hbm, y_ref,
           xb, gainb, coarse_ref, fine_ref, ab, wqb, wkvb, wob, kb, vb, qb, ob, ls, top_s, mix_s, of, yacc, cs,
           wsem, sent, arecv, krecv, qrecv, local_o, local_l, remote_o, remote_l, go, ready):
    dp, sp = lax.axis_index("dp"), lax.axis_index("sp")
    z, c = sp // 2, sp % 2
    n, wide = xb.shape
    rows = n // 4
    scale = HEAD**-0.5
    e = scale * LOG2E

    def push(src, dst, send, recv, to):
        pltpu.make_async_remote_copy(src, dst, sent.at[send], recv, device_id=(dp, to), device_id_type=MESH).start()

    def wait(ref, sem):
        pltpu.make_async_copy(ref, ref, sem).wait()

    def x_copy(i):
        at = pl.ds(i * rows, rows)
        return pltpu.make_async_copy(x_hbm.at[at], xb.at[at], wsem.at[i])

    def w_copy(hbm, dst, g, width, sem):
        at = pl.ds(pl.multiple_of((c * 2 + g) * width, width), width)
        return pltpu.make_async_copy(hbm.at[:, at], dst, sem)

    wk_copy = lambda g: w_copy(wk_hbm, wkvb.at[g, :, pl.ds(0, HEAD)], g, HEAD, wsem.at[4 + g])
    wv_copy = lambda g: w_copy(wv_hbm, wkvb.at[g, :, pl.ds(HEAD, HEAD)], g, HEAD, wsem.at[4 + g])
    wq_copy = lambda g: w_copy(wq_hbm, wqb.at[g], g, 2 * HEAD, wsem.at[6 + g])
    wo_copy = pltpu.make_async_copy(wo_hbm, wob, wsem.at[8])
    g_first = jnp.where(z == 0, 1, 0)

    count = 2 * n // FINE
    gain_copy = pltpu.make_async_copy(gain_hbm, gainb, wsem.at[9])
    tables = [pltpu.make_async_copy(fine_hbm, fine_ref, wsem.at[10]),
              pltpu.make_async_copy(coarse_hbm.at[:, pl.ds(pl.multiple_of(z * count, 8), count)], coarse_ref, wsem.at[11])]

    for copy in gain_copy, *tables:
        copy.start()
    for i in PAIR:
        x_copy(i).start()
    wk_copy(g_first).start()
    wv_copy(g_first).start()

    barrier = pltpu.get_barrier_semaphore()

    def here_now(chip, core):
        pl.semaphore_signal(barrier, 1, device_id=(dp, 2 * chip + core), device_id_type=MESH)

    here_now(z, 1 - c)

    @pl.when((z == 1) | (z == 2))
    def _():
        here_now(0, c)

    @pl.when(z == 1)
    def _():
        here_now(2, c)
        for core in PAIR:
            here_now(3, core)

    @pl.when(z == 2)
    def _():
        here_now(3, c)

    @pl.when(z >= 2)
    def _():
        for core in PAIR:
            here_now(z - 1, core)

    for copy in tables:
        copy.wait()
    fc, fs = fine_ref[0], fine_ref[1]

    def turn_table(i, _):
        cc = coarse_ref[0, pl.ds(i, 1), :]
        ss = coarse_ref[1, pl.ds(i, 1), :]
        at = pl.ds(pl.multiple_of(i * FINE, FINE), FINE)
        cs[0, at, :] = cc * fc - ss * fs
        cs[1, at, :] = ss * fc + cc * fs

    lax.fori_loop(0, count, turn_table, None)

    def send_keys(g, h, to, r):
        ref = kb.at[g, 2 * z + h, pl.ds(r * (n // 2), n // 2)]
        push(ref, ref, 1, krecv.at[g, z], 2 * to + c)

    def send_values(g, h, to):
        ref = vb.at[g, 2 * z + h]
        push(ref, ref, 1, krecv.at[g, z], 2 * to + c)

    def send_both(g, h, to):
        for r in PAIR:
            send_keys(g, h, to, r)
        send_values(g, h, to)

    def send_queries(g, h, to):
        ref = qb.at[g, 2 * z + h]
        push(ref, ref, 1, qrecv.at[2 * z + h - 4], 2 * to + c)

    def turned(t, first):
        at = pl.ds(pl.multiple_of(first, n // 2), t.shape[0])
        cos, sin = cs[0, at, :], cs[1, at, :]
        t = t.astype(BF).astype(F32)
        a, b = t[:, : HEAD // 2], t[:, HEAD // 2 :]
        return jnp.concatenate([a * cos - b * sin, b * cos + a * sin], -1).astype(BF)

    def make_keys(g, gi, h, r):
        def send(what, *more):
            for at, gg, to in ((z == 1) & (g == 0), 0, 2), ((z == 2) & (g == 1), 1, 3), ((z == 0) & (gi == 0), 1, 1):
                pl.when(at)(functools.partial(what, gg, h, to, *more))

        at = slice(r * (n // 2), (r + 1) * (n // 2))
        kv = _dot(ab[h, at, :], wkvb[g], 1, 0)
        kb[g, 2 * z + h, at, :] = turned(kv[:, :HEAD], h * n + r * (n // 2))
        send(send_keys, r)
        vb[g, 2 * z + h, :, at] = kv[:, HEAD:].astype(BF).T
        if r == 1:
            send(send_values)

    gain_copy.wait()
    gain = gainb[...].astype(F32)[None, :]
    for r in PAIR:
        for i in PAIR:
            x_copy(2 * r + i).wait()
            if r == 0:
                x_copy(2 + i).start()
            at = pl.ds((2 * r + i) * rows, rows)
            w = xb[at, :].astype(F32)
            ab[c, at, :] = (w * lax.rsqrt(jnp.mean(w * w, -1, keepdims=True) + 1e-6) * gain).astype(BF)
        if r == 0:
            wait(wkvb.at[g_first], wsem.at[4 + g_first])
            pl.semaphore_wait(barrier, jnp.where(z >= 2, 4, 3))

            @pl.when(z == 3)
            def _():
                for core in PAIR:
                    pl.semaphore_signal(ready, 1, device_id=(dp, 2 + core), device_id_type=MESH)
        else:
            push(ab.at[c], ab.at[c], 0, arecv, z * 2 + 1 - c)
        make_keys(g_first, 0, c, r)
    wk_copy(1 - g_first).start()
    wv_copy(1 - g_first).start()
    wq_copy(1).start()
    wq_copy(0).start()

    def project(hh, _):
        h = jnp.where(hh == 0, c, 1 - c)

        @pl.when(hh == 1)
        def _():
            wait(ab.at[1 - c], arecv)
            wo_copy.start()

        def keys(gi, _):
            g = jnp.where(gi == 0, g_first, 1 - g_first)

            @pl.when(hh == 0)
            def _():
                wait(wkvb.at[g], wsem.at[4 + g])

            for r in PAIR:
                make_keys(g, gi, h, r)

            @pl.when((z == 0) & (gi == 1))
            def _():
                send_both(0, h, 2)

                @pl.when(hh == 1)
                def _():
                    send_both(0, c, 1)
                    send_both(0, 1 - c, 1)

        lax.fori_loop(jnp.where(hh == 0, 1, 0), 2, keys, None)

        def queries(gi, _):
            g = 1 - gi

            @pl.when(hh == 0)
            def _():
                wq_copy(g).wait()

            q = _dot(ab[h], wqb[g], 1, 0)
            for s in PAIR:
                qb[g, 2 * z + h, s] = turned(q[:, s * HEAD : (s + 1) * HEAD], h * n)

            @pl.when((z == 3) & (g == 1))
            def _():
                send_queries(1, h, 1)

            @pl.when((z == 3) & (hh == 1) & (g == 0))
            def _():
                send_queries(0, c, 2)
                send_queries(0, 1 - c, 2)

        lax.fori_loop(0, 2, queries, None)

    lax.fori_loop(0, 2, project, None)
    yacc[...] = xb[...].astype(F32)

    for l in range(2):
        for g in PAIR:
            @pl.when((z < 2) | ((z == 2) & (g == 0)))
            def _():
                ob[REMOTE + l * 2 + g] = jnp.zeros(ob.shape[1:], BF)
                ls[REMOTE + l * 2 + g] = jnp.full(ls.shape[1:], NEG, F32)

    ones = jnp.ones((8, n), BF)

    wo_copy.wait()

    def task(code):
        _, g, q, t, waits = fields(code)
        local = q // 2 == z
        first = _pick(z, g, FIRST)
        def q_wait(qq):
            wait(qb.at[g, qq], qrecv.at[qq - 4])

        @pl.when((z == 1) & (waits > 0) & (g == 1))
        def _():
            q_wait(6)
            q_wait(7)
            pl.semaphore_wait(ready, 2)
            pl.semaphore_signal(go, 1, device_id=(dp, sp + 2), device_id_type=MESH)

        @pl.when((z == 2) & (waits > 0))
        def _():
            pl.semaphore_wait(go, 1)
            send_queries(1, c, 1)
            send_queries(1, 1 - c, 1)

        @pl.when(jnp.logical_not(local) & ((z == 2) | (q < 6)))
        def _():
            q_wait(q)

        for o in range(3):
            @pl.when((waits // 2**o) % 2 == 1)
            def _():
                wait(kb.at[g, pl.ds(0, 4)], krecv.at[g, o])

        top_s[...] = jnp.full(top_s.shape, NEG, F32)
        mix_s[...] = jnp.zeros(mix_s.shape, F32)

        def block(j, masked):
            scores = [_dot(kb[g, j], qb[g, q, s], 1, 1) for s in range(2)]
            weights, keeps = [], []
            for s in PAIR:
                score = scores[s]
                if masked:
                    ok = lax.broadcasted_iota(jnp.int32, (n, n), 0) <= lax.broadcasted_iota(jnp.int32, (n, n), 1)
                    score = jnp.where(ok, score, 2 * NEG)
                old = top_s[s : s + 1, :]
                top = jnp.maximum(old, score.max(axis=0, keepdims=True))
                top_s[s : s + 1, :] = top
                weights.append(jnp.exp2((score - top) * e).astype(BF))
                keeps.append(jnp.exp2((old - top) * e))
            values = jnp.concatenate([vb[g, j], ones], axis=0)
            for s in PAIR:
                mix_s[s] = mix_s[s] * keeps[s] + _dot(values, weights[s], 1, 0)

        lax.fori_loop(first, jnp.minimum(q, 2 * z + 2), lambda j, _: block(j, False), None)

        @pl.when(local)
        def _():
            block(q, True)

        slot = jnp.where(local, LOCAL, REMOTE) + c * 2 + g
        here = jnp.where(q == sp, slot, t)
        for s in PAIR:
            total = mix_s[s, HEAD : HEAD + 1, :]
            o = (mix_s[s, :HEAD, :] * (1 / total)).astype(BF)
            for half in PAIR:
                ob[here, s, half] = o[:, half * n // 2 : (half + 1) * n // 2]
            lse = top_s[s : s + 1, :] * e + jnp.log2(total)
            per = n // 128
            for i in range(per):
                ls[here, s * per + i : s * per + i + 1, :] = lse[:, i * 128 : (i + 1) * 128]

        @pl.when(local & (q != sp))
        def _():
            push(ls.at[t], ls.at[slot], 3, local_l.at[g], q)
            push(ob.at[t], ob.at[slot], 2, local_o.at[g], q)

        @pl.when(jnp.logical_not(local))
        def _():
            own = q % 2 == c
            push(ls.at[t], ls.at[slot], 3, remote_l.at[g, jnp.where(own, 0, 1)], q)

            @pl.when(own)
            def _():
                push(ob.at[t], ob.at[slot], 2, remote_o.at[g, 0], q)

            @pl.when(jnp.logical_not(own))
            def _():
                for s in PAIR:
                    for half in PAIR:
                        push(ob.at[t, s, half], ob.at[slot, s, half], 2, remote_o.at[g, 1 + 2 * s + half], q)

    def merged(base, s, half):
        per = n // 256
        la, lb = (jnp.concatenate([ls[at + base, pl.ds((2 * s + half) * per + k, 1), :] for k in range(per)], axis=1) for at in (LOCAL, REMOTE))
        m = jnp.maximum(la, lb)
        wa, wb = jnp.exp2(la - m), jnp.exp2(lb - m)
        r = 1 / (wa + wb)
        o = ob[LOCAL + base, s, half].astype(F32) * (wa * r) + ob[REMOTE + base, s, half].astype(F32) * (wb * r)
        return o.T.astype(BF)

    def arrivals(g, other, first, pieces):
        piece = ob.at[0, 0, 0]

        @pl.when(first & (other == 1))
        def _():
            wait(ls.at[0], local_l.at[g])
            wait(ob.at[0], local_o.at[g])

        @pl.when((z == 3) | ((z == 2) & (g == 1)))
        def _():
            @pl.when(first)
            def _():
                wait(ls.at[0], remote_l.at[g, other])

            @pl.when(other == 0)
            def _():
                wait(ob.at[0], remote_o.at[g, 0])

            @pl.when(other == 1)
            def _():
                for i in pieces:
                    wait(piece, remote_o.at[g, 1 + i])

    third = wide // 3

    def finish_line(code):
        _, g, what, _, _ = fields(code)
        other = what // 4
        l = (c + other) % 2
        base = l * 2 + g
        arrivals(g, other, True, range(4))
        for s in PAIR:
            for half in PAIR:
                of[half * (n // 2) : (half + 1) * (n // 2), s * HEAD : (s + 1) * HEAD] = merged(base, s, half)
        at = pl.ds(pl.multiple_of((l * 4 + g * 2) * HEAD, 2 * HEAD), 2 * HEAD)

        def columns(k, _):
            cols = pl.ds(pl.multiple_of(k * third, 128), third)
            yacc[:, cols] += _dot(of[...], wob[at, cols], 1, 0)

        lax.fori_loop(0, 3, columns, None)

    def finish_piece(code, last):
        _, g, what, _, _ = fields(code)
        s, half = (what // 2) % 2, what % 2
        l = 1 - c
        base = l * 2 + g
        arrivals(g, 1, what == 4, [what - 4])
        of[0 : n // 2, 0:HEAD] = merged(base, s, half)
        at = pl.ds(pl.multiple_of((l * 4 + g * 2 + s) * HEAD, HEAD), HEAD)
        tokens = pl.ds(pl.multiple_of(half * (n // 2), n // 2), n // 2)

        @pl.when(jnp.logical_not(last))
        def _():
            for k in range(3):
                cols = slice(k * third, (k + 1) * third)
                yacc[tokens, cols] += _dot(of[0 : n // 2, 0:HEAD], wob[at, cols], 1, 0)

        @pl.when(last)
        def _():
            for k in range(3):
                cols = slice(k * third, (k + 1) * third)
                y_ref[tokens, cols] = (yacc[tokens, cols] + _dot(of[0 : n // 2, 0:HEAD], wob[at, cols], 1, 0)).astype(BF)

    steps = jnp.where(z == 1, 15, jnp.where(z == 2, 13, 11))

    def drain():
        wait(ab.at[c], sent.at[0])
        for zz in range(4):
            @pl.when(z == zz)
            def _():
                wait(qb.at[0, pl.ds(0, SENT[zz])], sent.at[1])
                wait(ob.at[pl.ds(0, STAGED[zz])], sent.at[2])
                wait(ls.at[pl.ds(0, STAGED[zz])], sent.at[3])

    def step(i, _):
        code = _pick(sp, i, PLAN)

        @pl.when(code % 4 == 0)
        def _():
            task(code)

        @pl.when(code % 4 == 2)
        def _():
            finish_line(code)

        @pl.when(code % 4 == 1)
        def _():
            @pl.when((z != 1) & (i == steps - 1))
            def _():
                drain()

            finish_piece(code, i >= steps - 2)

    lax.fori_loop(0, steps, step, None)

    @pl.when(z == 1)
    def _():
        drain()


def solution(mesh):
    def step(x, gain, wq, wk, wv, wo):
        n, wide = x.shape
        half = HEAD // 2
        rate = np.float64(THETA) ** (-np.arange(half) / half)
        table = lambda places: jnp.asarray(np.stack([f(places[:, None] * rate) for f in (np.cos, np.sin)]).astype(np.float32))
        coarse, fine = table(np.arange(8 * n // FINE) * FINE), table(np.arange(FINE))
        hbm, vmem = pl.BlockSpec(memory_space=pl.ANY), pl.BlockSpec(memory_space=pltpu.VMEM)
        dma = pltpu.SemaphoreType.DMA
        return pl.pallas_call(
            kernel,
            out_shape=pltpu.VMEM((n, wide), BF),
            in_specs=[hbm] * 8,
            out_specs=vmem,
            scratch_shapes=[
                pltpu.VMEM((n, wide), BF),
                pltpu.VMEM((wide,), BF),
                pltpu.VMEM((2, 2 * n // FINE, half), F32),
                pltpu.VMEM((2, FINE, half), F32),
                pltpu.VMEM((2, n, wide), BF),
                pltpu.VMEM((2, wide, 2 * HEAD), BF),
                pltpu.VMEM((2, wide, 2 * HEAD), BF),
                pltpu.VMEM((8 * HEAD, wide), BF),
                pltpu.VMEM((2, 8, n, HEAD), BF),
                pltpu.VMEM((2, 8, HEAD, n), BF),
                pltpu.VMEM((2, 8, 2, n, HEAD), BF),
                pltpu.VMEM((16, 2, 2, HEAD, n // 2), BF),
                pltpu.VMEM((16, 8, 128), F32),
                pltpu.VMEM((8, n), F32),
                pltpu.VMEM((2, HEAD + 8, n), F32),
                pltpu.VMEM((n, 2 * HEAD), BF),
                pltpu.VMEM((n, wide), F32),
                pltpu.VMEM((2, 2 * n, half), F32),
                dma((12,)), dma((4,)), dma,
                dma((2, 3)), dma((4,)),
                dma((2,)), dma((2,)), dma((2, 5)), dma((2, 2)),
                pltpu.SemaphoreType.REGULAR, pltpu.SemaphoreType.REGULAR,
            ],
            compiler_params=pltpu.CompilerParams(collective_id=0, has_side_effects=True, vmem_limit_bytes=61 << 20),
        )(x, gain, coarse, fine, wq, wk, wv, wo)

    tokens, whole = P(("dp", "sp"), None), P(None, None)
    return jax.shard_map(
        step,
        mesh=mesh,
        in_specs=(tokens, P(None), whole, whole, whole, whole),
        out_specs=tokens,
        check_vma=False,
    )
```

```python
import functools

import jax
import jax.numpy as jnp
import numpy as np
from jax import lax
from jax.experimental import pallas as pl
from jax.experimental.pallas import tpu as pltpu
from jax.sharding import PartitionSpec as P

HEAD = 256
THETA = 10000
NEG = -1e30
LOG2E = 1.4426950408889634
FINE = 32
MESH = pl.DeviceIdType.MESH
BF, F32 = jnp.bfloat16, jnp.float32
PAIR = (0, 1)
LOCAL, REMOTE = 8, 12

FIRST = [[0, 0], [0, 0], [0, 4], [6, 4]]
STAGED = [2, 6, 4, 2]
SENT = [6, 2, 4, 4]
SIZES = (4, 2, 8, 8)


def plan(z, c):
    steps, staged = [], 0

    def step(kind, g, what, slot=0, waits=0):
        code = waits
        for field, size in reversed(list(zip((kind, g, what, slot), SIZES))):
            code = code * size + field
        steps.append(code)

    def attention(g, a, b, waits=0):
        nonlocal staged
        for q in (a, b) if c == 0 else (b, a):
            step(0, g, q, staged, waits)
            waits = 0
            staged += q != 2 * z + c

    def output(g, last=False):
        step(2, g, 0)
        for piece in range(4, 8 if last else 5):
            step(1 if last else 2, g, piece)

    if z == 0:
        attention(1, 0, 1), attention(0, 0, 1), output(1), output(0, True)
    elif z == 1:
        attention(1, 6, 7, 1), attention(1, 2, 3), attention(1, 4, 5), output(1), attention(0, 2, 3, 1), output(0, True)
    elif z == 2:
        attention(1, 4, 5), attention(0, 6, 7, 3), attention(0, 4, 5), output(0), output(1, True)
    else:
        attention(0, 6, 7), attention(1, 6, 7, 4), output(1), output(0, True)
    return steps


PLAN = [plan(z, c) for z in range(4) for c in PAIR]


def fields(code):
    got = []
    for size in SIZES:
        got.append(code % size)
        code = code // size
    return *got, code


def _dot(a, b, ca, cb):
    return lax.dot_general(a, b, (((ca,), (cb,)), ((), ())), preferred_element_type=F32)


def _pick(z, i, table):
    out = jnp.int32(0)
    for zz, row in enumerate(table):
        got = jnp.int32(0)
        for ii, value in enumerate(row):
            got = jnp.where(i == ii, jnp.int32(value), got)
        out = jnp.where(z == zz, got, out)
    return out


def kernel(x_hbm, gain_hbm, coarse_hbm, fine_hbm, wq_hbm, wk_hbm, wv_hbm, wo_hbm, y_ref,
           xb, gainb, coarse_ref, fine_ref, ab, wqb, wkvb, wob, kb, vb, qb, ob, ls, top_s, mix_s, of, yacc, cs,
           wsem, sent, arecv, krecv, qrecv, local_o, local_l, remote_o, remote_l, go, ready):
    dp, sp = lax.axis_index("dp"), lax.axis_index("sp")
    z, c = sp // 2, sp % 2
    n, wide = xb.shape
    rows = n // 4
    scale = HEAD**-0.5
    e = scale * LOG2E

    def push(src, dst, send, recv, to):
        pltpu.make_async_remote_copy(src, dst, sent.at[send], recv, device_id=(dp, to), device_id_type=MESH).start()

    def wait(ref, sem):
        pltpu.make_async_copy(ref, ref, sem).wait()

    def x_copy(i):
        at = pl.ds(i * rows, rows)
        return pltpu.make_async_copy(x_hbm.at[at], xb.at[at], wsem.at[i])

    def w_copy(hbm, dst, g, width, sem):
        at = pl.ds(pl.multiple_of((c * 2 + g) * width, width), width)
        return pltpu.make_async_copy(hbm.at[:, at], dst, sem)

    wk_copy = lambda g: w_copy(wk_hbm, wkvb.at[g, :, pl.ds(0, HEAD)], g, HEAD, wsem.at[4 + g])
    wv_copy = lambda g: w_copy(wv_hbm, wkvb.at[g, :, pl.ds(HEAD, HEAD)], g, HEAD, wsem.at[12 + g])
    wq_copy = lambda g: w_copy(wq_hbm, wqb.at[g], g, 2 * HEAD, wsem.at[6 + g])
    wo_copy = pltpu.make_async_copy(wo_hbm, wob, wsem.at[8])
    g_first = jnp.where(z == 0, 1, 0)

    count = 2 * n // FINE
    gain_copy = pltpu.make_async_copy(gain_hbm, gainb, wsem.at[9])
    tables = [pltpu.make_async_copy(fine_hbm, fine_ref, wsem.at[10]),
              pltpu.make_async_copy(coarse_hbm.at[:, pl.ds(pl.multiple_of(z * count, 8), count)], coarse_ref, wsem.at[11])]

    for copy in gain_copy, x_copy(0), wk_copy(g_first), *tables, x_copy(1), wv_copy(g_first):
        copy.start()

    barrier = pltpu.get_barrier_semaphore()

    def here_now(chip, core):
        pl.semaphore_signal(barrier, 1, device_id=(dp, 2 * chip + core), device_id_type=MESH)

    here_now(z, 1 - c)

    @pl.when(z == 0)
    def _():
        here_now(2, c)

    @pl.when(z == 1)
    def _():
        here_now(0, c)
        here_now(2, c)
        for core in PAIR:
            here_now(3, core)

    @pl.when(z == 2)
    def _():
        here_now(3, c)

    @pl.when(z >= 2)
    def _():
        for core in PAIR:
            here_now(z - 1, core)

    def send_keys(g, h, to, at):
        ref = kb.at[g, 2 * z + h, at]
        push(ref, ref, 1, krecv.at[g, z], 2 * to + c)

    def send_values(g, h, to):
        ref = vb.at[g, 2 * z + h]
        push(ref, ref, 1, krecv.at[g, z], 2 * to + c)

    def send_both(g, h, to):
        send_keys(g, h, to, pl.ds(0, n))
        send_values(g, h, to)

    def send_queries(g, h, to):
        ref = qb.at[g, 2 * z + h]
        push(ref, ref, 1, qrecv.at[2 * z + h - 4], 2 * to + c)

    def turned(t, first):
        at = pl.ds(pl.multiple_of(first, rows), t.shape[0])
        cos, sin = cs[0, at, :], cs[1, at, :]
        t = t.astype(BF).astype(F32)
        a, b = t[:, : HEAD // 2], t[:, HEAD // 2 :]
        return jnp.concatenate([a * cos - b * sin, b * cos + a * sin], -1).astype(BF)

    def send(g, gi, h, what, *more):
        for at, gg, to in ((z == 1) & (g == 0), 0, 2), ((z == 2) & (g == 1), 1, 3), ((z == 0) & (gi == 0), 1, 1):
            pl.when(at)(functools.partial(what, gg, h, to, *more))

    def keep_keys(g, gi, h, k, first):
        at = pl.ds(first, k.shape[0])
        kb[g, 2 * z + h, at, :] = turned(k, h * n + first)
        send(g, gi, h, send_keys, at)

    def keep_values(g, h, v, first):
        vb[g, 2 * z + h, :, first : first + v.shape[0]] = v.astype(BF).T

    def make_both(g, gi, h, first):
        kv = _dot(ab[h, first : first + n // 2, :], wkvb[g], 1, 0)
        keep_keys(g, gi, h, kv[:, :HEAD], first)
        keep_values(g, h, kv[:, HEAD:], first)
        if first:
            send(g, gi, h, send_values)

    def turn_table(i, _):
        fc, fs = fine_ref[0], fine_ref[1]
        cc = coarse_ref[0, pl.ds(i, 1), :]
        ss = coarse_ref[1, pl.ds(i, 1), :]
        at = pl.ds(pl.multiple_of(i * FINE, FINE), FINE)
        cs[0, at, :] = cc * fc - ss * fs
        cs[1, at, :] = ss * fc + cc * fs

    def norm(i):
        x_copy(i).wait()
        at = pl.ds(i * rows, rows)
        w = xb[at, :].astype(F32)
        ab[c, at, :] = (w * lax.rsqrt(jnp.mean(w * w, -1, keepdims=True) + 1e-6) * gain).astype(BF)

    gain_copy.wait()
    gain = gainb[...].astype(F32)[None, :]
    for i in PAIR:
        norm(i)
        x_copy(2 + i).start()
        if i == 0:
            for copy in tables:
                copy.wait()
            lax.fori_loop(0, count, turn_table, None, unroll=8)
            wk_copy(g_first).wait()
            pl.semaphore_wait(barrier, _pick(0, z, [[2, 3, 5, 4]]))
        keep_keys(g_first, 0, c, _dot(ab[c, i * rows : (i + 1) * rows, :], wkvb[g_first, :, :HEAD], 1, 0), i * rows)

    @pl.when(z == 2)
    def _():
        pl.semaphore_signal(ready, 1, device_id=(dp, c), device_id_type=MESH)

    @pl.when(z == 3)
    def _():
        for core in PAIR:
            pl.semaphore_signal(ready, 1, device_id=(dp, 2 + core), device_id_type=MESH)

    wv_copy(g_first).wait()
    keep_values(g_first, c, _dot(ab[c, : n // 2, :], wkvb[g_first, :, HEAD:], 1, 0), 0)
    for i in PAIR:
        norm(2 + i)
    push(ab.at[c], ab.at[c], 0, arecv, z * 2 + 1 - c)
    make_both(g_first, 0, c, n // 2)
    wk_copy(1 - g_first).start()
    wv_copy(1 - g_first).start()
    wq_copy(1).start()
    wq_copy(0).start()

    def project(hh, _):
        h = jnp.where(hh == 0, c, 1 - c)

        @pl.when(hh == 1)
        def _():
            wait(ab.at[1 - c], arecv)
            wo_copy.start()

        def keys(gi, _):
            g = jnp.where(gi == 0, g_first, 1 - g_first)

            @pl.when(hh == 0)
            def _():
                wk_copy(g).wait()
                wv_copy(g).wait()

            for r in PAIR:
                make_both(g, gi, h, r * (n // 2))

            @pl.when((z == 0) & (gi == 1))
            def _():
                @pl.when(hh == 0)
                def _():
                    pl.semaphore_wait(ready, 1)

                send_both(0, h, 2)

                @pl.when(hh == 1)
                def _():
                    send_both(0, c, 1)
                    send_both(0, 1 - c, 1)

        lax.fori_loop(jnp.where(hh == 0, 1, 0), 2, keys, None)

        def queries(gi, _):
            g = 1 - gi

            @pl.when(hh == 0)
            def _():
                wq_copy(g).wait()

            q = _dot(ab[h], wqb[g], 1, 0)
            for s in PAIR:
                qb[g, 2 * z + h, s] = turned(q[:, s * HEAD : (s + 1) * HEAD], h * n)

            @pl.when((z == 3) & (g == 1))
            def _():
                send_queries(1, h, 1)

            @pl.when((z == 3) & (hh == 1) & (g == 0))
            def _():
                send_queries(0, c, 2)
                send_queries(0, 1 - c, 2)

        lax.fori_loop(0, 2, queries, None)

    lax.fori_loop(0, 2, project, None)
    yacc[...] = xb[...].astype(F32)

    for l in range(2):
        for g in PAIR:
            @pl.when((z < 2) | ((z == 2) & (g == 0)))
            def _():
                ob[REMOTE + l * 2 + g] = jnp.zeros(ob.shape[1:], BF)
                ls[REMOTE + l * 2 + g] = jnp.full(ls.shape[1:], NEG, F32)

    ones = jnp.ones((8, n), BF)

    wo_copy.wait()

    def task(code):
        _, g, q, t, waits = fields(code)
        local = q // 2 == z
        first = _pick(z, g, FIRST)
        def q_wait(qq):
            wait(qb.at[g, qq], qrecv.at[qq - 4])

        @pl.when((z == 1) & (waits > 0) & (g == 1))
        def _():
            q_wait(6)
            q_wait(7)
            pl.semaphore_wait(ready, 2)
            pl.semaphore_signal(go, 1, device_id=(dp, sp + 2), device_id_type=MESH)

        @pl.when((z == 2) & (waits > 0))
        def _():
            pl.semaphore_wait(go, 1)
            send_queries(1, c, 1)
            send_queries(1, 1 - c, 1)

        @pl.when(jnp.logical_not(local) & ((z == 2) | (q < 6)))
        def _():
            q_wait(q)

        for o in range(3):
            @pl.when((waits // 2**o) % 2 == 1)
            def _():
                wait(kb.at[g, pl.ds(0, 4)], krecv.at[g, o])

        top_s[...] = jnp.full(top_s.shape, NEG, F32)
        mix_s[...] = jnp.zeros(mix_s.shape, F32)

        def block(j, masked):
            scores = [_dot(kb[g, j], qb[g, q, s], 1, 1) for s in range(2)]
            weights, keeps = [], []
            for s in PAIR:
                score = scores[s]
                if masked:
                    ok = lax.broadcasted_iota(jnp.int32, (n, n), 0) <= lax.broadcasted_iota(jnp.int32, (n, n), 1)
                    score = jnp.where(ok, score, 2 * NEG)
                old = top_s[s : s + 1, :]
                top = jnp.maximum(old, score.max(axis=0, keepdims=True))
                top_s[s : s + 1, :] = top
                weights.append(jnp.exp2((score - top) * e).astype(BF))
                keeps.append(jnp.exp2((old - top) * e))
            values = jnp.concatenate([vb[g, j], ones], axis=0)
            for s in PAIR:
                mix_s[s] = mix_s[s] * keeps[s] + _dot(values, weights[s], 1, 0)

        lax.fori_loop(first, jnp.minimum(q, 2 * z + 2), lambda j, _: block(j, False), None)

        @pl.when(local)
        def _():
            block(q, True)

        slot = jnp.where(local, LOCAL, REMOTE) + c * 2 + g
        here = jnp.where(q == sp, slot, t)
        for s in PAIR:
            total = mix_s[s, HEAD : HEAD + 1, :]
            o = (mix_s[s, :HEAD, :] * (1 / total)).astype(BF)
            for half in PAIR:
                ob[here, s, half] = o[:, half * n // 2 : (half + 1) * n // 2]
            lse = top_s[s : s + 1, :] * e + jnp.log2(total)
            per = n // 128
            for i in range(per):
                ls[here, s * per + i : s * per + i + 1, :] = lse[:, i * 128 : (i + 1) * 128]

        @pl.when(local & (q != sp))
        def _():
            push(ls.at[t], ls.at[slot], 3, local_l.at[g], q)
            push(ob.at[t], ob.at[slot], 2, local_o.at[g], q)

        @pl.when(jnp.logical_not(local))
        def _():
            own = q % 2 == c
            push(ls.at[t], ls.at[slot], 3, remote_l.at[g, jnp.where(own, 0, 1)], q)

            @pl.when(own)
            def _():
                push(ob.at[t], ob.at[slot], 2, remote_o.at[g, 0], q)

            @pl.when(jnp.logical_not(own))
            def _():
                for s in PAIR:
                    for half in PAIR:
                        push(ob.at[t, s, half], ob.at[slot, s, half], 2, remote_o.at[g, 1 + 2 * s + half], q)

    def merged(base, s, half):
        per = n // 256
        la, lb = (jnp.concatenate([ls[at + base, pl.ds((2 * s + half) * per + k, 1), :] for k in range(per)], axis=1) for at in (LOCAL, REMOTE))
        m = jnp.maximum(la, lb)
        wa, wb = jnp.exp2(la - m), jnp.exp2(lb - m)
        r = 1 / (wa + wb)
        o = ob[LOCAL + base, s, half].astype(F32) * (wa * r) + ob[REMOTE + base, s, half].astype(F32) * (wb * r)
        return o.T.astype(BF)

    def arrivals(g, other, first, pieces):
        piece = ob.at[0, 0, 0]

        @pl.when(first & (other == 1))
        def _():
            wait(ls.at[0], local_l.at[g])
            wait(ob.at[0], local_o.at[g])

        @pl.when((z == 3) | ((z == 2) & (g == 1)))
        def _():
            @pl.when(first)
            def _():
                wait(ls.at[0], remote_l.at[g, other])

            @pl.when(other == 0)
            def _():
                wait(ob.at[0], remote_o.at[g, 0])

            @pl.when(other == 1)
            def _():
                for i in pieces:
                    wait(piece, remote_o.at[g, 1 + i])

    third = wide // 3

    def finish_line(code):
        _, g, what, _, _ = fields(code)
        other = what // 4
        l = (c + other) % 2
        base = l * 2 + g
        arrivals(g, other, True, range(4))
        for s in PAIR:
            for half in PAIR:
                of[half * (n // 2) : (half + 1) * (n // 2), s * HEAD : (s + 1) * HEAD] = merged(base, s, half)
        at = pl.ds(pl.multiple_of((l * 4 + g * 2) * HEAD, 2 * HEAD), 2 * HEAD)

        def columns(k, _):
            cols = pl.ds(pl.multiple_of(k * third, 128), third)
            yacc[:, cols] += _dot(of[...], wob[at, cols], 1, 0)

        lax.fori_loop(0, 3, columns, None)

    def finish_piece(code, last):
        _, g, what, _, _ = fields(code)
        s, half = (what // 2) % 2, what % 2
        l = 1 - c
        base = l * 2 + g
        arrivals(g, 1, what == 4, [what - 4])
        of[0 : n // 2, 0:HEAD] = merged(base, s, half)
        at = pl.ds(pl.multiple_of((l * 4 + g * 2 + s) * HEAD, HEAD), HEAD)
        tokens = pl.ds(pl.multiple_of(half * (n // 2), n // 2), n // 2)

        @pl.when(jnp.logical_not(last))
        def _():
            for k in range(3):
                cols = slice(k * third, (k + 1) * third)
                yacc[tokens, cols] += _dot(of[0 : n // 2, 0:HEAD], wob[at, cols], 1, 0)

        @pl.when(last)
        def _():
            for k in range(3):
                cols = slice(k * third, (k + 1) * third)
                y_ref[tokens, cols] = (yacc[tokens, cols] + _dot(of[0 : n // 2, 0:HEAD], wob[at, cols], 1, 0)).astype(BF)

    steps = jnp.where(z == 1, 15, jnp.where(z == 2, 13, 11))

    def drain():
        wait(ab.at[c], sent.at[0])
        for zz in range(4):
            @pl.when(z == zz)
            def _():
                wait(qb.at[0, pl.ds(0, SENT[zz])], sent.at[1])
                wait(ob.at[pl.ds(0, STAGED[zz])], sent.at[2])
                wait(ls.at[pl.ds(0, STAGED[zz])], sent.at[3])

    def step(i, _):
        code = _pick(sp, i, PLAN)

        @pl.when(code % 4 == 0)
        def _():
            task(code)

        @pl.when(code % 4 == 2)
        def _():
            finish_line(code)

        @pl.when(code % 4 == 1)
        def _():
            @pl.when((z != 1) & (i == steps - 1))
            def _():
                drain()

            finish_piece(code, i >= steps - 2)

    lax.fori_loop(0, steps, step, None)

    @pl.when(z == 1)
    def _():
        drain()


def solution(mesh):
    def step(x, gain, wq, wk, wv, wo):
        n, wide = x.shape
        half = HEAD // 2
        rate = np.float64(THETA) ** (-np.arange(half) / half)
        table = lambda places: jnp.asarray(np.stack([f(places[:, None] * rate) for f in (np.cos, np.sin)]).astype(np.float32))
        coarse, fine = table(np.arange(8 * n // FINE) * FINE), table(np.arange(FINE))
        hbm, vmem = pl.BlockSpec(memory_space=pl.ANY), pl.BlockSpec(memory_space=pltpu.VMEM)
        dma = pltpu.SemaphoreType.DMA
        return pl.pallas_call(
            kernel,
            out_shape=pltpu.VMEM((n, wide), BF),
            in_specs=[hbm] * 8,
            out_specs=vmem,
            scratch_shapes=[
                pltpu.VMEM((n, wide), BF),
                pltpu.VMEM((wide,), BF),
                pltpu.VMEM((2, 2 * n // FINE, half), F32),
                pltpu.VMEM((2, FINE, half), F32),
                pltpu.VMEM((2, n, wide), BF),
                pltpu.VMEM((2, wide, 2 * HEAD), BF),
                pltpu.VMEM((2, wide, 2 * HEAD), BF),
                pltpu.VMEM((8 * HEAD, wide), BF),
                pltpu.VMEM((2, 8, n, HEAD), BF),
                pltpu.VMEM((2, 8, HEAD, n), BF),
                pltpu.VMEM((2, 8, 2, n, HEAD), BF),
                pltpu.VMEM((16, 2, 2, HEAD, n // 2), BF),
                pltpu.VMEM((16, 8, 128), F32),
                pltpu.VMEM((8, n), F32),
                pltpu.VMEM((2, HEAD + 8, n), F32),
                pltpu.VMEM((n, 2 * HEAD), BF),
                pltpu.VMEM((n, wide), F32),
                pltpu.VMEM((2, 2 * n, half), F32),
                dma((14,)), dma((4,)), dma,
                dma((2, 3)), dma((4,)),
                dma((2,)), dma((2,)), dma((2, 5)), dma((2, 2)),
                pltpu.SemaphoreType.REGULAR, pltpu.SemaphoreType.REGULAR,
            ],
            compiler_params=pltpu.CompilerParams(collective_id=0, has_side_effects=True, vmem_limit_bytes=61 << 20),
        )(x, gain, coarse, fine, wq, wk, wv, wo)

    tokens, whole = P(("dp", "sp"), None), P(None, None)
    return jax.shard_map(
        step,
        mesh=mesh,
        in_specs=(tokens, P(None), whole, whole, whole, whole),
        out_specs=tokens,
        check_vma=False,
    )
```

```python
import functools

import jax
import jax.numpy as jnp
import numpy as np
from jax import lax
from jax.experimental import pallas as pl
from jax.experimental.pallas import tpu as pltpu
from jax.sharding import PartitionSpec as P

HEAD = 256
THETA = 10000
NEG = -1e30
LOG2E = 1.4426950408889634
FINE = 32
MESH = pl.DeviceIdType.MESH
BF, F32 = jnp.bfloat16, jnp.float32
PAIR = (0, 1)
THIRDS = (0, 1, 2)
LOCAL, REMOTE = 8, 12

FIRST = [[0, 0], [0, 0], [0, 4], [6, 4]]
STAGED = [2, 6, 4, 2]
SENT = [6, 2, 4, 4]
SIZES = (4, 2, 8, 8)


def plan(z, c):
    steps, staged = [], 0

    def step(kind, g, what, slot=0, waits=0):
        code = waits
        for field, size in reversed(list(zip((kind, g, what, slot), SIZES))):
            code = code * size + field
        steps.append(code)

    def attention(g, a, b, waits=0):
        nonlocal staged
        for q in (a, b) if c == 0 else (b, a):
            step(0, g, q, staged, waits)
            waits = 0
            staged += q != 2 * z + c

    def output(g, last=False):
        step(2, g, 0)
        for piece in range(4, 8 if last else 5):
            step(1 if last else 2, g, piece)

    if z == 0:
        attention(1, 0, 1), attention(0, 0, 1), output(1), output(0, True)
    elif z == 1:
        attention(1, 6, 7, 1), attention(1, 2, 3), attention(1, 4, 5), output(1), attention(0, 2, 3, 1), output(0, True)
    elif z == 2:
        attention(1, 4, 5), attention(0, 6, 7, 3), attention(0, 4, 5), output(0), output(1, True)
    else:
        attention(0, 6, 7), attention(1, 6, 7, 4), output(1), output(0, True)
    return steps


PLAN = [plan(z, c) for z in range(4) for c in PAIR]


def fields(code):
    got = []
    for size in SIZES:
        got.append(code % size)
        code = code // size
    return *got, code


def _dot(a, b, ca, cb):
    return lax.dot_general(a, b, (((ca,), (cb,)), ((), ())), preferred_element_type=F32)


def _product(a, w):
    return _dot(a, w, 1, 0)


def _pick(z, i, table):
    out = jnp.int32(0)
    for zz, row in enumerate(table):
        got = jnp.int32(0)
        for ii, value in enumerate(row):
            got = jnp.where(i == ii, jnp.int32(value), got)
        out = jnp.where(z == zz, got, out)
    return out


def kernel(x_hbm, gain_hbm, coarse_hbm, fine_hbm, wq_hbm, wk_hbm, wv_hbm, wo_hbm, y_ref, yacc, o_last, w_last,
           xb, gainb, coarse_ref, fine_ref, ab, wqb, wkvb, wob, kb, vb, qb, ob, ls, top_s, mix_s, of, cs,
           wsem, sent, arecv, krecv, qrecv, local_o, local_l, remote_o, remote_l, go, ready):
    dp, sp = lax.axis_index("dp"), lax.axis_index("sp")
    z, c = sp // 2, sp % 2
    n, wide = xb.shape
    rows = n // 4
    scale = HEAD**-0.5
    e = scale * LOG2E

    def push(src, dst, send, recv, to):
        pltpu.make_async_remote_copy(src, dst, sent.at[send], recv, device_id=(dp, to), device_id_type=MESH).start()

    def wait(ref, sem):
        pltpu.make_async_copy(ref, ref, sem).wait()

    def x_copy(i):
        at = pl.ds(i * rows, rows)
        return pltpu.make_async_copy(x_hbm.at[at], xb.at[at], wsem.at[i])

    def w_copy(hbm, dst, g, width, sem):
        at = pl.ds(pl.multiple_of((c * 2 + g) * width, width), width)
        return pltpu.make_async_copy(hbm.at[:, at], dst, sem)

    wk_copy = lambda g: w_copy(wk_hbm, wkvb.at[g, :, pl.ds(0, HEAD)], g, HEAD, wsem.at[4 + g])
    wv_copy = lambda g: w_copy(wv_hbm, wkvb.at[g, :, pl.ds(HEAD, HEAD)], g, HEAD, wsem.at[12 + g])
    wq_copy = lambda g: w_copy(wq_hbm, wqb.at[g], g, 2 * HEAD, wsem.at[6 + g])
    wo_copy = pltpu.make_async_copy(wo_hbm, wob, wsem.at[8])
    g_last = jnp.where(z == 2, 1, 0)
    last_copy = pltpu.make_async_copy(wo_hbm.at[pl.ds(pl.multiple_of(((1 - c) * 4 + g_last * 2 + 1) * HEAD, HEAD), HEAD)], w_last, wsem.at[14])
    g_first = jnp.where(z == 0, 1, 0)

    count = 2 * n // FINE
    gain_copy = pltpu.make_async_copy(gain_hbm, gainb, wsem.at[9])
    tables = [pltpu.make_async_copy(fine_hbm, fine_ref, wsem.at[10]),
              pltpu.make_async_copy(coarse_hbm.at[:, pl.ds(pl.multiple_of(z * count, 8), count)], coarse_ref, wsem.at[11])]

    for copy in gain_copy, x_copy(0), wk_copy(g_first), *tables, x_copy(1), wv_copy(g_first):
        copy.start()

    barrier = pltpu.get_barrier_semaphore()

    def here_now(chip, core):
        pl.semaphore_signal(barrier, 1, device_id=(dp, 2 * chip + core), device_id_type=MESH)

    here_now(z, 1 - c)

    @pl.when(z == 0)
    def _():
        here_now(2, c)

    @pl.when(z == 1)
    def _():
        here_now(0, c)
        here_now(2, c)
        for core in PAIR:
            here_now(3, core)

    @pl.when(z == 2)
    def _():
        here_now(3, c)

    @pl.when(z >= 2)
    def _():
        for core in PAIR:
            here_now(z - 1, core)

    def send_keys(g, h, to, at):
        ref = kb.at[g, 2 * z + h, at]
        push(ref, ref, 1, krecv.at[g, z], 2 * to + c)

    def send_values(g, h, to):
        ref = vb.at[g, 2 * z + h]
        push(ref, ref, 1, krecv.at[g, z], 2 * to + c)

    def send_both(g, h, to):
        send_keys(g, h, to, pl.ds(0, n))
        send_values(g, h, to)

    def send_queries(g, h, to):
        ref = qb.at[g, 2 * z + h]
        push(ref, ref, 1, qrecv.at[2 * z + h - 4], 2 * to + c)

    def turned(t, first):
        at = pl.ds(pl.multiple_of(first, rows), t.shape[0])
        cos, sin = cs[0, at, :], cs[1, at, :]
        t = t.astype(BF).astype(F32)
        a, b = t[:, : HEAD // 2], t[:, HEAD // 2 :]
        return jnp.concatenate([a * cos - b * sin, b * cos + a * sin], -1).astype(BF)

    def send(g, gi, h, what, *more):
        for at, gg, to in ((z == 1) & (g == 0), 0, 2), ((z == 2) & (g == 1), 1, 3), ((z == 0) & (gi == 0), 1, 1):
            pl.when(at)(functools.partial(what, gg, h, to, *more))

    def keep_keys(g, gi, h, k, first):
        at = pl.ds(first, k.shape[0])
        kb[g, 2 * z + h, at, :] = turned(k, h * n + first)
        send(g, gi, h, send_keys, at)

    def keep_values(g, h, v, first):
        vb[g, 2 * z + h, :, first : first + v.shape[0]] = v.astype(BF).T

    def make_both(g, gi, h, first):
        kv = _product(ab[h, first : first + n // 2, :], wkvb[g])
        keep_keys(g, gi, h, kv[:, :HEAD], first)
        keep_values(g, h, kv[:, HEAD:], first)
        if first:
            send(g, gi, h, send_values)

    def turn_table(i, _):
        fc, fs = fine_ref[0], fine_ref[1]
        cc = coarse_ref[0, pl.ds(i, 1), :]
        ss = coarse_ref[1, pl.ds(i, 1), :]
        at = pl.ds(pl.multiple_of(i * FINE, FINE), FINE)
        cs[0, at, :] = cc * fc - ss * fs
        cs[1, at, :] = ss * fc + cc * fs

    def norm(i):
        x_copy(i).wait()
        at = pl.ds(i * rows, rows)
        w = xb[at, :].astype(F32)
        ab[c, at, :] = (w * lax.rsqrt(jnp.mean(w * w, -1, keepdims=True) + 1e-6) * gain).astype(BF)

    gain_copy.wait()
    gain = gainb[...].astype(F32)[None, :]
    for i in PAIR:
        norm(i)
        x_copy(2 + i).start()
        if i == 0:
            for copy in tables:
                copy.wait()
            lax.fori_loop(0, count, turn_table, None, unroll=8)
            wk_copy(g_first).wait()
            pl.semaphore_wait(barrier, _pick(0, z, [[2, 3, 5, 4]]))
        keep_keys(g_first, 0, c, _product(ab[c, i * rows : (i + 1) * rows, :], wkvb[g_first, :, :HEAD]), i * rows)

    @pl.when(z == 2)
    def _():
        pl.semaphore_signal(ready, 1, device_id=(dp, c), device_id_type=MESH)

    @pl.when(z == 3)
    def _():
        for core in PAIR:
            pl.semaphore_signal(ready, 1, device_id=(dp, 2 + core), device_id_type=MESH)

    wv_copy(g_first).wait()
    keep_values(g_first, c, _product(ab[c, : n // 2, :], wkvb[g_first, :, HEAD:]), 0)
    for i in PAIR:
        norm(2 + i)
    push(ab.at[c], ab.at[c], 0, arecv, z * 2 + 1 - c)
    make_both(g_first, 0, c, n // 2)
    wk_copy(1 - g_first).start()
    wv_copy(1 - g_first).start()
    wq_copy(1).start()
    wq_copy(0).start()

    def project(hh, _):
        h = jnp.where(hh == 0, c, 1 - c)

        @pl.when(hh == 1)
        def _():
            wait(ab.at[1 - c], arecv)
            wo_copy.start()
            last_copy.start()

        def keys(gi, _):
            g = jnp.where(gi == 0, g_first, 1 - g_first)

            @pl.when(hh == 0)
            def _():
                wk_copy(g).wait()
                wv_copy(g).wait()

            for r in PAIR:
                make_both(g, gi, h, r * (n // 2))

            @pl.when((z == 0) & (gi == 1))
            def _():
                @pl.when(hh == 0)
                def _():
                    pl.semaphore_wait(ready, 1)

                send_both(0, h, 2)

                @pl.when(hh == 1)
                def _():
                    send_both(0, c, 1)
                    send_both(0, 1 - c, 1)

        lax.fori_loop(jnp.where(hh == 0, 1, 0), 2, keys, None)

        def queries(gi, _):
            g = 1 - gi

            @pl.when(hh == 0)
            def _():
                wq_copy(g).wait()

            q = _product(ab[h], wqb[g])
            for s in PAIR:
                qb[g, 2 * z + h, s] = turned(q[:, s * HEAD : (s + 1) * HEAD], h * n)

            @pl.when((z == 3) & (g == 1))
            def _():
                send_queries(1, h, 1)

            @pl.when((z == 3) & (hh == 1) & (g == 0))
            def _():
                send_queries(0, c, 2)
                send_queries(0, 1 - c, 2)

        lax.fori_loop(0, 2, queries, None)

    lax.fori_loop(0, 2, project, None)
    yacc[...] = xb[...].astype(F32)

    for l in range(2):
        for g in PAIR:
            @pl.when((z < 2) | ((z == 2) & (g == 0)))
            def _():
                ob[REMOTE + l * 2 + g] = jnp.zeros(ob.shape[1:], BF)
                ls[REMOTE + l * 2 + g] = jnp.full(ls.shape[1:], NEG, F32)

    ones = jnp.ones((8, n), BF)

    wo_copy.wait()
    last_copy.wait()

    def task(code):
        _, g, q, t, waits = fields(code)
        local = q // 2 == z
        first = _pick(z, g, FIRST)
        def q_wait(qq):
            wait(qb.at[g, qq], qrecv.at[qq - 4])

        @pl.when((z == 1) & (waits > 0) & (g == 1))
        def _():
            q_wait(6)
            q_wait(7)
            pl.semaphore_wait(ready, 2)
            pl.semaphore_signal(go, 1, device_id=(dp, sp + 2), device_id_type=MESH)

        @pl.when((z == 2) & (waits > 0))
        def _():
            pl.semaphore_wait(go, 1)
            send_queries(1, c, 1)
            send_queries(1, 1 - c, 1)

        @pl.when(jnp.logical_not(local) & ((z == 2) | (q < 6)))
        def _():
            q_wait(q)

        for o in THIRDS:
            @pl.when((waits // 2**o) % 2 == 1)
            def _():
                wait(kb.at[g, pl.ds(0, 4)], krecv.at[g, o])

        top_s[...] = jnp.full(top_s.shape, NEG, F32)
        mix_s[...] = jnp.zeros(mix_s.shape, F32)

        def block(j, masked):
            scores = [_dot(kb[g, j], qb[g, q, s], 1, 1) for s in range(2)]
            weights, keeps = [], []
            for s in PAIR:
                score = scores[s]
                if masked:
                    ok = lax.broadcasted_iota(jnp.int32, (n, n), 0) <= lax.broadcasted_iota(jnp.int32, (n, n), 1)
                    score = jnp.where(ok, score, 2 * NEG)
                old = top_s[s : s + 1, :]
                top = jnp.maximum(old, score.max(axis=0, keepdims=True))
                top_s[s : s + 1, :] = top
                weights.append(jnp.exp2((score - top) * e).astype(BF))
                keeps.append(jnp.exp2((old - top) * e))
            values = jnp.concatenate([vb[g, j], ones], axis=0)
            for s in PAIR:
                mix_s[s] = mix_s[s] * keeps[s] + _product(values, weights[s])

        lax.fori_loop(first, jnp.minimum(q, 2 * z + 2), lambda j, _: block(j, False), None)

        @pl.when(local)
        def _():
            block(q, True)

        slot = jnp.where(local, LOCAL, REMOTE) + c * 2 + g
        here = jnp.where(q == sp, slot, t)
        for s in PAIR:
            total = mix_s[s, HEAD : HEAD + 1, :]
            o = (mix_s[s, :HEAD, :] * (1 / total)).astype(BF)
            for half in PAIR:
                ob[here, s, half] = o[:, half * n // 2 : (half + 1) * n // 2]
            lse = top_s[s : s + 1, :] * e + jnp.log2(total)
            per = n // 128
            for i in range(per):
                ls[here, s * per + i : s * per + i + 1, :] = lse[:, i * 128 : (i + 1) * 128]

        @pl.when(local & (q != sp))
        def _():
            push(ls.at[t], ls.at[slot], 3, local_l.at[g], q)
            push(ob.at[t], ob.at[slot], 2, local_o.at[g], q)

        @pl.when(jnp.logical_not(local))
        def _():
            own = q % 2 == c
            push(ls.at[t], ls.at[slot], 3, remote_l.at[g, jnp.where(own, 0, 1)], q)

            @pl.when(own)
            def _():
                push(ob.at[t], ob.at[slot], 2, remote_o.at[g, 0], q)

            @pl.when(jnp.logical_not(own))
            def _():
                for s in PAIR:
                    for half in PAIR:
                        push(ob.at[t, s, half], ob.at[slot, s, half], 2, remote_o.at[g, 1 + 2 * s + half], q)

    def merged(base, s, half):
        per = n // 256
        la, lb = (jnp.concatenate([ls[at + base, pl.ds((2 * s + half) * per + k, 1), :] for k in range(per)], axis=1) for at in (LOCAL, REMOTE))
        m = jnp.maximum(la, lb)
        wa, wb = jnp.exp2(la - m), jnp.exp2(lb - m)
        r = 1 / (wa + wb)
        o = ob[LOCAL + base, s, half].astype(F32) * (wa * r) + ob[REMOTE + base, s, half].astype(F32) * (wb * r)
        return o.T.astype(BF)

    def arrivals(g, other, first, pieces):
        piece = ob.at[0, 0, 0]

        @pl.when(first & (other == 1))
        def _():
            wait(ls.at[0], local_l.at[g])
            wait(ob.at[0], local_o.at[g])

        @pl.when((z == 3) | ((z == 2) & (g == 1)))
        def _():
            @pl.when(first)
            def _():
                wait(ls.at[0], remote_l.at[g, other])

            @pl.when(other == 0)
            def _():
                wait(ob.at[0], remote_o.at[g, 0])

            @pl.when(other == 1)
            def _():
                for i in pieces:
                    wait(piece, remote_o.at[g, 1 + i])

    third = wide // 3

    def finish_line(code):
        _, g, what, _, _ = fields(code)
        other = what // 4
        l = (c + other) % 2
        base = l * 2 + g
        arrivals(g, other, True, range(4))
        for s in PAIR:
            for half in PAIR:
                of[half * (n // 2) : (half + 1) * (n // 2), s * HEAD : (s + 1) * HEAD] = merged(base, s, half)
        at = pl.ds(pl.multiple_of((l * 4 + g * 2) * HEAD, 2 * HEAD), 2 * HEAD)

        def columns(k, _):
            cols = pl.ds(pl.multiple_of(k * third, 128), third)
            yacc[:, cols] += _product(of[...], wob[at, cols])

        lax.fori_loop(0, 3, columns, None)

    def finish_piece(code):
        _, g, what, _, _ = fields(code)
        s, half = (what // 2) % 2, what % 2
        l = 1 - c
        base = l * 2 + g
        arrivals(g, 1, what == 4, [what - 4])
        o = merged(base, s, half)
        at = pl.ds(pl.multiple_of((l * 4 + g * 2 + s) * HEAD, HEAD), HEAD)
        tokens = pl.ds(pl.multiple_of(half * (n // 2), n // 2), n // 2)

        def add(store):
            of[0 : n // 2, 0:HEAD] = o
            for k in THIRDS:
                cols = slice(k * third, (k + 1) * third)
                store(cols, yacc[tokens, cols] + _product(of[0 : n // 2, 0:HEAD], wob[at, cols]))

        @pl.when(s == 0)
        def _():
            def store(cols, y):
                yacc[tokens, cols] = y

            add(store)

        @pl.when((s == 1) & (half == 0))
        def _():
            def store(cols, y):
                y_ref[:, cols] = y.astype(BF)

            add(store)

        @pl.when((s == 1) & (half == 1))
        def _():
            o_last[...] = o

    steps = jnp.where(z == 1, 15, jnp.where(z == 2, 13, 11))

    def drain():
        wait(ab.at[c], sent.at[0])
        for zz in range(4):
            @pl.when(z == zz)
            def _():
                wait(qb.at[0, pl.ds(0, SENT[zz])], sent.at[1])
                wait(ob.at[pl.ds(0, STAGED[zz])], sent.at[2])
                wait(ls.at[pl.ds(0, STAGED[zz])], sent.at[3])

    def step(i, _):
        code = _pick(sp, i, PLAN)

        @pl.when(code % 4 == 0)
        def _():
            task(code)

        @pl.when(code % 4 == 2)
        def _():
            finish_line(code)

        @pl.when(code % 4 == 1)
        def _():
            @pl.when((z != 1) & (i == steps - 1))
            def _():
                drain()

            finish_piece(code)

    lax.fori_loop(0, steps, step, None)

    @pl.when(z == 1)
    def _():
        drain()


def write(y_ref, yacc, o_last, w_last, y_hbm, out, sem):
    n, wide = y_ref.shape
    first = pltpu.make_async_copy(y_ref, y_hbm.at[pl.ds(0, n)], sem.at[3])
    first.start()
    copies = [first]
    for k in THIRDS:
        cols = slice(k * (wide // 3), (k + 1) * (wide // 3))
        out[k] = (yacc[n:, cols] + _product(o_last[...], w_last[:, cols])).astype(BF)
        copies.append(pltpu.make_async_copy(out.at[k], y_hbm.at[pl.ds(n, n), cols], sem.at[k]))
        copies[-1].start()
    for copy in copies:
        copy.wait()


def solution(mesh):
    def step(x, gain, wq, wk, wv, wo):
        n, wide = x.shape
        half = HEAD // 2
        rate = np.float64(THETA) ** (-np.arange(half) / half)
        table = lambda places: jnp.asarray(np.stack([f(places[:, None] * rate) for f in (np.cos, np.sin)]).astype(np.float32))
        coarse, fine = table(np.arange(8 * n // FINE) * FINE), table(np.arange(FINE))
        hbm, vmem = pl.BlockSpec(memory_space=pl.ANY), pl.BlockSpec(memory_space=pltpu.VMEM)
        dma = pltpu.SemaphoreType.DMA
        parts = pl.pallas_call(
            kernel,
            out_shape=[pltpu.VMEM((n // 2, wide), BF), pltpu.VMEM((n, wide), F32), pltpu.VMEM((n // 2, HEAD), BF), pltpu.VMEM((HEAD, wide), BF)],
            in_specs=[hbm] * 8,
            out_specs=[vmem] * 4,
            scratch_shapes=[
                pltpu.VMEM((n, wide), BF),
                pltpu.VMEM((wide,), BF),
                pltpu.VMEM((2, 2 * n // FINE, half), F32),
                pltpu.VMEM((2, FINE, half), F32),
                pltpu.VMEM((2, n, wide), BF),
                pltpu.VMEM((2, wide, 2 * HEAD), BF),
                pltpu.VMEM((2, wide, 2 * HEAD), BF),
                pltpu.VMEM((8 * HEAD, wide), BF),
                pltpu.VMEM((2, 8, n, HEAD), BF),
                pltpu.VMEM((2, 8, HEAD, n), BF),
                pltpu.VMEM((2, 8, 2, n, HEAD), BF),
                pltpu.VMEM((16, 2, 2, HEAD, n // 2), BF),
                pltpu.VMEM((16, 8, 128), F32),
                pltpu.VMEM((8, n), F32),
                pltpu.VMEM((2, HEAD + 8, n), F32),
                pltpu.VMEM((n, 2 * HEAD), BF),
                pltpu.VMEM((2, 2 * n, half), F32),
                dma((15,)), dma((4,)), dma,
                dma((2, 3)), dma((4,)),
                dma((2,)), dma((2,)), dma((2, 5)), dma((2, 2)),
                pltpu.SemaphoreType.REGULAR, pltpu.SemaphoreType.REGULAR,
            ],
            compiler_params=pltpu.CompilerParams(collective_id=0, has_side_effects=True, vmem_limit_bytes=57 << 20),
        )(x, gain, coarse, fine, wq, wk, wv, wo)
        return pl.pallas_call(
            write,
            out_shape=jax.ShapeDtypeStruct((n, wide), BF),
            in_specs=[vmem] * 4,
            out_specs=hbm,
            scratch_shapes=[pltpu.VMEM((3, n // 2, wide // 3), BF), dma((4,))],
            compiler_params=pltpu.CompilerParams(vmem_limit_bytes=4 << 20),
        )(*(pltpu.with_memory_space_constraint(part, pltpu.VMEM) for part in parts))

    tokens, whole = P(("dp", "sp"), None), P(None, None)
    return jax.shard_map(
        step,
        mesh=mesh,
        in_specs=(tokens, P(None), whole, whole, whole, whole),
        out_specs=tokens,
        check_vma=False,
    )
```

```python
import functools

import jax
import jax.numpy as jnp
import numpy as np
from jax import lax
from jax.experimental import pallas as pl
from jax.experimental.pallas import tpu as pltpu
from jax.sharding import PartitionSpec as P

HEAD = 256
THETA = 10000
NEG = -1e30
LOG2E = 1.4426950408889634
FINE = 32
MESH = pl.DeviceIdType.MESH
BF, F32 = jnp.bfloat16, jnp.float32
PAIR = (0, 1)
QUARTERS = (0, 1, 2, 3)
THIRDS = (0, 1, 2)
WHOLE = 10
LOCAL, REMOTE = 8, 12

FIRST = [[0, 0], [0, 0], [0, 4], [6, 4]]
STAGED = [2, 6, 4, 2]
SENT = [6, 2, 4, 4]
SIZES = (4, 2, 8, 8)


def plan(z, c):
    steps, staged = [], 0

    def step(kind, g, what, slot=0, waits=0):
        code = waits
        for field, size in reversed(list(zip((kind, g, what, slot), SIZES))):
            code = code * size + field
        steps.append(code)

    def attention(g, a, b, waits=0):
        nonlocal staged
        for q in (a, b) if c == 0 else (b, a):
            step(0, g, q, staged, waits)
            waits = 0
            staged += q != 2 * z + c

    def output(g, last=False):
        step(2, g, 0)
        for piece in range(8) if last else [4]:
            step(1 if last else 2, g, piece)

    if z == 0:
        attention(1, 0, 1), attention(0, 0, 1), output(1), output(0, True)
    elif z == 1:
        attention(1, 6, 7, 1), attention(1, 2, 3), attention(1, 4, 5), output(1), attention(0, 2, 3, 1), output(0, True)
    elif z == 2:
        attention(1, 4, 5), attention(0, 6, 7, 3), attention(0, 4, 5), output(0), output(1, True)
    else:
        attention(0, 6, 7), attention(1, 6, 7, 4), output(1), output(0, True)
    return steps


PLAN = [plan(z, c) for z in range(4) for c in PAIR]


def fields(code):
    got = []
    for size in SIZES:
        got.append(code % size)
        code = code // size
    return *got, code


def _dot(a, b, ca, cb):
    return lax.dot_general(a, b, (((ca,), (cb,)), ((), ())), preferred_element_type=F32)


def _product(a, w):
    return _dot(a, w, 1, 0)


def _pick(z, i, table):
    out = jnp.int32(0)
    for zz, row in enumerate(table):
        got = jnp.int32(0)
        for ii, value in enumerate(row):
            got = jnp.where(i == ii, jnp.int32(value), got)
        out = jnp.where(z == zz, got, out)
    return out


def kernel(x_hbm, gain_hbm, coarse_hbm, fine_hbm, wq_hbm, wk_hbm, wv_hbm, wo_hbm, y_ref, yacc, o_last, w_last,
           xb, gainb, coarse_ref, fine_ref, ab, wqb, wkvb, wob, kb, vb, qb, ob, ls, top_s, mix_s, of, cs,
           wsem, sent, arecv, krecv, qrecv, local_o, local_l, remote_o, remote_l, go, ready):
    dp, sp = lax.axis_index("dp"), lax.axis_index("sp")
    z, c = sp // 2, sp % 2
    n, wide = xb.shape
    rows = n // 4
    scale = HEAD**-0.5
    e = scale * LOG2E

    def push(src, dst, send, recv, to):
        pltpu.make_async_remote_copy(src, dst, sent.at[send], recv, device_id=(dp, to), device_id_type=MESH).start()

    def wait(ref, sem):
        pltpu.make_async_copy(ref, ref, sem).wait()

    def x_copy(i):
        at = pl.ds(i * rows, rows)
        return pltpu.make_async_copy(x_hbm.at[at], xb.at[at], wsem.at[i % 2])

    def w_copy(hbm, dst, g, width, sem):
        at = pl.ds(pl.multiple_of((c * 2 + g) * width, width), width)
        return pltpu.make_async_copy(hbm.at[:, at], dst, sem)

    wk_copy = lambda g: w_copy(wk_hbm, wkvb.at[g, :, pl.ds(0, HEAD)], g, HEAD, wsem.at[5 + g])
    wv_copy = lambda g: w_copy(wv_hbm, wkvb.at[g, :, pl.ds(HEAD, HEAD)], g, HEAD, wsem.at[7 + g])
    wq_copy = lambda g: w_copy(wq_hbm, wqb.at[g], g, 2 * HEAD, wsem.at[2 + g])
    wo_copy = pltpu.make_async_copy(wo_hbm, wob, wsem.at[0])
    g_last = jnp.where(z == 2, 1, 0)
    last_copy = pltpu.make_async_copy(wo_hbm.at[pl.ds(pl.multiple_of(((1 - c) * 4 + g_last * 2 + 1) * HEAD, HEAD), HEAD)], w_last, wsem.at[1])
    g_first = jnp.where(z == 0, 1, 0)

    count = 2 * n // FINE
    gain_copy = pltpu.make_async_copy(gain_hbm, gainb, wsem.at[2])
    tables = [pltpu.make_async_copy(fine_hbm, fine_ref, wsem.at[3]),
              pltpu.make_async_copy(coarse_hbm.at[:, pl.ds(pl.multiple_of(z * count, 8), count)], coarse_ref, wsem.at[4])]

    for copy in gain_copy, *tables, x_copy(0), wk_copy(g_first), x_copy(1), wv_copy(g_first):
        copy.start()

    barrier = pltpu.get_barrier_semaphore()

    def here_now(chip, core):
        pl.semaphore_signal(barrier, 1, device_id=(dp, 2 * chip + core), device_id_type=MESH)

    here_now(z, 1 - c)

    @pl.when(z == 0)
    def _():
        here_now(2, c)

    @pl.when(z == 1)
    def _():
        here_now(0, c)
        here_now(2, c)
        for core in PAIR:
            here_now(3, core)

    @pl.when(z == 2)
    def _():
        here_now(3, c)

    @pl.when(z >= 2)
    def _():
        for core in PAIR:
            here_now(z - 1, core)

    def send_keys(g, h, to, at):
        ref = kb.at[g, 2 * z + h, at]
        push(ref, ref, 1, krecv.at[g if to == 1 else z % 2], 2 * to + c)

    def send_values(g, h, to):
        ref = vb.at[g, 2 * z + h]
        push(ref, ref, 1, krecv.at[g if to == 1 else z % 2], 2 * to + c)

    def send_both(g, h, to):
        send_keys(g, h, to, pl.ds(0, n))
        send_values(g, h, to)

    def send_queries(g, h, to):
        ref = qb.at[g, 2 * z + h]
        push(ref, ref, 1, qrecv.at[2 * z + h - 4], 2 * to + c)

    def turned(t, first):
        at = pl.ds(pl.multiple_of(first, rows), t.shape[0])
        cos, sin = cs[0, at, :], cs[1, at, :]
        t = t.astype(BF).astype(F32)
        a, b = t[:, : HEAD // 2], t[:, HEAD // 2 :]
        return jnp.concatenate([a * cos - b * sin, b * cos + a * sin], -1).astype(BF)

    def send(g, gi, h, what, *more):
        for at, gg, to in ((z == 1) & (g == 0), 0, 2), ((z == 2) & (g == 1), 1, 3), ((z == 0) & (gi == 0), 1, 1):
            pl.when(at)(functools.partial(what, gg, h, to, *more))

    def keep_keys(g, gi, h, k, first, greet=False):
        at = pl.ds(first, k.shape[0])
        kb[g, 2 * z + h, at, :] = turned(k, h * n + first)
        if greet:
            pl.semaphore_wait(barrier, _pick(0, z, [[2, 3, 5, 4]]))
        send(g, gi, h, send_keys, at)

    def keep_values(g, h, v, first):
        vb[g, 2 * z + h, :, first : first + v.shape[0]] = v.astype(BF).T

    def make_both(g, gi, h, first):
        kv = _product(ab[h, first : first + n // 2, :], wkvb[g])
        keep_keys(g, gi, h, kv[:, :HEAD], first)
        keep_values(g, h, kv[:, HEAD:], first)
        if first:
            send(g, gi, h, send_values)

    def turn_table(i, _):
        fc, fs = fine_ref[0], fine_ref[1]
        cc = coarse_ref[0, pl.ds(i, 1), :]
        ss = coarse_ref[1, pl.ds(i, 1), :]
        at = pl.ds(pl.multiple_of(i * FINE, FINE), FINE)
        cs[0, at, :] = cc * fc - ss * fs
        cs[1, at, :] = ss * fc + cc * fs

    def norm(i):
        x_copy(i).wait()
        at = pl.ds(i * rows, rows)
        w = xb[at, :].astype(F32)
        ab[c, at, :] = (w * lax.rsqrt(jnp.mean(w * w, -1, keepdims=True) + 1e-6) * gain).astype(BF)

    for copy in gain_copy, *tables:
        copy.wait()
    lax.fori_loop(0, count, turn_table, None, unroll=8)
    gain = gainb[...].astype(F32)[None, :]
    for i in PAIR:
        norm(i)
        x_copy(2 + i).start()
        if i == 0:
            wk_copy(g_first).wait()
        k = _product(ab[c, i * rows : (i + 1) * rows, :], wkvb[g_first, :, :HEAD])
        keep_keys(g_first, 0, c, k, i * rows, i == 0)

    @pl.when(z == 2)
    def _():
        pl.semaphore_signal(ready, 1, device_id=(dp, c), device_id_type=MESH)

    @pl.when(z == 3)
    def _():
        for core in PAIR:
            pl.semaphore_signal(ready, 1, device_id=(dp, 2 + core), device_id_type=MESH)

    wv_copy(g_first).wait()
    keep_values(g_first, c, _product(ab[c, : n // 2, :], wkvb[g_first, :, HEAD:]), 0)
    for i in PAIR:
        norm(2 + i)
    push(ab.at[c], ab.at[c], 0, arecv, z * 2 + 1 - c)
    make_both(g_first, 0, c, n // 2)
    wk_copy(1 - g_first).start()
    wv_copy(1 - g_first).start()
    wq_copy(1).start()
    wq_copy(0).start()

    def project(hh, _):
        h = jnp.where(hh == 0, c, 1 - c)

        @pl.when(hh == 1)
        def _():
            wait(ab.at[1 - c], arecv)
            wo_copy.start()
            last_copy.start()

        def keys(gi, _):
            g = jnp.where(gi == 0, g_first, 1 - g_first)

            @pl.when(hh == 0)
            def _():
                wk_copy(g).wait()
                wv_copy(g).wait()

            for r in PAIR:
                make_both(g, gi, h, r * (n // 2))

            @pl.when((z == 0) & (gi == 1))
            def _():
                @pl.when(hh == 0)
                def _():
                    pl.semaphore_wait(ready, 1)

                send_both(0, h, 2)

                @pl.when(hh == 1)
                def _():
                    send_both(0, c, 1)
                    send_both(0, 1 - c, 1)

        lax.fori_loop(jnp.where(hh == 0, 1, 0), 2, keys, None)

        def queries(gi, _):
            g = 1 - gi

            @pl.when(hh == 0)
            def _():
                wq_copy(g).wait()

            q = _product(ab[h], wqb[g])
            for s in PAIR:
                qb[g, 2 * z + h, s] = turned(q[:, s * HEAD : (s + 1) * HEAD], h * n)

            @pl.when((z == 3) & (g == 1))
            def _():
                send_queries(1, h, 1)

            @pl.when((z == 3) & (hh == 1) & (g == 0))
            def _():
                send_queries(0, c, 2)
                send_queries(0, 1 - c, 2)

        lax.fori_loop(0, 2, queries, None)

    lax.fori_loop(0, 2, project, None)
    yacc[...] = xb[...].astype(F32)

    for l in range(2):
        for g in PAIR:
            @pl.when((z < 2) | ((z == 2) & (g == 0)))
            def _():
                ob[REMOTE + l * 2 + g] = jnp.zeros(ob.shape[1:], BF)
                ls[REMOTE + l * 2 + g] = jnp.full(ls.shape[1:], NEG, F32)

    ones = jnp.ones((8, n), BF)

    wo_copy.wait()
    last_copy.wait()

    def task(code):
        _, g, q, t, waits = fields(code)
        local = q // 2 == z
        first = _pick(z, g, FIRST)
        def q_wait(qq):
            wait(qb.at[g, qq], qrecv.at[qq - 4])

        @pl.when((z == 1) & (waits > 0) & (g == 1))
        def _():
            q_wait(6)
            q_wait(7)
            pl.semaphore_wait(ready, 2)
            pl.semaphore_signal(go, 1, device_id=(dp, sp + 2), device_id_type=MESH)

        @pl.when((z == 2) & (waits > 0))
        def _():
            pl.semaphore_wait(go, 1)
            send_queries(1, c, 1)
            send_queries(1, 1 - c, 1)

        @pl.when(jnp.logical_not(local) & ((z == 2) | (q < 6)))
        def _():
            q_wait(q)

        for o in THIRDS:
            @pl.when((waits // 2**o) % 2 == 1)
            def _():
                wait(kb.at[g, pl.ds(0, 4)], krecv.at[jnp.where(z == 1, g, o % 2)])

        top_s[...] = jnp.full(top_s.shape, NEG, F32)
        mix_s[...] = jnp.zeros(mix_s.shape, F32)

        def block(j, masked):
            scores = [_dot(kb[g, j], qb[g, q, s], 1, 1) for s in range(2)]
            weights, keeps = [], []
            for s in PAIR:
                score = scores[s]
                if masked:
                    ok = lax.broadcasted_iota(jnp.int32, (n, n), 0) <= lax.broadcasted_iota(jnp.int32, (n, n), 1)
                    score = jnp.where(ok, score, 2 * NEG)
                old = top_s[s : s + 1, :]
                top = jnp.maximum(old, score.max(axis=0, keepdims=True))
                top_s[s : s + 1, :] = top
                weights.append(jnp.exp2((score - top) * e).astype(BF))
                keeps.append(jnp.exp2((old - top) * e))
            values = jnp.concatenate([vb[g, j], ones], axis=0)
            for s in PAIR:
                mix_s[s] = mix_s[s] * keeps[s] + _product(values, weights[s])

        lax.fori_loop(first, jnp.minimum(q, 2 * z + 2), lambda j, _: block(j, False), None)

        @pl.when(local)
        def _():
            block(q, True)

        slot = jnp.where(local, LOCAL, REMOTE) + c * 2 + g
        here = jnp.where(q == sp, slot, t)
        for s in PAIR:
            total = mix_s[s, HEAD : HEAD + 1, :]
            o = (mix_s[s, :HEAD, :] * (1 / total)).astype(BF)
            for part in QUARTERS:
                ob[here, s, part] = o[:, part * rows : (part + 1) * rows]
            lse = top_s[s : s + 1, :] * e + jnp.log2(total)
            for part in QUARTERS:
                row = 4 * s + part
                ls[here, row : row + 1, :] = lse[:, part * rows : (part + 1) * rows]

        @pl.when(local & (q != sp))
        def _():
            push(ls.at[t], ls.at[slot], 3, local_l.at[g], q)
            push(ob.at[t], ob.at[slot], 2, local_o.at[g], q)

        @pl.when(jnp.logical_not(local))
        def _():
            own = q % 2 == c
            push(ls.at[t], ls.at[slot], 3, remote_l.at[g, jnp.where(own, 0, 1)], q)

            last = (g == 1) == (q // 2 == 2)

            @pl.when(own | jnp.logical_not(last))
            def _():
                push(ob.at[t], ob.at[slot], 2, remote_o.at[jnp.where(own, g, WHOLE)], q)

            @pl.when(jnp.logical_not(own) & last)
            def _():
                for s in PAIR:
                    for part in QUARTERS:
                        push(ob.at[t, s, part], ob.at[slot, s, part], 2, remote_o.at[2 + 4 * s + part], q)

    def merged(base, s, part):
        la, lb = (ls[at + base, pl.ds(4 * s + part, 1), :] for at in (LOCAL, REMOTE))
        m = jnp.maximum(la, lb)
        wa, wb = jnp.exp2(la - m), jnp.exp2(lb - m)
        r = 1 / (wa + wb)
        o = ob[LOCAL + base, s, part].astype(F32) * (wa * r) + ob[REMOTE + base, s, part].astype(F32) * (wb * r)
        return o.T.astype(BF)

    def arrivals(g, other, first, what, sem):
        @pl.when(first & (other == 1))
        def _():
            wait(ls.at[0], local_l.at[g])
            wait(ob.at[0], local_o.at[g])

        @pl.when((z == 3) | ((z == 2) & (g == 1)))
        def _():
            @pl.when(first)
            def _():
                wait(ls.at[0], remote_l.at[g, other])

            wait(what, remote_o.at[sem])

    third = wide // 3

    def finish_line(code):
        _, g, what, _, _ = fields(code)
        other = what // 4
        l = (c + other) % 2
        base = l * 2 + g
        arrivals(g, other, True, ob.at[0], jnp.where(other == 0, g, WHOLE))
        for s in PAIR:
            for part in QUARTERS:
                of[part * rows : (part + 1) * rows, s * HEAD : (s + 1) * HEAD] = merged(base, s, part)
        at = pl.ds(pl.multiple_of((l * 4 + g * 2) * HEAD, 2 * HEAD), 2 * HEAD)

        def columns(k, _):
            cols = pl.ds(pl.multiple_of(k * third, 128), third)
            yacc[:, cols] += _product(of[...], wob[at, cols])

        lax.fori_loop(0, 3, columns, None)

    def finish_piece(code):
        _, g, what, _, _ = fields(code)
        s, part = what // 4, what % 4
        l = 1 - c
        base = l * 2 + g
        arrivals(g, 1, what == 0, ob.at[0, 0, 0], 2 + what)
        o = merged(base, s, part)
        at = pl.ds(pl.multiple_of((l * 4 + g * 2 + s) * HEAD, HEAD), HEAD)
        tokens = pl.ds(pl.multiple_of(part * rows, rows), rows)

        def add(store):
            of[0:rows, 0:HEAD] = o
            for k in THIRDS:
                cols = slice(k * third, (k + 1) * third)
                store(cols, yacc[tokens, cols] + _product(of[0:rows, 0:HEAD], wob[at, cols]))

        @pl.when(s == 0)
        def _():
            def store(cols, y):
                yacc[tokens, cols] = y

            add(store)

        @pl.when((s == 1) & (part < 3))
        def _():
            def store(cols, y):
                y_ref[tokens, cols] = y.astype(BF)

            add(store)

        @pl.when((s == 1) & (part == 3))
        def _():
            o_last[...] = o

    steps = jnp.where(z == 1, 19, jnp.where(z == 2, 17, 15))

    def drain():
        wait(ab.at[c], sent.at[0])
        for zz in range(4):
            @pl.when(z == zz)
            def _():
                wait(qb.at[0, pl.ds(0, SENT[zz])], sent.at[1])
                wait(ob.at[pl.ds(0, STAGED[zz])], sent.at[2])
                wait(ls.at[pl.ds(0, STAGED[zz])], sent.at[3])

    def step(i, _):
        code = _pick(sp, i, PLAN)

        @pl.when(code % 4 == 0)
        def _():
            task(code)

        @pl.when(code % 4 == 2)
        def _():
            finish_line(code)

        @pl.when(code % 4 == 1)
        def _():
            @pl.when((z != 1) & (i == steps - 1))
            def _():
                drain()

            finish_piece(code)

    lax.fori_loop(0, steps, step, None)

    @pl.when(z == 1)
    def _():
        drain()


def write(y_ref, yacc, o_last, w_last, y_hbm, out, sem):
    n, wide = y_ref.shape
    first = pltpu.make_async_copy(y_ref, y_hbm.at[pl.ds(0, n)], sem.at[3])
    first.start()
    copies = [first]
    for k in THIRDS:
        cols = slice(k * (wide // 3), (k + 1) * (wide // 3))
        out[k] = (yacc[n:, cols] + _product(o_last[...], w_last[:, cols])).astype(BF)
        copies.append(pltpu.make_async_copy(out.at[k], y_hbm.at[pl.ds(n, n // 3), cols], sem.at[k]))
        copies[-1].start()
    for copy in copies:
        copy.wait()


def solution(mesh):
    def step(x, gain, wq, wk, wv, wo):
        n, wide = x.shape
        half = HEAD // 2
        rate = np.float64(THETA) ** (-np.arange(half) / half)
        table = lambda places: jnp.asarray(np.stack([f(places[:, None] * rate) for f in (np.cos, np.sin)]).astype(np.float32))
        coarse, fine = table(np.arange(8 * n // FINE) * FINE), table(np.arange(FINE))
        hbm, vmem = pl.BlockSpec(memory_space=pl.ANY), pl.BlockSpec(memory_space=pltpu.VMEM)
        dma = pltpu.SemaphoreType.DMA
        parts = pl.pallas_call(
            kernel,
            out_shape=[pltpu.VMEM((3 * n // 4, wide), BF), pltpu.VMEM((n, wide), F32), pltpu.VMEM((n // 4, HEAD), BF), pltpu.VMEM((HEAD, wide), BF)],
            in_specs=[hbm] * 8,
            out_specs=[vmem] * 4,
            scratch_shapes=[
                pltpu.VMEM((n, wide), BF),
                pltpu.VMEM((wide,), BF),
                pltpu.VMEM((2, 2 * n // FINE, half), F32),
                pltpu.VMEM((2, FINE, half), F32),
                pltpu.VMEM((2, n, wide), BF),
                pltpu.VMEM((2, wide, 2 * HEAD), BF),
                pltpu.VMEM((2, wide, 2 * HEAD), BF),
                pltpu.VMEM((8 * HEAD, wide), BF),
                pltpu.VMEM((2, 8, n, HEAD), BF),
                pltpu.VMEM((2, 8, HEAD, n), BF),
                pltpu.VMEM((2, 8, 2, n, HEAD), BF),
                pltpu.VMEM((16, 2, 4, HEAD, n // 4), BF),
                pltpu.VMEM((16, 8, 128), F32),
                pltpu.VMEM((8, n), F32),
                pltpu.VMEM((2, HEAD + 8, n), F32),
                pltpu.VMEM((n, 2 * HEAD), BF),
                pltpu.VMEM((2, 2 * n, half), F32),
                dma((9,)), dma((4,)), dma,
                dma((2,)), dma((4,)),
                dma((2,)), dma((2,)), dma((11,)), dma((2, 2)),
                pltpu.SemaphoreType.REGULAR, pltpu.SemaphoreType.REGULAR,
            ],
            compiler_params=pltpu.CompilerParams(collective_id=0, has_side_effects=True, vmem_limit_bytes=55 << 20),
        )(x, gain, coarse, fine, wq, wk, wv, wo)
        return pl.pallas_call(
            write,
            out_shape=jax.ShapeDtypeStruct((n, wide), BF),
            in_specs=[vmem] * 4,
            out_specs=hbm,
            scratch_shapes=[pltpu.VMEM((3, n // 4, wide // 3), BF), dma((4,))],
            compiler_params=pltpu.CompilerParams(vmem_limit_bytes=4 << 20),
        )(*(pltpu.with_memory_space_constraint(part, pltpu.VMEM) for part in parts))

    tokens, whole = P(("dp", "sp"), None), P(None, None)
    return jax.shard_map(
        step,
        mesh=mesh,
        in_specs=(tokens, P(None), whole, whole, whole, whole),
        out_specs=tokens,
        check_vma=False,
    )
```

```python
import functools

import jax
import jax.numpy as jnp
import numpy as np
from jax import lax
from jax.experimental import pallas as pl
from jax.experimental.pallas import tpu as pltpu
from jax.sharding import PartitionSpec as P

HEAD = 256
THETA = 10000
LOWEST = float(np.finfo(np.float32).min)
LOG2E = 1.4426950408889634
FINE = 32
MESH = pl.DeviceIdType.MESH
BF, F32 = jnp.bfloat16, jnp.float32
PAIR = (0, 1)
QUARTERS = (0, 1, 2, 3)
THIRDS = (0, 1, 2)
WHOLE = 10
LOCAL, REMOTE = 8, 12

FIRST = [[0, 0], [0, 0], [0, 4], [6, 4]]
STAGED = [2, 6, 4, 2]
SENT = [6, 2, 4, 4]
SIZES = (4, 2, 8, 8)


def plan(z, c):
    steps, staged = [], 0

    def step(kind, g, what, slot=0, waits=0):
        code = waits
        for field, size in reversed(list(zip((kind, g, what, slot), SIZES))):
            code = code * size + field
        steps.append(code)

    def attention(g, a, b, waits=0):
        nonlocal staged
        for q in (a, b) if c == 0 else (b, a):
            step(0, g, q, staged, waits)
            waits = 0
            staged += q != 2 * z + c

    def output(g, last=False):
        step(2, g, 0)
        for piece in range(8) if last else [4]:
            step(1 if last else 2, g, piece)

    if z == 0:
        attention(1, 0, 1), attention(0, 0, 1), output(1), output(0, True)
    elif z == 1:
        attention(1, 6, 7, 1), attention(1, 2, 3), attention(1, 4, 5), output(1), attention(0, 2, 3, 1), output(0, True)
    elif z == 2:
        attention(1, 4, 5), attention(0, 6, 7, 3), attention(0, 4, 5), output(0), output(1, True)
    else:
        attention(0, 6, 7), attention(1, 6, 7, 4), output(1), output(0, True)
    return steps


PLAN = [plan(z, c) for z in range(4) for c in PAIR]


def fields(code):
    got = []
    for size in SIZES:
        got.append(code % size)
        code = code // size
    return *got, code


def _dot(a, b, ca, cb):
    return lax.dot_general(a, b, (((ca,), (cb,)), ((), ())), preferred_element_type=F32)


def _product(a, w):
    return _dot(a, w, 1, 0)


def _pick(z, i, table):
    out = jnp.int32(0)
    for zz, row in enumerate(table):
        got = jnp.int32(0)
        for ii, value in enumerate(row):
            got = jnp.where(i == ii, jnp.int32(value), got)
        out = jnp.where(z == zz, got, out)
    return out


def kernel(x_hbm, gain_hbm, coarse_hbm, fine_hbm, wq_hbm, wk_hbm, wv_hbm, wo_hbm, y_ref, yacc, o_last, w_last,
           xb, gainb, coarse_ref, fine_ref, ab, wqb, wkvb, wob, kb, vb, qb, ob, ls, top_s, mix_s, of, cs,
           wsem, sent, arecv, krecv, qrecv, local_o, local_l, remote_o, remote_l, go, ready):
    dp, sp = lax.axis_index("dp"), lax.axis_index("sp")
    z, c = sp // 2, sp % 2
    n, wide = xb.shape
    rows = n // 4
    scale = HEAD**-0.5
    e = scale * LOG2E

    def push(src, dst, send, recv, to):
        pltpu.make_async_remote_copy(src, dst, sent.at[send], recv, device_id=(dp, to), device_id_type=MESH).start()

    def wait(ref, sem):
        pltpu.make_async_copy(ref, ref, sem).wait()

    def x_copy(i):
        at = pl.ds(i * rows, rows)
        return pltpu.make_async_copy(x_hbm.at[at], xb.at[at], wsem.at[i % 2])

    def w_copy(hbm, dst, g, width, sem):
        at = pl.ds(pl.multiple_of((c * 2 + g) * width, width), width)
        return pltpu.make_async_copy(hbm.at[:, at], dst, sem)

    wk_copy = lambda g: w_copy(wk_hbm, wkvb.at[g, :, pl.ds(0, HEAD)], g, HEAD, wsem.at[5 + g])
    wv_copy = lambda g: w_copy(wv_hbm, wkvb.at[g, :, pl.ds(HEAD, HEAD)], g, HEAD, wsem.at[7 + g])
    wq_copy = lambda g: w_copy(wq_hbm, wqb.at[g], g, 2 * HEAD, wsem.at[2 + g])
    wo_copy = pltpu.make_async_copy(wo_hbm, wob, wsem.at[0])
    g_last = jnp.where(z == 2, 1, 0)
    last_copy = pltpu.make_async_copy(wo_hbm.at[pl.ds(pl.multiple_of(((1 - c) * 4 + g_last * 2 + 1) * HEAD, HEAD), HEAD)], w_last, wsem.at[1])
    g_first = jnp.where(z == 0, 1, 0)

    count = 2 * n // FINE
    gain_copy = pltpu.make_async_copy(gain_hbm, gainb, wsem.at[2])
    tables = [pltpu.make_async_copy(fine_hbm, fine_ref, wsem.at[3]),
              pltpu.make_async_copy(coarse_hbm.at[:, pl.ds(pl.multiple_of(z * count, 8), count)], coarse_ref, wsem.at[4])]

    for copy in gain_copy, *tables, x_copy(0), wk_copy(g_first), x_copy(1), wv_copy(g_first):
        copy.start()

    barrier = pltpu.get_barrier_semaphore()

    def here_now(chip, core):
        pl.semaphore_signal(barrier, 1, device_id=(dp, 2 * chip + core), device_id_type=MESH)

    here_now(z, 1 - c)

    @pl.when(z == 0)
    def _():
        here_now(2, c)

    @pl.when(z == 1)
    def _():
        here_now(0, c)
        here_now(2, c)
        for core in PAIR:
            here_now(3, core)

    @pl.when(z == 2)
    def _():
        here_now(3, c)

    @pl.when(z >= 2)
    def _():
        for core in PAIR:
            here_now(z - 1, core)

    def send_keys(g, h, to, at):
        ref = kb.at[g, 2 * z + h, at]
        push(ref, ref, 1, krecv.at[g if to == 1 else z % 2], 2 * to + c)

    def send_values(g, h, to):
        ref = vb.at[g, 2 * z + h]
        push(ref, ref, 1, krecv.at[g if to == 1 else z % 2], 2 * to + c)

    def send_both(g, h, to):
        send_keys(g, h, to, pl.ds(0, n))
        send_values(g, h, to)

    def send_queries(g, h, to):
        ref = qb.at[g, 2 * z + h]
        push(ref, ref, 1, qrecv.at[2 * z + h - 4], 2 * to + c)

    def turned(t, first):
        at = pl.ds(pl.multiple_of(first, rows), t.shape[0])
        cos, sin = cs[0, at, :], cs[1, at, :]
        t = t.astype(BF).astype(F32)
        a, b = t[:, : HEAD // 2], t[:, HEAD // 2 :]
        return jnp.concatenate([a * cos - b * sin, b * cos + a * sin], -1).astype(BF)

    def send(g, gi, h, what, *more):
        for at, gg, to in ((z == 1) & (g == 0), 0, 2), ((z == 2) & (g == 1), 1, 3), ((z == 0) & (gi == 0), 1, 1):
            pl.when(at)(functools.partial(what, gg, h, to, *more))

    def keep_keys(g, gi, h, k, first, greet=False):
        at = pl.ds(first, k.shape[0])
        kb[g, 2 * z + h, at, :] = turned(k, h * n + first)
        if greet:
            pl.semaphore_wait(barrier, _pick(0, z, [[2, 3, 5, 4]]))
        send(g, gi, h, send_keys, at)

    def keep_values(g, h, v, first):
        vb[g, 2 * z + h, :, first : first + v.shape[0]] = v.astype(BF).T

    def make_both(g, gi, h, first):
        kv = _product(ab[h, first : first + n // 2, :], wkvb[g])
        keep_keys(g, gi, h, kv[:, :HEAD], first)
        keep_values(g, h, kv[:, HEAD:], first)
        if first:
            send(g, gi, h, send_values)

    def turn_table(i, _):
        fc, fs = fine_ref[0], fine_ref[1]
        cc = coarse_ref[0, pl.ds(i, 1), :]
        ss = coarse_ref[1, pl.ds(i, 1), :]
        at = pl.ds(pl.multiple_of(i * FINE, FINE), FINE)
        cs[0, at, :] = cc * fc - ss * fs
        cs[1, at, :] = ss * fc + cc * fs

    def norm(i):
        x_copy(i).wait()
        at = pl.ds(i * rows, rows)
        w = xb[at, :].astype(F32)
        ab[c, at, :] = (w * lax.rsqrt(jnp.mean(w * w, -1, keepdims=True) + 1e-6) * gain).astype(BF)

    for copy in gain_copy, *tables:
        copy.wait()
    lax.fori_loop(0, count, turn_table, None, unroll=8)
    gain = gainb[...].astype(F32)[None, :]
    for i in PAIR:
        norm(i)
        x_copy(2 + i).start()
        if i == 0:
            wk_copy(g_first).wait()
        k = _product(ab[c, i * rows : (i + 1) * rows, :], wkvb[g_first, :, :HEAD])
        keep_keys(g_first, 0, c, k, i * rows, i == 0)

    @pl.when(z == 2)
    def _():
        pl.semaphore_signal(ready, 1, device_id=(dp, c), device_id_type=MESH)

    @pl.when(z == 3)
    def _():
        for core in PAIR:
            pl.semaphore_signal(ready, 1, device_id=(dp, 2 + core), device_id_type=MESH)

    wv_copy(g_first).wait()
    keep_values(g_first, c, _product(ab[c, : n // 2, :], wkvb[g_first, :, HEAD:]), 0)
    for i in PAIR:
        norm(2 + i)
    push(ab.at[c], ab.at[c], 0, arecv, z * 2 + 1 - c)
    make_both(g_first, 0, c, n // 2)
    wk_copy(1 - g_first).start()
    wv_copy(1 - g_first).start()
    wq_copy(1).start()
    wq_copy(0).start()

    def project(hh, _):
        h = jnp.where(hh == 0, c, 1 - c)

        @pl.when(hh == 1)
        def _():
            wait(ab.at[1 - c], arecv)
            wo_copy.start()
            last_copy.start()

        def keys(gi, _):
            g = jnp.where(gi == 0, g_first, 1 - g_first)

            @pl.when(hh == 0)
            def _():
                wk_copy(g).wait()
                wv_copy(g).wait()

            for r in PAIR:
                make_both(g, gi, h, r * (n // 2))

            @pl.when((z == 0) & (gi == 1))
            def _():
                @pl.when(hh == 0)
                def _():
                    pl.semaphore_wait(ready, 1)

                send_both(0, h, 2)

                @pl.when(hh == 1)
                def _():
                    send_both(0, c, 1)
                    send_both(0, 1 - c, 1)

        lax.fori_loop(jnp.where(hh == 0, 1, 0), 2, keys, None)

        def queries(gi, _):
            g = 1 - gi

            @pl.when(hh == 0)
            def _():
                wq_copy(g).wait()

            q = _product(ab[h], wqb[g])
            for s in PAIR:
                qb[g, 2 * z + h, s] = turned(q[:, s * HEAD : (s + 1) * HEAD], h * n)

            @pl.when((z == 3) & (g == 1))
            def _():
                send_queries(1, h, 1)

            @pl.when((z == 3) & (hh == 1) & (g == 0))
            def _():
                send_queries(0, c, 2)
                send_queries(0, 1 - c, 2)

        lax.fori_loop(0, 2, queries, None)

    lax.fori_loop(0, 2, project, None)
    yacc[...] = xb[...].astype(F32)

    for l in range(2):
        for g in PAIR:
            @pl.when((z < 2) | ((z == 2) & (g == 0)))
            def _():
                ob[REMOTE + l * 2 + g] = jnp.zeros(ob.shape[1:], BF)
                ls[REMOTE + l * 2 + g] = jnp.full(ls.shape[1:], LOWEST, F32)

    ones = jnp.ones((8, n), BF)

    wo_copy.wait()
    last_copy.wait()

    def task(code):
        _, g, q, t, waits = fields(code)
        local = q // 2 == z
        first = _pick(z, g, FIRST)
        def q_wait(qq):
            wait(qb.at[g, qq], qrecv.at[qq - 4])

        @pl.when((z == 1) & (waits > 0) & (g == 1))
        def _():
            q_wait(6)
            q_wait(7)
            pl.semaphore_wait(ready, 2)
            pl.semaphore_signal(go, 1, device_id=(dp, sp + 2), device_id_type=MESH)

        @pl.when((z == 2) & (waits > 0))
        def _():
            pl.semaphore_wait(go, 1)
            send_queries(1, c, 1)
            send_queries(1, 1 - c, 1)

        @pl.when(jnp.logical_not(local) & ((z == 2) | (q < 6)))
        def _():
            q_wait(q)

        for o in THIRDS:
            @pl.when((waits // 2**o) % 2 == 1)
            def _():
                wait(kb.at[g, pl.ds(0, 4)], krecv.at[jnp.where(z == 1, g, o % 2)])

        top_s[...] = jnp.full(top_s.shape, LOWEST, F32)
        mix_s[...] = jnp.zeros(mix_s.shape, F32)

        def block(j, masked):
            scores = [_dot(kb[g, j], qb[g, q, s], 1, 1) for s in range(2)]
            weights, keeps = [], []
            for s in PAIR:
                score = scores[s]
                if masked:
                    ok = lax.broadcasted_iota(jnp.int32, (n, n), 0) <= lax.broadcasted_iota(jnp.int32, (n, n), 1)
                    score = jnp.where(ok, score, LOWEST)
                old = top_s[s : s + 1, :]
                top = jnp.maximum(old, score.max(axis=0, keepdims=True))
                top_s[s : s + 1, :] = top
                weights.append(jnp.exp2((score - top) * e).astype(BF))
                keeps.append(jnp.exp2((old - top) * e))
            values = jnp.concatenate([vb[g, j], ones], axis=0)
            for s in PAIR:
                mix_s[s] = mix_s[s] * keeps[s] + _product(values, weights[s])

        lax.fori_loop(first, jnp.minimum(q, 2 * z + 2), lambda j, _: block(j, False), None)

        @pl.when(local)
        def _():
            block(q, True)

        slot = jnp.where(local, LOCAL, REMOTE) + c * 2 + g
        here = jnp.where(q == sp, slot, t)
        for s in PAIR:
            total = mix_s[s, HEAD : HEAD + 1, :]
            o = (mix_s[s, :HEAD, :] * (1 / total)).astype(BF)
            for part in QUARTERS:
                ob[here, s, part] = o[:, part * rows : (part + 1) * rows]
            lse = top_s[s : s + 1, :] * e + jnp.log2(total)
            for part in QUARTERS:
                row = 4 * s + part
                ls[here, row : row + 1, :] = lse[:, part * rows : (part + 1) * rows]

        @pl.when(local & (q != sp))
        def _():
            push(ls.at[t], ls.at[slot], 3, local_l.at[g], q)
            push(ob.at[t], ob.at[slot], 2, local_o.at[g], q)

        @pl.when(jnp.logical_not(local))
        def _():
            own = q % 2 == c
            push(ls.at[t], ls.at[slot], 3, remote_l.at[g, jnp.where(own, 0, 1)], q)

            last = (g == 1) == (q // 2 == 2)

            @pl.when(own | jnp.logical_not(last))
            def _():
                push(ob.at[t], ob.at[slot], 2, remote_o.at[jnp.where(own, g, WHOLE)], q)

            @pl.when(jnp.logical_not(own) & last)
            def _():
                for s in PAIR:
                    for part in QUARTERS:
                        push(ob.at[t, s, part], ob.at[slot, s, part], 2, remote_o.at[2 + 4 * s + part], q)

    def merged(base, s, part):
        la, lb = (ls[at + base, pl.ds(4 * s + part, 1), :] for at in (LOCAL, REMOTE))
        m = jnp.maximum(la, lb)
        wa, wb = jnp.exp2(la - m), jnp.exp2(lb - m)
        r = 1 / (wa + wb)
        o = ob[LOCAL + base, s, part].astype(F32) * (wa * r) + ob[REMOTE + base, s, part].astype(F32) * (wb * r)
        return o.T.astype(BF)

    def arrivals(g, other, first, what, sem):
        @pl.when(first & (other == 1))
        def _():
            wait(ls.at[0], local_l.at[g])
            wait(ob.at[0], local_o.at[g])

        @pl.when((z == 3) | ((z == 2) & (g == 1)))
        def _():
            @pl.when(first)
            def _():
                wait(ls.at[0], remote_l.at[g, other])

            wait(what, remote_o.at[sem])

    third = wide // 3

    def finish_line(code):
        _, g, what, _, _ = fields(code)
        other = what // 4
        l = (c + other) % 2
        base = l * 2 + g
        arrivals(g, other, True, ob.at[0], jnp.where(other == 0, g, WHOLE))
        for s in PAIR:
            for part in QUARTERS:
                of[part * rows : (part + 1) * rows, s * HEAD : (s + 1) * HEAD] = merged(base, s, part)
        at = pl.ds(pl.multiple_of((l * 4 + g * 2) * HEAD, 2 * HEAD), 2 * HEAD)

        def columns(k, _):
            cols = pl.ds(pl.multiple_of(k * third, 128), third)
            yacc[:, cols] += _product(of[...], wob[at, cols])

        lax.fori_loop(0, 3, columns, None)

    def finish_piece(code):
        _, g, what, _, _ = fields(code)
        s, part = what // 4, what % 4
        l = 1 - c
        base = l * 2 + g
        arrivals(g, 1, what == 0, ob.at[0, 0, 0], 2 + what)
        o = merged(base, s, part)
        at = pl.ds(pl.multiple_of((l * 4 + g * 2 + s) * HEAD, HEAD), HEAD)
        tokens = pl.ds(pl.multiple_of(part * rows, rows), rows)

        def add(store):
            of[0:rows, 0:HEAD] = o
            for k in THIRDS:
                cols = slice(k * third, (k + 1) * third)
                store(cols, yacc[tokens, cols] + _product(of[0:rows, 0:HEAD], wob[at, cols]))

        @pl.when(s == 0)
        def _():
            def store(cols, y):
                yacc[tokens, cols] = y

            add(store)

        @pl.when((s == 1) & (part < 3))
        def _():
            def store(cols, y):
                y_ref[tokens, cols] = y.astype(BF)

            add(store)

        @pl.when((s == 1) & (part == 3))
        def _():
            o_last[...] = o

    steps = jnp.where(z == 1, 19, jnp.where(z == 2, 17, 15))

    def drain():
        wait(ab.at[c], sent.at[0])
        for zz in range(4):
            @pl.when(z == zz)
            def _():
                wait(qb.at[0, pl.ds(0, SENT[zz])], sent.at[1])
                wait(ob.at[pl.ds(0, STAGED[zz])], sent.at[2])
                wait(ls.at[pl.ds(0, STAGED[zz])], sent.at[3])

    def step(i, _):
        code = _pick(sp, i, PLAN)

        @pl.when(code % 4 == 0)
        def _():
            task(code)

        @pl.when(code % 4 == 2)
        def _():
            finish_line(code)

        @pl.when(code % 4 == 1)
        def _():
            @pl.when((z != 1) & (i == steps - 1))
            def _():
                drain()

            finish_piece(code)

    lax.fori_loop(0, steps, step, None)

    @pl.when(z == 1)
    def _():
        drain()


def write(y_ref, yacc, o_last, w_last, y_hbm, out, sem):
    n, wide = y_ref.shape
    pltpu.make_async_copy(y_ref, y_hbm.at[pl.ds(0, n)], sem).start()
    for k in THIRDS:
        cols = slice(k * (wide // 3), (k + 1) * (wide // 3))
        out[k] = (yacc[n:, cols] + _product(o_last[...], w_last[:, cols])).astype(BF)
        pltpu.make_async_copy(out.at[k], y_hbm.at[pl.ds(n, n // 3), cols], sem).start()
    pltpu.make_async_copy(y_hbm, y_hbm, sem).wait()


def solution(mesh):
    def step(x, gain, wq, wk, wv, wo):
        n, wide = x.shape
        half = HEAD // 2
        rate = np.float64(THETA) ** (-np.arange(half) / half)
        table = lambda places: jnp.asarray(np.stack([f(places[:, None] * rate) for f in (np.cos, np.sin)]).astype(np.float32))
        coarse, fine = table(np.arange(8 * n // FINE) * FINE), table(np.arange(FINE))
        hbm, vmem = pl.BlockSpec(memory_space=pl.ANY), pl.BlockSpec(memory_space=pltpu.VMEM)
        dma = pltpu.SemaphoreType.DMA
        parts = pl.pallas_call(
            kernel,
            out_shape=[pltpu.VMEM((3 * n // 4, wide), BF), pltpu.VMEM((n, wide), F32), pltpu.VMEM((n // 4, HEAD), BF), pltpu.VMEM((HEAD, wide), BF)],
            in_specs=[hbm] * 8,
            out_specs=[vmem] * 4,
            scratch_shapes=[
                pltpu.VMEM((n, wide), BF),
                pltpu.VMEM((wide,), BF),
                pltpu.VMEM((2, 2 * n // FINE, half), F32),
                pltpu.VMEM((2, FINE, half), F32),
                pltpu.VMEM((2, n, wide), BF),
                pltpu.VMEM((2, wide, 2 * HEAD), BF),
                pltpu.VMEM((2, wide, 2 * HEAD), BF),
                pltpu.VMEM((8 * HEAD, wide), BF),
                pltpu.VMEM((2, 8, n, HEAD), BF),
                pltpu.VMEM((2, 8, HEAD, n), BF),
                pltpu.VMEM((2, 8, 2, n, HEAD), BF),
                pltpu.VMEM((16, 2, 4, HEAD, n // 4), BF),
                pltpu.VMEM((16, 8, 128), F32),
                pltpu.VMEM((8, n), F32),
                pltpu.VMEM((2, HEAD + 8, n), F32),
                pltpu.VMEM((n, 2 * HEAD), BF),
                pltpu.VMEM((2, 2 * n, half), F32),
                dma((9,)), dma((4,)), dma,
                dma((2,)), dma((4,)),
                dma((2,)), dma((2,)), dma((11,)), dma((2, 2)),
                pltpu.SemaphoreType.REGULAR, pltpu.SemaphoreType.REGULAR,
            ],
            compiler_params=pltpu.CompilerParams(collective_id=0, has_side_effects=True, vmem_limit_bytes=55 << 20),
        )(x, gain, coarse, fine, wq, wk, wv, wo)
        return pl.pallas_call(
            write,
            out_shape=jax.ShapeDtypeStruct((n, wide), BF),
            in_specs=[vmem] * 4,
            out_specs=hbm,
            scratch_shapes=[pltpu.VMEM((3, n // 4, wide // 3), BF), dma],
            compiler_params=pltpu.CompilerParams(vmem_limit_bytes=4 << 20),
        )(*(pltpu.with_memory_space_constraint(part, pltpu.VMEM) for part in parts))

    tokens, whole = P(("dp", "sp"), None), P(None, None)
    return jax.shard_map(
        step,
        mesh=mesh,
        in_specs=(tokens, P(None), whole, whole, whole, whole),
        out_specs=tokens,
        check_vma=False,
    )
```

```python
import functools

import jax
import jax.numpy as jnp
import numpy as np
from jax import lax
from jax.experimental import pallas as pl
from jax.experimental.pallas import tpu as pltpu
from jax.sharding import PartitionSpec as P

HEAD = 256
THETA = 10000
LOWEST = float(np.finfo(np.float32).min)
LOG2E = 1.4426950408889634
FINE = 32
MESH = pl.DeviceIdType.MESH
BF, F32 = jnp.bfloat16, jnp.float32
PAIR = (0, 1)
QUARTERS = (0, 1, 2, 3)
THIRDS = (0, 1, 2)
WHOLE = 10
LOCAL, REMOTE = 8, 12

FIRST = [[0, 0], [0, 0], [0, 4], [6, 4]]
STAGED = [2, 6, 4, 2]
SENT = [6, 2, 4, 4]
SIZES = (4, 2, 8, 8)


def plan(z, c):
    steps, staged = [], 0

    def step(kind, g, what, slot=0, waits=0):
        code = waits
        for field, size in reversed(list(zip((kind, g, what, slot), SIZES))):
            code = code * size + field
        steps.append(code)

    def attention(g, a, b, waits=0):
        nonlocal staged
        for q in (a, b) if c == 0 else (b, a):
            step(0, g, q, staged, waits)
            waits = 0
            staged += q != 2 * z + c

    def output(g, last=False):
        step(2, g, 0)
        for piece in range(8) if last else [4]:
            step(1 if last else 2, g, piece)

    if z == 0:
        attention(1, 0, 1), attention(0, 0, 1), output(1), output(0, True)
    elif z == 1:
        attention(1, 6, 7, 1), attention(1, 2, 3), attention(1, 4, 5), output(1), attention(0, 2, 3, 1), output(0, True)
    elif z == 2:
        attention(1, 4, 5), attention(0, 6, 7, 3), attention(0, 4, 5), output(0), output(1, True)
    else:
        attention(0, 6, 7), attention(1, 6, 7, 4), output(1), output(0, True)
    return steps


PLAN = [plan(z, c) for z in range(4) for c in PAIR]


def fields(code):
    got = []
    for size in SIZES:
        got.append(code % size)
        code = code // size
    return *got, code


def _dot(a, b, ca, cb):
    return lax.dot_general(a, b, (((ca,), (cb,)), ((), ())), preferred_element_type=F32)


def _product(a, w):
    return _dot(a, w, 1, 0)


def _pick(z, i, table):
    out = jnp.int32(0)
    for zz, row in enumerate(table):
        got = jnp.int32(0)
        for ii, value in enumerate(row):
            got = jnp.where(i == ii, jnp.int32(value), got)
        out = jnp.where(z == zz, got, out)
    return out


def kernel(x_hbm, gain_hbm, coarse_hbm, fine_hbm, wq_hbm, wk_hbm, wv_hbm, wo_hbm, y_ref, yacc, o_last, w_last,
           xb, gainb, coarse_ref, fine_ref, ab, wqb, wkvb, wob, kb, vb, qb, ob, ls, top_s, mix_s, of, cs,
           sent, arecv, krecv, qrecv, local_o, local_l, remote_o, remote_l, go, ready):
    dp, sp = lax.axis_index("dp"), lax.axis_index("sp")
    z, c = sp // 2, sp % 2
    n, wide = xb.shape
    rows = n // 4
    scale = HEAD**-0.5
    e = scale * LOG2E

    def push(src, dst, send, recv, to):
        pltpu.make_async_remote_copy(src, dst, sent.at[send], recv, device_id=(dp, to), device_id_type=MESH).start()

    def wait(ref, sem):
        pltpu.make_async_copy(ref, ref, sem).wait()

    def send_queries(g, h, to):
        ref = qb.at[g, 2 * z + h]
        push(ref, ref, 1, qrecv.at[2 * z + h - 4], 2 * to + c)

    def project_all(wsem):
        def x_copy(i):
            at = pl.ds(i * rows, rows)
            return pltpu.make_async_copy(x_hbm.at[at], xb.at[at], wsem.at[i % 2])

        def w_copy(hbm, dst, g, width, sem):
            at = pl.ds(pl.multiple_of((c * 2 + g) * width, width), width)
            return pltpu.make_async_copy(hbm.at[:, at], dst, sem)

        wk_copy = lambda g: w_copy(wk_hbm, wkvb.at[g, :, pl.ds(0, HEAD)], g, HEAD, wsem.at[5 + g])
        wv_copy = lambda g: w_copy(wv_hbm, wkvb.at[g, :, pl.ds(HEAD, HEAD)], g, HEAD, wsem.at[7 + g])
        wq_copy = lambda g: w_copy(wq_hbm, wqb.at[g], g, 2 * HEAD, wsem.at[2 + g])
        wo_copy = pltpu.make_async_copy(wo_hbm, wob, wsem.at[0])
        g_last = jnp.where(z == 2, 1, 0)
        last_copy = pltpu.make_async_copy(wo_hbm.at[pl.ds(pl.multiple_of(((1 - c) * 4 + g_last * 2 + 1) * HEAD, HEAD), HEAD)], w_last, wsem.at[1])
        g_first = jnp.where(z == 0, 1, 0)

        count = 2 * n // FINE
        gain_copy = pltpu.make_async_copy(gain_hbm, gainb, wsem.at[2])
        tables = [pltpu.make_async_copy(fine_hbm, fine_ref, wsem.at[3]),
                  pltpu.make_async_copy(coarse_hbm.at[:, pl.ds(pl.multiple_of(z * count, 8), count)], coarse_ref, wsem.at[4])]

        for copy in gain_copy, *tables, x_copy(0), wk_copy(g_first), x_copy(1), wv_copy(g_first):
            copy.start()

        barrier = pltpu.get_barrier_semaphore()

        def here_now(chip, core):
            pl.semaphore_signal(barrier, 1, device_id=(dp, 2 * chip + core), device_id_type=MESH)

        here_now(z, 1 - c)

        @pl.when(z == 0)
        def _():
            here_now(2, c)

        @pl.when(z == 1)
        def _():
            here_now(0, c)
            here_now(2, c)
            for core in PAIR:
                here_now(3, core)

        @pl.when(z == 2)
        def _():
            here_now(3, c)

        @pl.when(z >= 2)
        def _():
            for core in PAIR:
                here_now(z - 1, core)

        def send_keys(g, h, to, at):
            ref = kb.at[g, 2 * z + h, at]
            push(ref, ref, 1, krecv.at[g if to == 1 else z % 2], 2 * to + c)

        def send_values(g, h, to):
            ref = vb.at[g, 2 * z + h]
            push(ref, ref, 1, krecv.at[g if to == 1 else z % 2], 2 * to + c)

        def send_both(g, h, to):
            send_keys(g, h, to, pl.ds(0, n))
            send_values(g, h, to)

        def turned(t, first):
            at = pl.ds(pl.multiple_of(first, rows), t.shape[0])
            cos, sin = cs[0, at, :], cs[1, at, :]
            t = t.astype(BF).astype(F32)
            a, b = t[:, : HEAD // 2], t[:, HEAD // 2 :]
            return jnp.concatenate([a * cos - b * sin, b * cos + a * sin], -1).astype(BF)

        def send(g, gi, h, what, *more):
            for at, gg, to in ((z == 1) & (g == 0), 0, 2), ((z == 2) & (g == 1), 1, 3), ((z == 0) & (gi == 0), 1, 1):
                pl.when(at)(functools.partial(what, gg, h, to, *more))

        def keep_keys(g, gi, h, k, first, greet=False):
            at = pl.ds(first, k.shape[0])
            kb[g, 2 * z + h, at, :] = turned(k, h * n + first)
            if greet:
                pl.semaphore_wait(barrier, _pick(0, z, [[2, 3, 5, 4]]))
            send(g, gi, h, send_keys, at)

        def keep_values(g, h, v, first):
            vb[g, 2 * z + h, :, first : first + v.shape[0]] = v.astype(BF).T

        def make_both(g, gi, h, first):
            kv = _product(ab[h, first : first + n // 2, :], wkvb[g])
            keep_keys(g, gi, h, kv[:, :HEAD], first)
            keep_values(g, h, kv[:, HEAD:], first)
            if first:
                send(g, gi, h, send_values)

        def turn_table(i, _):
            fc, fs = fine_ref[0], fine_ref[1]
            cc = coarse_ref[0, pl.ds(i, 1), :]
            ss = coarse_ref[1, pl.ds(i, 1), :]
            at = pl.ds(pl.multiple_of(i * FINE, FINE), FINE)
            cs[0, at, :] = cc * fc - ss * fs
            cs[1, at, :] = ss * fc + cc * fs

        def norm(i):
            x_copy(i).wait()
            at = pl.ds(i * rows, rows)
            w = xb[at, :].astype(F32)
            ab[c, at, :] = (w * lax.rsqrt(jnp.mean(w * w, -1, keepdims=True) + 1e-6) * gain).astype(BF)

        for copy in gain_copy, *tables:
            copy.wait()
        lax.fori_loop(0, count, turn_table, None, unroll=8)
        gain = gainb[...].astype(F32)[None, :]
        for i in PAIR:
            norm(i)
            x_copy(2 + i).start()
            if i == 0:
                wk_copy(g_first).wait()
            k = _product(ab[c, i * rows : (i + 1) * rows, :], wkvb[g_first, :, :HEAD])
            keep_keys(g_first, 0, c, k, i * rows, i == 0)

        @pl.when(z == 2)
        def _():
            pl.semaphore_signal(ready, 1, device_id=(dp, c), device_id_type=MESH)

        @pl.when(z == 3)
        def _():
            for core in PAIR:
                pl.semaphore_signal(ready, 1, device_id=(dp, 2 + core), device_id_type=MESH)

        wv_copy(g_first).wait()
        keep_values(g_first, c, _product(ab[c, : n // 2, :], wkvb[g_first, :, HEAD:]), 0)
        for i in PAIR:
            norm(2 + i)
        push(ab.at[c], ab.at[c], 0, arecv, z * 2 + 1 - c)
        make_both(g_first, 0, c, n // 2)
        wk_copy(1 - g_first).start()
        wv_copy(1 - g_first).start()
        wq_copy(1).start()
        wq_copy(0).start()

        def project(hh, _):
            h = jnp.where(hh == 0, c, 1 - c)

            @pl.when(hh == 1)
            def _():
                wait(ab.at[1 - c], arecv)
                wo_copy.start()
                last_copy.start()

            def keys(gi, _):
                g = jnp.where(gi == 0, g_first, 1 - g_first)

                @pl.when(hh == 0)
                def _():
                    wk_copy(g).wait()
                    wv_copy(g).wait()

                for r in PAIR:
                    make_both(g, gi, h, r * (n // 2))

                @pl.when((z == 0) & (gi == 1))
                def _():
                    @pl.when(hh == 0)
                    def _():
                        pl.semaphore_wait(ready, 1)

                    send_both(0, h, 2)

                    @pl.when(hh == 1)
                    def _():
                        send_both(0, c, 1)
                        send_both(0, 1 - c, 1)

            lax.fori_loop(jnp.where(hh == 0, 1, 0), 2, keys, None)

            def queries(gi, _):
                g = 1 - gi

                @pl.when(hh == 0)
                def _():
                    wq_copy(g).wait()

                q = _product(ab[h], wqb[g])
                for s in PAIR:
                    qb[g, 2 * z + h, s] = turned(q[:, s * HEAD : (s + 1) * HEAD], h * n)

                @pl.when((z == 3) & (g == 1))
                def _():
                    send_queries(1, h, 1)

                @pl.when((z == 3) & (hh == 1) & (g == 0))
                def _():
                    send_queries(0, c, 2)
                    send_queries(0, 1 - c, 2)

            lax.fori_loop(0, 2, queries, None)

        lax.fori_loop(0, 2, project, None)
        yacc[...] = xb[...].astype(F32)

        for l in range(2):
            for g in PAIR:
                @pl.when((z < 2) | ((z == 2) & (g == 0)))
                def _():
                    ob[REMOTE + l * 2 + g] = jnp.zeros(ob.shape[1:], BF)
                    ls[REMOTE + l * 2 + g] = jnp.full(ls.shape[1:], LOWEST, F32)
        wo_copy.wait()
        last_copy.wait()

    pl.run_scoped(project_all, pltpu.SemaphoreType.DMA((9,)))

    ones = jnp.ones((8, n), BF)

    def task(code):
        _, g, q, t, waits = fields(code)
        local = q // 2 == z
        first = _pick(z, g, FIRST)
        def q_wait(qq):
            wait(qb.at[g, qq], qrecv.at[qq - 4])

        @pl.when((z == 1) & (waits > 0) & (g == 1))
        def _():
            q_wait(6)
            q_wait(7)
            pl.semaphore_wait(ready, 2)
            pl.semaphore_signal(go, 1, device_id=(dp, sp + 2), device_id_type=MESH)

        @pl.when((z == 2) & (waits > 0))
        def _():
            pl.semaphore_wait(go, 1)
            send_queries(1, c, 1)
            send_queries(1, 1 - c, 1)

        @pl.when(jnp.logical_not(local) & ((z == 2) | (q < 6)))
        def _():
            q_wait(q)

        for o in THIRDS:
            @pl.when((waits // 2**o) % 2 == 1)
            def _():
                wait(kb.at[g, pl.ds(0, 4)], krecv.at[jnp.where(z == 1, g, o % 2)])

        top_s[...] = jnp.full(top_s.shape, LOWEST, F32)
        mix_s[...] = jnp.zeros(mix_s.shape, F32)

        def block(j, masked):
            scores = [_dot(kb[g, j], qb[g, q, s], 1, 1) for s in range(2)]
            weights, keeps = [], []
            for s in PAIR:
                score = scores[s]
                if masked:
                    ok = lax.broadcasted_iota(jnp.int32, (n, n), 0) <= lax.broadcasted_iota(jnp.int32, (n, n), 1)
                    score = jnp.where(ok, score, LOWEST)
                old = top_s[s : s + 1, :]
                top = jnp.maximum(old, score.max(axis=0, keepdims=True))
                top_s[s : s + 1, :] = top
                weights.append(jnp.exp2((score - top) * e).astype(BF))
                keeps.append(jnp.exp2((old - top) * e))
            values = jnp.concatenate([vb[g, j], ones], axis=0)
            for s in PAIR:
                mix_s[s] = mix_s[s] * keeps[s] + _product(values, weights[s])

        lax.fori_loop(first, jnp.minimum(q, 2 * z + 2), lambda j, _: block(j, False), None)

        @pl.when(local)
        def _():
            block(q, True)

        slot = jnp.where(local, LOCAL, REMOTE) + c * 2 + g
        here = jnp.where(q == sp, slot, t)
        for s in PAIR:
            total = mix_s[s, HEAD : HEAD + 1, :]
            o = (mix_s[s, :HEAD, :] * (1 / total)).astype(BF)
            for part in QUARTERS:
                ob[here, s, part] = o[:, part * rows : (part + 1) * rows]
            lse = top_s[s : s + 1, :] * e + jnp.log2(total)
            for part in QUARTERS:
                row = 4 * s + part
                ls[here, row : row + 1, :] = lse[:, part * rows : (part + 1) * rows]

        @pl.when(local & (q != sp))
        def _():
            push(ls.at[t], ls.at[slot], 3, local_l.at[g], q)
            push(ob.at[t], ob.at[slot], 2, local_o.at[g], q)

        @pl.when(jnp.logical_not(local))
        def _():
            own = q % 2 == c
            push(ls.at[t], ls.at[slot], 3, remote_l.at[g, jnp.where(own, 0, 1)], q)

            last = (g == 1) == (q // 2 == 2)

            @pl.when(own | jnp.logical_not(last))
            def _():
                push(ob.at[t], ob.at[slot], 2, remote_o.at[jnp.where(own, g, WHOLE)], q)

            @pl.when(jnp.logical_not(own) & last)
            def _():
                for s in PAIR:
                    for part in QUARTERS:
                        push(ob.at[t, s, part], ob.at[slot, s, part], 2, remote_o.at[2 + 4 * s + part], q)

    def merged(base, s, part):
        la, lb = (ls[at + base, pl.ds(4 * s + part, 1), :] for at in (LOCAL, REMOTE))
        m = jnp.maximum(la, lb)
        wa, wb = jnp.exp2(la - m), jnp.exp2(lb - m)
        r = 1 / (wa + wb)
        o = ob[LOCAL + base, s, part].astype(F32) * (wa * r) + ob[REMOTE + base, s, part].astype(F32) * (wb * r)
        return o.T.astype(BF)

    def arrivals(g, other, first, what, sem):
        @pl.when(first & (other == 1))
        def _():
            wait(ls.at[0], local_l.at[g])
            wait(ob.at[0], local_o.at[g])

        @pl.when((z == 3) | ((z == 2) & (g == 1)))
        def _():
            @pl.when(first)
            def _():
                wait(ls.at[0], remote_l.at[g, other])

            wait(what, remote_o.at[sem])

    third = wide // 3

    def finish_line(code):
        _, g, what, _, _ = fields(code)
        other = what // 4
        l = (c + other) % 2
        base = l * 2 + g
        arrivals(g, other, True, ob.at[0], jnp.where(other == 0, g, WHOLE))
        for s in PAIR:
            for part in QUARTERS:
                of[part * rows : (part + 1) * rows, s * HEAD : (s + 1) * HEAD] = merged(base, s, part)
        at = pl.ds(pl.multiple_of((l * 4 + g * 2) * HEAD, 2 * HEAD), 2 * HEAD)

        def columns(k, _):
            cols = pl.ds(pl.multiple_of(k * third, 128), third)
            yacc[:, cols] += _product(of[...], wob[at, cols])

        lax.fori_loop(0, 3, columns, None)

    def finish_piece(code):
        _, g, what, _, _ = fields(code)
        s, part = what // 4, what % 4
        l = 1 - c
        base = l * 2 + g
        arrivals(g, 1, what == 0, ob.at[0, 0, 0], 2 + what)
        o = merged(base, s, part)
        at = pl.ds(pl.multiple_of((l * 4 + g * 2 + s) * HEAD, HEAD), HEAD)
        tokens = pl.ds(pl.multiple_of(part * rows, rows), rows)

        def add(store):
            of[0:rows, 0:HEAD] = o
            for k in THIRDS:
                cols = slice(k * third, (k + 1) * third)
                store(cols, yacc[tokens, cols] + _product(of[0:rows, 0:HEAD], wob[at, cols]))

        @pl.when(s == 0)
        def _():
            def store(cols, y):
                yacc[tokens, cols] = y

            add(store)

        @pl.when((s == 1) & (part < 3))
        def _():
            def store(cols, y):
                y_ref[tokens, cols] = y.astype(BF)

            add(store)

        @pl.when((s == 1) & (part == 3))
        def _():
            o_last[...] = o

    steps = jnp.where(z == 1, 19, jnp.where(z == 2, 17, 15))

    def drain():
        wait(ab.at[c], sent.at[0])
        for zz in range(4):
            @pl.when(z == zz)
            def _():
                wait(qb.at[0, pl.ds(0, SENT[zz])], sent.at[1])
                wait(ob.at[pl.ds(0, STAGED[zz])], sent.at[2])
                wait(ls.at[pl.ds(0, STAGED[zz])], sent.at[3])

    def step(i, _):
        code = _pick(sp, i, PLAN)

        @pl.when(code % 4 == 0)
        def _():
            task(code)

        @pl.when(code % 4 == 2)
        def _():
            finish_line(code)

        @pl.when(code % 4 == 1)
        def _():
            @pl.when((z != 1) & (i == steps - 1))
            def _():
                drain()

            finish_piece(code)

    lax.fori_loop(0, steps, step, None)

    @pl.when(z == 1)
    def _():
        drain()


def write(y_ref, yacc, o_last, w_last, y_hbm, out, sem):
    n, wide = y_ref.shape
    pltpu.make_async_copy(y_ref, y_hbm.at[pl.ds(0, n)], sem).start()
    for k in THIRDS:
        cols = slice(k * (wide // 3), (k + 1) * (wide // 3))
        out[k] = (yacc[n:, cols] + _product(o_last[...], w_last[:, cols])).astype(BF)
        pltpu.make_async_copy(out.at[k], y_hbm.at[pl.ds(n, n // 3), cols], sem).start()
    pltpu.make_async_copy(y_hbm, y_hbm, sem).wait()


def solution(mesh):
    def step(x, gain, wq, wk, wv, wo):
        n, wide = x.shape
        half = HEAD // 2
        rate = np.float64(THETA) ** (-np.arange(half) / half)
        table = lambda places: jnp.asarray(np.stack([f(places[:, None] * rate) for f in (np.cos, np.sin)]).astype(np.float32))
        coarse, fine = table(np.arange(8 * n // FINE) * FINE), table(np.arange(FINE))
        hbm, vmem = pl.BlockSpec(memory_space=pl.ANY), pl.BlockSpec(memory_space=pltpu.VMEM)
        dma = pltpu.SemaphoreType.DMA
        parts = pl.pallas_call(
            kernel,
            out_shape=[pltpu.VMEM((3 * n // 4, wide), BF), pltpu.VMEM((n, wide), F32), pltpu.VMEM((n // 4, HEAD), BF), pltpu.VMEM((HEAD, wide), BF)],
            in_specs=[hbm] * 8,
            out_specs=[vmem] * 4,
            scratch_shapes=[
                pltpu.VMEM((n, wide), BF),
                pltpu.VMEM((wide,), BF),
                pltpu.VMEM((2, 2 * n // FINE, half), F32),
                pltpu.VMEM((2, FINE, half), F32),
                pltpu.VMEM((2, n, wide), BF),
                pltpu.VMEM((2, wide, 2 * HEAD), BF),
                pltpu.VMEM((2, wide, 2 * HEAD), BF),
                pltpu.VMEM((8 * HEAD, wide), BF),
                pltpu.VMEM((2, 8, n, HEAD), BF),
                pltpu.VMEM((2, 8, HEAD, n), BF),
                pltpu.VMEM((2, 8, 2, n, HEAD), BF),
                pltpu.VMEM((16, 2, 4, HEAD, n // 4), BF),
                pltpu.VMEM((16, 8, 128), F32),
                pltpu.VMEM((8, n), F32),
                pltpu.VMEM((2, HEAD + 8, n), F32),
                pltpu.VMEM((n, 2 * HEAD), BF),
                pltpu.VMEM((2, 2 * n, half), F32),
                dma((4,)), dma,
                dma((2,)), dma((4,)),
                dma((2,)), dma((2,)), dma((11,)), dma((2, 2)),
                pltpu.SemaphoreType.REGULAR, pltpu.SemaphoreType.REGULAR,
            ],
            compiler_params=pltpu.CompilerParams(collective_id=0, has_side_effects=True, vmem_limit_bytes=55 << 20),
        )(x, gain, coarse, fine, wq, wk, wv, wo)
        return pl.pallas_call(
            write,
            out_shape=jax.ShapeDtypeStruct((n, wide), BF),
            in_specs=[vmem] * 4,
            out_specs=hbm,
            scratch_shapes=[pltpu.VMEM((3, n // 4, wide // 3), BF), dma],
            compiler_params=pltpu.CompilerParams(vmem_limit_bytes=4 << 20),
        )(*(pltpu.with_memory_space_constraint(part, pltpu.VMEM) for part in parts))

    tokens, whole = P(("dp", "sp"), None), P(None, None)
    return jax.shard_map(
        step,
        mesh=mesh,
        in_specs=(tokens, P(None), whole, whole, whole, whole),
        out_specs=tokens,
        check_vma=False,
    )
```

```python
import functools

import jax
import jax.numpy as jnp
import numpy as np
from jax import lax
from jax.experimental import pallas as pl
from jax.experimental.pallas import tpu as pltpu
from jax.sharding import PartitionSpec as P

HEAD = 256
THETA = 10000
LOWEST = float(np.finfo(np.float32).min)
LOG2E = 1.4426950408889634
FINE = 32
MESH = pl.DeviceIdType.MESH
BF, F32 = jnp.bfloat16, jnp.float32
PAIR = (0, 1)
QUARTERS = (0, 1, 2, 3)
THIRDS = (0, 1, 2)
WHOLE = 10
LOCAL, REMOTE = 8, 12

FIRST = [[0, 0], [0, 0], [0, 4], [6, 4]]
STAGED = [2, 6, 4, 2]
SENT = [6, 2, 4, 4]
SIZES = (4, 2, 8, 8)


def plan(z, c):
    steps, staged = [], 0

    def step(kind, g, what, slot=0, waits=0):
        code = waits
        for field, size in reversed(list(zip((kind, g, what, slot), SIZES))):
            code = code * size + field
        steps.append(code)

    def attention(g, a, b, waits=0):
        nonlocal staged
        for q in (a, b) if c == 0 else (b, a):
            step(0, g, q, staged, waits)
            waits = 0
            staged += q != 2 * z + c

    def output(g, last=False):
        step(2, g, 0)
        for piece in range(8) if last else [4]:
            step(1 if last else 2, g, piece)

    if z == 0:
        attention(1, 0, 1), attention(0, 0, 1), output(1), output(0, True)
    elif z == 1:
        attention(1, 6, 7, 1), attention(1, 2, 3), attention(1, 4, 5), output(1), attention(0, 2, 3, 1), output(0, True)
    elif z == 2:
        attention(1, 4, 5), attention(0, 6, 7, 3), attention(0, 4, 5), output(0), output(1, True)
    else:
        attention(0, 6, 7), attention(1, 6, 7, 4), output(1), output(0, True)
    return steps


PLAN = [plan(z, c) for z in range(4) for c in PAIR]


def fields(code):
    got = []
    for size in SIZES:
        got.append(code % size)
        code = code // size
    return *got, code


def _dot(a, b, ca, cb):
    return lax.dot_general(a, b, (((ca,), (cb,)), ((), ())), preferred_element_type=F32)


def _product(a, w):
    return _dot(a, w, 1, 0)


def _pick(z, i, table):
    out = jnp.int32(0)
    for zz, row in enumerate(table):
        got = jnp.int32(0)
        for ii, value in enumerate(row):
            got = jnp.where(i == ii, jnp.int32(value), got)
        out = jnp.where(z == zz, got, out)
    return out


def kernel(x_hbm, gain_hbm, coarse_hbm, fine_hbm, wq_hbm, wk_hbm, wv_hbm, wo_hbm, y_ref, yacc, o_last, w_last,
           xb, gainb, coarse_ref, fine_ref, ab, wqb, wkvb, wob, kb, vb, qb, ob, ls, top_s, mix_s, of, cs,
           sent, arecv, krecv, qrecv, local_o, local_l, remote_o, remote_l, go):
    dp, sp = lax.axis_index("dp"), lax.axis_index("sp")
    z, c = sp // 2, sp % 2
    n, wide = xb.shape
    rows = n // 4
    scale = HEAD**-0.5
    e = scale * LOG2E

    def push(src, dst, send, recv, to):
        pltpu.make_async_remote_copy(src, dst, sent.at[send - 1], recv, device_id=(dp, to), device_id_type=MESH).start()

    def wait(ref, sem):
        pltpu.make_async_copy(ref, ref, sem).wait()

    def send_queries(g, h, to):
        ref = qb.at[g, 2 * z + h]
        push(ref, ref, 1, qrecv.at[2 * z + h - 4], 2 * to + c)

    def project_all(wsem):
        def x_copy(i):
            at = pl.ds(i * rows, rows)
            return pltpu.make_async_copy(x_hbm.at[at], xb.at[at], wsem.at[i % 2])

        def w_copy(hbm, dst, g, width, sem):
            at = pl.ds(pl.multiple_of((c * 2 + g) * width, width), width)
            return pltpu.make_async_copy(hbm.at[:, at], dst, sem)

        wk_copy = lambda g: w_copy(wk_hbm, wkvb.at[g, :, pl.ds(0, HEAD)], g, HEAD, wsem.at[5 + g])
        wv_copy = lambda g: w_copy(wv_hbm, wkvb.at[g, :, pl.ds(HEAD, HEAD)], g, HEAD, wsem.at[7 + g])
        wq_copy = lambda g: w_copy(wq_hbm, wqb.at[g], g, 2 * HEAD, wsem.at[2 + g])
        wo_copy = pltpu.make_async_copy(wo_hbm, wob, wsem.at[0])
        g_last = jnp.where(z == 2, 1, 0)
        last_copy = pltpu.make_async_copy(wo_hbm.at[pl.ds(pl.multiple_of(((1 - c) * 4 + g_last * 2 + 1) * HEAD, HEAD), HEAD)], w_last, wsem.at[1])
        g_first = jnp.where(z == 0, 1, 0)

        count = 2 * n // FINE
        gain_copy = pltpu.make_async_copy(gain_hbm, gainb, wsem.at[2])
        tables = [pltpu.make_async_copy(fine_hbm, fine_ref, wsem.at[3]),
                  pltpu.make_async_copy(coarse_hbm.at[:, pl.ds(pl.multiple_of(z * count, 8), count)], coarse_ref, wsem.at[4])]

        for copy in gain_copy, *tables, x_copy(0), wk_copy(g_first), x_copy(1), wv_copy(g_first):
            copy.start()

        barrier = pltpu.get_barrier_semaphore()

        def here_now(chip, core):
            pl.semaphore_signal(barrier, 1, device_id=(dp, 2 * chip + core), device_id_type=MESH)

        here_now(z, 1 - c)

        @pl.when(z == 0)
        def _():
            here_now(2, c)

        @pl.when(z == 1)
        def _():
            here_now(0, c)
            here_now(2, c)
            for core in PAIR:
                here_now(3, core)

        @pl.when(z == 2)
        def _():
            here_now(3, c)

        @pl.when(z >= 2)
        def _():
            for core in PAIR:
                here_now(z - 1, core)

        def send_keys(g, h, to, at):
            ref = kb.at[g, 2 * z + h, at]
            push(ref, ref, 1, krecv.at[g if to == 1 else z % 2], 2 * to + c)

        def send_values(g, h, to):
            ref = vb.at[g, 2 * z + h]
            push(ref, ref, 1, krecv.at[g if to == 1 else z % 2], 2 * to + c)

        def send_both(g, h, to):
            send_keys(g, h, to, pl.ds(0, n))
            send_values(g, h, to)

        def turned(t, first):
            at = pl.ds(pl.multiple_of(first, rows), t.shape[0])
            cos, sin = cs[0, at, :], cs[1, at, :]
            t = t.astype(BF).astype(F32)
            a, b = t[:, : HEAD // 2], t[:, HEAD // 2 :]
            return jnp.concatenate([a * cos - b * sin, b * cos + a * sin], -1).astype(BF)

        def send(g, gi, h, what, *more):
            for at, gg, to in ((z == 1) & (g == 0), 0, 2), ((z == 2) & (g == 1), 1, 3), ((z == 0) & (gi == 0), 1, 1):
                pl.when(at)(functools.partial(what, gg, h, to, *more))

        def keep_keys(g, gi, h, k, first, greet=False):
            at = pl.ds(first, k.shape[0])
            kb[g, 2 * z + h, at, :] = turned(k, h * n + first)
            if greet:
                pl.semaphore_wait(barrier, _pick(0, z, [[2, 3, 5, 4]]))
            send(g, gi, h, send_keys, at)

        def keep_values(g, h, v, first):
            vb[g, 2 * z + h, :, first : first + v.shape[0]] = v.astype(BF).T

        def make_both(g, gi, h, first):
            kv = _product(ab[h, first : first + n // 2, :], wkvb[g])
            keep_keys(g, gi, h, kv[:, :HEAD], first)
            keep_values(g, h, kv[:, HEAD:], first)
            if first:
                send(g, gi, h, send_values)

        def turn_table(i, _):
            fc, fs = fine_ref[0], fine_ref[1]
            cc = coarse_ref[0, pl.ds(i, 1), :]
            ss = coarse_ref[1, pl.ds(i, 1), :]
            at = pl.ds(pl.multiple_of(i * FINE, FINE), FINE)
            cs[0, at, :] = cc * fc - ss * fs
            cs[1, at, :] = ss * fc + cc * fs

        def norm(i):
            x_copy(i).wait()
            at = pl.ds(i * rows, rows)
            w = xb[at, :].astype(F32)
            ab[c, at, :] = (w * lax.rsqrt(jnp.mean(w * w, -1, keepdims=True) + 1e-6) * gain).astype(BF)

        for copy in gain_copy, *tables:
            copy.wait()
        lax.fori_loop(0, count, turn_table, None, unroll=8)
        gain = gainb[...].astype(F32)[None, :]
        for i in PAIR:
            norm(i)
            x_copy(2 + i).start()
            if i == 0:
                wk_copy(g_first).wait()
            k = _product(ab[c, i * rows : (i + 1) * rows, :], wkvb[g_first, :, :HEAD])
            keep_keys(g_first, 0, c, k, i * rows, i == 0)

        @pl.when(z == 2)
        def _():
            pl.semaphore_signal(go, 1, device_id=(dp, c), device_id_type=MESH)

        @pl.when(z == 3)
        def _():
            for core in PAIR:
                pl.semaphore_signal(go, 1, device_id=(dp, 2 + core), device_id_type=MESH)

        wv_copy(g_first).wait()
        keep_values(g_first, c, _product(ab[c, : n // 2, :], wkvb[g_first, :, HEAD:]), 0)
        for i in PAIR:
            norm(2 + i)
        rows_sent = pltpu.make_async_remote_copy(ab.at[c], ab.at[c], wsem.at[9], arecv, device_id=(dp, z * 2 + 1 - c), device_id_type=MESH)
        rows_sent.start()
        make_both(g_first, 0, c, n // 2)
        wk_copy(1 - g_first).start()
        wv_copy(1 - g_first).start()
        wq_copy(1).start()
        wq_copy(0).start()

        def project(hh, _):
            h = jnp.where(hh == 0, c, 1 - c)

            @pl.when(hh == 1)
            def _():
                wait(ab.at[1 - c], arecv)
                wo_copy.start()
                last_copy.start()

            def keys(gi, _):
                g = jnp.where(gi == 0, g_first, 1 - g_first)

                @pl.when(hh == 0)
                def _():
                    wk_copy(g).wait()
                    wv_copy(g).wait()

                for r in PAIR:
                    make_both(g, gi, h, r * (n // 2))

                @pl.when((z == 0) & (gi == 1))
                def _():
                    @pl.when(hh == 0)
                    def _():
                        pl.semaphore_wait(go, 1)

                    send_both(0, h, 2)

                    @pl.when(hh == 1)
                    def _():
                        send_both(0, c, 1)
                        send_both(0, 1 - c, 1)

            lax.fori_loop(jnp.where(hh == 0, 1, 0), 2, keys, None)

            def queries(gi, _):
                g = 1 - gi

                @pl.when(hh == 0)
                def _():
                    wq_copy(g).wait()

                q = _product(ab[h], wqb[g])
                for s in PAIR:
                    qb[g, 2 * z + h, s] = turned(q[:, s * HEAD : (s + 1) * HEAD], h * n)

                @pl.when((z == 3) & (g == 1))
                def _():
                    send_queries(1, h, 1)

                @pl.when((z == 3) & (hh == 1) & (g == 0))
                def _():
                    send_queries(0, c, 2)
                    send_queries(0, 1 - c, 2)

            lax.fori_loop(0, 2, queries, None)

        lax.fori_loop(0, 2, project, None)
        yacc[...] = xb[...].astype(F32)

        for l in range(2):
            for g in PAIR:
                @pl.when((z < 2) | ((z == 2) & (g == 0)))
                def _():
                    ob[REMOTE + l * 2 + g] = jnp.zeros(ob.shape[1:], BF)
                    ls[REMOTE + l * 2 + g] = jnp.full(ls.shape[1:], LOWEST, F32)
        wo_copy.wait()
        last_copy.wait()
        rows_sent.wait_send()

    pl.run_scoped(project_all, pltpu.SemaphoreType.DMA((10,)))

    ones = jnp.ones((8, n), BF)

    def task(code):
        _, g, q, t, waits = fields(code)
        local = q // 2 == z
        first = _pick(z, g, FIRST)
        def q_wait(qq):
            wait(qb.at[g, qq], qrecv.at[qq - 4])

        @pl.when((z == 1) & (waits > 0) & (g == 1))
        def _():
            q_wait(6)
            q_wait(7)
            pl.semaphore_wait(go, 2)
            pl.semaphore_signal(go, 1, device_id=(dp, sp + 2), device_id_type=MESH)

        @pl.when((z == 2) & (waits > 0))
        def _():
            pl.semaphore_wait(go, 1)
            send_queries(1, c, 1)
            send_queries(1, 1 - c, 1)

        @pl.when(jnp.logical_not(local) & ((z == 2) | (q < 6)))
        def _():
            q_wait(q)

        for o in THIRDS:
            @pl.when((waits // 2**o) % 2 == 1)
            def _():
                wait(kb.at[g, pl.ds(0, 4)], krecv.at[jnp.where(z == 1, g, o % 2)])

        top_s[...] = jnp.full(top_s.shape, LOWEST, F32)
        mix_s[...] = jnp.zeros(mix_s.shape, F32)

        def block(j, masked):
            scores = [_dot(kb[g, j], qb[g, q, s], 1, 1) for s in range(2)]
            weights, keeps = [], []
            for s in PAIR:
                score = scores[s]
                if masked:
                    ok = lax.broadcasted_iota(jnp.int32, (n, n), 0) <= lax.broadcasted_iota(jnp.int32, (n, n), 1)
                    score = jnp.where(ok, score, LOWEST)
                old = top_s[s : s + 1, :]
                top = jnp.maximum(old, score.max(axis=0, keepdims=True))
                top_s[s : s + 1, :] = top
                weights.append(jnp.exp2((score - top) * e).astype(BF))
                keeps.append(jnp.exp2((old - top) * e))
            values = jnp.concatenate([vb[g, j], ones], axis=0)
            for s in PAIR:
                mix_s[s] = mix_s[s] * keeps[s] + _product(values, weights[s])

        lax.fori_loop(first, jnp.minimum(q, 2 * z + 2), lambda j, _: block(j, False), None)

        @pl.when(local)
        def _():
            block(q, True)

        slot = jnp.where(local, LOCAL, REMOTE) + c * 2 + g
        here = jnp.where(q == sp, slot, t)
        for s in PAIR:
            total = mix_s[s, HEAD : HEAD + 1, :]
            o = (mix_s[s, :HEAD, :] * (1 / total)).astype(BF)
            for part in QUARTERS:
                ob[here, s, part] = o[:, part * rows : (part + 1) * rows]
            lse = top_s[s : s + 1, :] * e + jnp.log2(total)
            for part in QUARTERS:
                row = 4 * s + part
                ls[here, row : row + 1, :] = lse[:, part * rows : (part + 1) * rows]

        @pl.when(local & (q != sp))
        def _():
            push(ls.at[t], ls.at[slot], 3, local_l.at[g], q)
            push(ob.at[t], ob.at[slot], 2, local_o.at[g], q)

        @pl.when(jnp.logical_not(local))
        def _():
            own = q % 2 == c
            push(ls.at[t], ls.at[slot], 3, remote_l.at[g, jnp.where(own, 0, 1)], q)

            last = (g == 1) == (q // 2 == 2)

            @pl.when(own | jnp.logical_not(last))
            def _():
                push(ob.at[t], ob.at[slot], 2, remote_o.at[jnp.where(own, g, WHOLE)], q)

            @pl.when(jnp.logical_not(own) & last)
            def _():
                for s in PAIR:
                    for part in QUARTERS:
                        push(ob.at[t, s, part], ob.at[slot, s, part], 2, remote_o.at[2 + 4 * s + part], q)

    def merged(base, s, part):
        la, lb = (ls[at + base, pl.ds(4 * s + part, 1), :] for at in (LOCAL, REMOTE))
        m = jnp.maximum(la, lb)
        wa, wb = jnp.exp2(la - m), jnp.exp2(lb - m)
        r = 1 / (wa + wb)
        o = ob[LOCAL + base, s, part].astype(F32) * (wa * r) + ob[REMOTE + base, s, part].astype(F32) * (wb * r)
        return o.T.astype(BF)

    def arrivals(g, other, first, what, sem):
        @pl.when(first & (other == 1))
        def _():
            wait(ls.at[0], local_l.at[g])
            wait(ob.at[0], local_o.at[g])

        @pl.when((z == 3) | ((z == 2) & (g == 1)))
        def _():
            @pl.when(first)
            def _():
                wait(ls.at[0], remote_l.at[g, other])

            wait(what, remote_o.at[sem])

    third = wide // 3

    def finish_line(code):
        _, g, what, _, _ = fields(code)
        other = what // 4
        l = (c + other) % 2
        base = l * 2 + g
        arrivals(g, other, True, ob.at[0], jnp.where(other == 0, g, WHOLE))
        for s in PAIR:
            for part in QUARTERS:
                of[part * rows : (part + 1) * rows, s * HEAD : (s + 1) * HEAD] = merged(base, s, part)
        at = pl.ds(pl.multiple_of((l * 4 + g * 2) * HEAD, 2 * HEAD), 2 * HEAD)

        def columns(k, _):
            cols = pl.ds(pl.multiple_of(k * third, 128), third)
            yacc[:, cols] += _product(of[...], wob[at, cols])

        lax.fori_loop(0, 3, columns, None)

    def finish_piece(code):
        _, g, what, _, _ = fields(code)
        s, part = what // 4, what % 4
        l = 1 - c
        base = l * 2 + g
        arrivals(g, 1, what == 0, ob.at[0, 0, 0], 2 + what)
        o = merged(base, s, part)
        at = pl.ds(pl.multiple_of((l * 4 + g * 2 + s) * HEAD, HEAD), HEAD)
        tokens = pl.ds(pl.multiple_of(part * rows, rows), rows)

        def add(store):
            of[0:rows, 0:HEAD] = o
            for k in THIRDS:
                cols = slice(k * third, (k + 1) * third)
                store(cols, yacc[tokens, cols] + _product(of[0:rows, 0:HEAD], wob[at, cols]))

        @pl.when(s == 0)
        def _():
            def store(cols, y):
                yacc[tokens, cols] = y

            add(store)

        @pl.when((s == 1) & (part < 3))
        def _():
            def store(cols, y):
                y_ref[tokens, cols] = y.astype(BF)

            add(store)

        @pl.when((s == 1) & (part == 3))
        def _():
            o_last[...] = o

    steps = jnp.where(z == 1, 19, jnp.where(z == 2, 17, 15))

    def drain():
        for zz in range(4):
            @pl.when(z == zz)
            def _():
                wait(qb.at[0, pl.ds(0, SENT[zz])], sent.at[0])
                wait(ob.at[pl.ds(0, STAGED[zz])], sent.at[1])
                wait(ls.at[pl.ds(0, STAGED[zz])], sent.at[2])

    def step(i, _):
        code = _pick(sp, i, PLAN)

        @pl.when(code % 4 == 0)
        def _():
            task(code)

        @pl.when(code % 4 == 2)
        def _():
            finish_line(code)

        @pl.when(code % 4 == 1)
        def _():
            @pl.when((z != 1) & (i == steps - 1))
            def _():
                drain()

            finish_piece(code)

    lax.fori_loop(0, steps, step, None)

    @pl.when(z == 1)
    def _():
        drain()


def write(y_ref, yacc, o_last, w_last, y_hbm, out, sem):
    n, wide = y_ref.shape
    pltpu.make_async_copy(y_ref, y_hbm.at[pl.ds(0, n)], sem).start()
    for k in THIRDS:
        cols = slice(k * (wide // 3), (k + 1) * (wide // 3))
        out[k] = (yacc[n:, cols] + _product(o_last[...], w_last[:, cols])).astype(BF)
        pltpu.make_async_copy(out.at[k], y_hbm.at[pl.ds(n, n // 3), cols], sem).start()
    pltpu.make_async_copy(y_hbm, y_hbm, sem).wait()


def solution(mesh):
    def step(x, gain, wq, wk, wv, wo):
        n, wide = x.shape
        half = HEAD // 2
        rate = np.float64(THETA) ** (-np.arange(half) / half)
        table = lambda places: jnp.asarray(np.stack([f(places[:, None] * rate) for f in (np.cos, np.sin)]).astype(np.float32))
        coarse, fine = table(np.arange(8 * n // FINE) * FINE), table(np.arange(FINE))
        hbm, vmem = pl.BlockSpec(memory_space=pl.ANY), pl.BlockSpec(memory_space=pltpu.VMEM)
        dma = pltpu.SemaphoreType.DMA
        parts = pl.pallas_call(
            kernel,
            out_shape=[pltpu.VMEM((3 * n // 4, wide), BF), pltpu.VMEM((n, wide), F32), pltpu.VMEM((n // 4, HEAD), BF), pltpu.VMEM((HEAD, wide), BF)],
            in_specs=[hbm] * 8,
            out_specs=[vmem] * 4,
            scratch_shapes=[
                pltpu.VMEM((n, wide), BF),
                pltpu.VMEM((wide,), BF),
                pltpu.VMEM((2, 2 * n // FINE, half), F32),
                pltpu.VMEM((2, FINE, half), F32),
                pltpu.VMEM((2, n, wide), BF),
                pltpu.VMEM((2, wide, 2 * HEAD), BF),
                pltpu.VMEM((2, wide, 2 * HEAD), BF),
                pltpu.VMEM((8 * HEAD, wide), BF),
                pltpu.VMEM((2, 8, n, HEAD), BF),
                pltpu.VMEM((2, 8, HEAD, n), BF),
                pltpu.VMEM((2, 8, 2, n, HEAD), BF),
                pltpu.VMEM((16, 2, 4, HEAD, n // 4), BF),
                pltpu.VMEM((16, 8, 128), F32),
                pltpu.VMEM((8, n), F32),
                pltpu.VMEM((2, HEAD + 8, n), F32),
                pltpu.VMEM((n, 2 * HEAD), BF),
                pltpu.VMEM((2, 2 * n, half), F32),
                dma((3,)), dma,
                dma((2,)), dma((4,)),
                dma((2,)), dma((2,)), dma((11,)), dma((2, 2)),
                pltpu.SemaphoreType.REGULAR,
            ],
            compiler_params=pltpu.CompilerParams(collective_id=0, has_side_effects=True, vmem_limit_bytes=55 << 20),
        )(x, gain, coarse, fine, wq, wk, wv, wo)
        return pl.pallas_call(
            write,
            out_shape=jax.ShapeDtypeStruct((n, wide), BF),
            in_specs=[vmem] * 4,
            out_specs=hbm,
            scratch_shapes=[pltpu.VMEM((3, n // 4, wide // 3), BF), dma],
            compiler_params=pltpu.CompilerParams(vmem_limit_bytes=4 << 20),
        )(*(pltpu.with_memory_space_constraint(part, pltpu.VMEM) for part in parts))

    tokens, whole = P(("dp", "sp"), None), P(None, None)
    return jax.shard_map(
        step,
        mesh=mesh,
        in_specs=(tokens, P(None), whole, whole, whole, whole),
        out_specs=tokens,
        check_vma=False,
    )
```
